128 devices in a mesh: dp: 1, ep: 128 (over z, y, x, core).
Axes of the slice: x: 4, y: 4, z: 4, core: 2. Of those that a mesh axis runs over, the one named last changes fastest.
Arguments:
- hidden: bfloat16 [32768, 2048], P(('dp', 'ep'))
- route_idx: int32 [32768, 8], P(('dp', 'ep'))
- gate_weights: float32 [32768, 8], P(('dp', 'ep'))
- w_gate: bfloat16 [128, 2048, 768], P('ep')
- w_up: bfloat16 [128, 2048, 768], P('ep')
- w_down: bfloat16 [128, 768, 2048], P('ep')
Outputs:
- output: bfloat16 [32768, 2048], P(('dp', 'ep'))
All inputs are finite; a program needn't handle non-finite values.
Results may differ from the reference program's by a relative error of at most 0.00154.
Values are sent between devices in bfloat16 or wider.
A program may use at most 1 GiB of HBM per device.

```python
import jax
import jax.numpy as jnp
from jax import lax

D_MODEL = 2048
D_FF = 768
EXPERTS = 128
TOP_K = 8
GROUP_SIZE = 128
TOKENS_DEV = 256
ROW_CAP = 64
HOT_EXPERTS = 8

COLD_EXPERTS = EXPERTS - HOT_EXPERTS
REST_SLOTS = TOKENS_DEV * TOP_K - HOT_EXPERTS * ROW_CAP
COLD_SPREAD = min(REST_SLOTS // COLD_EXPERTS - 1, ROW_CAP - (REST_SLOTS + COLD_EXPERTS - 1) // COLD_EXPERTS)
COLD_PAIRS = COLD_EXPERTS // 2
TOKENS_PART = GROUP_SIZE * TOKENS_DEV


def draw_routes(route_key):
    key_hot, key_src = jax.random.split(route_key)
    expert_order = jax.random.permutation(key_hot, EXPERTS)
    cold_pos = jnp.arange(COLD_EXPERTS)
    cold_base = (cold_pos + 1) * REST_SLOTS // COLD_EXPERTS - cold_pos * REST_SLOTS // COLD_EXPERTS
    hot_counts = jnp.full((HOT_EXPERTS,), ROW_CAP, jnp.int32)
    slot_seq = jnp.arange(TOKENS_DEV * TOP_K)

    def one_source(src_key):
        key_shift, key_cold, key_tok, key_rot = jax.random.split(src_key, 4)
        pair_shift = jax.random.randint(key_shift, (COLD_PAIRS,), 0, COLD_SPREAD + 1)
        count_delta = jnp.concatenate([jnp.stack([pair_shift, -pair_shift], axis=1).reshape(-1), jnp.zeros((COLD_EXPERTS - 2 * COLD_PAIRS,), jnp.int32)])
        cold_counts = (cold_base + count_delta)[jax.random.permutation(key_cold, COLD_EXPERTS)]
        block_ends = jnp.cumsum(jnp.concatenate([hot_counts, cold_counts]))
        seq_experts = expert_order[jnp.searchsorted(block_ends, slot_seq, side='right')]
        choice_table = seq_experts.reshape(TOP_K, TOKENS_DEV).T[jax.random.permutation(key_tok, TOKENS_DEV)]
        slot_shift = jax.random.randint(key_rot, (TOKENS_DEV, 1), 0, TOP_K)
        slot_cols = (jnp.arange(TOP_K)[None, :] + slot_shift) % TOP_K
        return jnp.take_along_axis(choice_table, slot_cols, axis=1)

    all_routes = jax.vmap(one_source)(jax.random.split(key_src, GROUP_SIZE))
    return all_routes.reshape(TOKENS_PART, TOP_K).astype(jnp.int32)


def setup_inputs(seed: int = 0, part: int = 0) -> dict:
    base_key = jax.random.key(seed)
    part_key = jax.random.fold_in(base_key, part)
    key_x, key_gate, key_route = jax.random.split(part_key, 3)
    key_wg, key_wu, key_wd = jax.random.split(jax.random.key(seed + 1), 3)
    hidden = jax.random.normal(key_x, (TOKENS_PART, D_MODEL), jnp.float32).astype(jnp.bfloat16)
    gate_weights = jax.random.uniform(key_gate, (TOKENS_PART, TOP_K), jnp.float32, 0.3, 0.7) * (2.0 / TOP_K)
    route_idx = draw_routes(key_route)
    w_gate = (jax.random.normal(key_wg, (EXPERTS, D_MODEL, D_FF), jnp.float32) * D_MODEL ** -0.5).astype(jnp.bfloat16)
    w_up = (jax.random.normal(key_wu, (EXPERTS, D_MODEL, D_FF), jnp.float32) * D_MODEL ** -0.5).astype(jnp.bfloat16)
    w_down = (jax.random.normal(key_wd, (EXPERTS, D_FF, D_MODEL), jnp.float32) * (2.0 * D_FF ** -0.5)).astype(jnp.bfloat16)
    return {'hidden': hidden, 'route_idx': route_idx, 'gate_weights': gate_weights, 'w_gate': w_gate, 'w_up': w_up, 'w_down': w_down}


def reference(hidden, route_idx, gate_weights, w_gate, w_up, w_down):
    expert_cap = GROUP_SIZE * ROW_CAP
    pair_count = TOKENS_PART * TOP_K
    flat_ids = route_idx.reshape(-1)
    sort_order = jnp.argsort(flat_ids, stable=True)
    counts = jnp.bincount(flat_ids, length=EXPERTS)
    starts = jnp.cumsum(counts) - counts
    slot_range = jnp.arange(expert_cap)
    pair_pos = jnp.minimum(starts[:, None] + slot_range[None, :], pair_count - 1)
    pair_ids = sort_order[pair_pos]
    is_valid = slot_range[None, :] < counts[:, None]
    tok_rows = pair_ids // TOP_K
    row_gates = jnp.where(is_valid, gate_weights.reshape(-1)[pair_ids], 0.0)

    def expert_step(y_accum, scan_items):
        tok_idx, gate_col, gate_mat, up_mat, down_mat = scan_items
        expert_in = hidden[tok_idx]
        gate_proj = jnp.dot(expert_in, gate_mat, preferred_element_type=jnp.float32)
        up_proj = jnp.dot(expert_in, up_mat, preferred_element_type=jnp.float32)
        hidden_act = (jax.nn.silu(gate_proj) * up_proj).astype(jnp.bfloat16)
        expert_out = jnp.dot(hidden_act, down_mat, preferred_element_type=jnp.float32).astype(jnp.bfloat16)
        y_accum = y_accum.at[tok_idx].add(gate_col[:, None] * expert_out.astype(jnp.float32))
        return y_accum, None

    y_total = lax.scan(expert_step, jnp.zeros((TOKENS_PART, D_MODEL), jnp.float32), (tok_rows, row_gates, w_gate, w_up, w_down))[0]
    return y_total.astype(jnp.bfloat16)
```

```python
import functools

import jax
import jax.numpy as jnp
from jax import lax
from jax.experimental import pallas as pl
from jax.experimental.pallas import tpu as pltpu
from jax.sharding import Mesh, PartitionSpec as P

BF16 = jnp.bfloat16
F32 = jnp.float32
GRID = ('z', 'y', 'x', 'c')
SIZES = (4, 4, 4, 2)
PLANE = ('z', 'y')
LINE = ('x', 'c')
ROW_CAP = 64
GROUP = 4


def split3(g):
    a = lax.reduce_precision(g, 8, 7)
    b = lax.reduce_precision(g - a, 8, 7)
    return a.astype(BF16), b.astype(BF16), (g - a - b).astype(BF16)


def down_kernel(h_ref, w_ref, g_ref, out_ref, o_ref):
    experts = h_ref.shape[0]
    slots = experts * ROW_CAP

    def one_expert(e, _):
        o = jnp.dot(h_ref[e], w_ref[e], preferred_element_type=F32).astype(BF16)
        at = pl.multiple_of(e * ROW_CAP, ROW_CAP)
        for q in range(GROUP):
            o_ref[q, pl.ds(at, ROW_CAP), :] = o[q * ROW_CAP:(q + 1) * ROW_CAP]
        return _

    lax.fori_loop(0, experts, one_expert, 0)

    def one_block(q, _):
        o = o_ref[q]
        g = g_ref[q]
        acc = jnp.dot(g[:, :slots], o, preferred_element_type=F32)
        acc += jnp.dot(g[:, slots:2 * slots], o, preferred_element_type=F32)
        acc += jnp.dot(g[:, 2 * slots:], o, preferred_element_type=F32)
        out_ref[q] = acc
        return _

    lax.fori_loop(0, GROUP, one_block, 0)


def down_and_mix(h, w, g):
    experts, rows, f = h.shape
    n = w.shape[2]
    blocks, tokens, _ = g.shape
    steps = blocks // GROUP
    flops = 2 * rows * experts * f * n + 2 * blocks * tokens * g.shape[2] * n
    return pl.pallas_call(
        down_kernel,
        grid=(steps,),
        in_specs=[
            pl.BlockSpec((experts, GROUP * ROW_CAP, f), lambda i: (0, i, 0)),
            pl.BlockSpec((experts, f, n), lambda i: (0, 0, 0)),
            pl.BlockSpec((GROUP, tokens, g.shape[2]), lambda i: (i, 0, 0)),
        ],
        out_specs=pl.BlockSpec((GROUP, tokens, n), lambda i: (i, 0, 0)),
        out_shape=jax.ShapeDtypeStruct((blocks, tokens, n), F32),
        scratch_shapes=[pltpu.VMEM((GROUP, experts * ROW_CAP, n), BF16)],
        compiler_params=pltpu.CompilerParams(vmem_limit_bytes=60 * 1024 * 1024),
        cost_estimate=pl.CostEstimate(flops=flops, bytes_accessed=2 * (h.size + w.size + g.size) + 4 * blocks * tokens * n, transcendentals=0),
        name='down_and_mix',
    )(h, w, g)


def solution(mesh):
    grid = Mesh(mesh.devices.reshape((mesh.shape['dp'],) + SIZES), ('dp',) + GRID)

    def body(hidden, route_idx, gate_weights, w_gate, w_up, w_down):
        T, K = route_idx.shape
        D = hidden.shape[1]
        half = D // 2
        gather = functools.partial(lax.all_gather, tiled=False)
        tok = lax.all_gather(hidden, PLANE, axis=0)
        wg = lax.all_gather(w_gate, LINE, axis=0, tiled=True)
        wu = lax.all_gather(w_up, LINE, axis=0, tiled=True)
        wd = [lax.all_gather(w_down[:, :, s:s + half], LINE, axis=0, tiled=True) for s in (0, half)]
        ids = lax.all_gather(route_idx, PLANE, axis=0)
        gates = lax.all_gather(gate_weights, PLANE, axis=0)
        E = wg.shape[0]
        B = tok.shape[0]
        base = (lax.axis_index('z') * SIZES[1] + lax.axis_index('y')) * E
        hit = ids[:, :, :, None] == base + jnp.arange(E)
        chosen = jnp.any(hit, axis=2)
        gate = jnp.sum(jnp.where(hit, gates[..., None], 0.0), axis=2)
        rank = jnp.cumsum(chosen.astype(jnp.int32), axis=1) - 1
        slot = jnp.where(chosen, rank, -1)
        pick = slot[..., None] == jnp.arange(ROW_CAP)
        onehot = pick.astype(BF16).reshape(B, T, E * ROW_CAP)
        mix = jnp.concatenate([jnp.where(pick, s[..., None], 0).reshape(B, T, E * ROW_CAP) for s in split3(gate)], axis=2)
        rows = jnp.einsum('btm,btd->bmd', onehot, tok, preferred_element_type=F32).astype(BF16)
        rows = rows.reshape(B, E, ROW_CAP, D).transpose(1, 0, 2, 3).reshape(E, B * ROW_CAP, D)
        a = jnp.einsum('erd,edf->erf', rows, wg, preferred_element_type=F32)
        b = jnp.einsum('erd,edf->erf', rows, wu, preferred_element_type=F32)
        h = (jax.nn.silu(a) * b).astype(BF16)
        outs = []
        for w in wd:
            part = down_and_mix(h, w, mix)
            out = lax.psum_scatter(part.reshape(B * T, half), PLANE, scatter_dimension=0, tiled=True)
            outs.append(out.astype(BF16))
        return jnp.concatenate(outs, axis=1)

    r = P(('dp',) + GRID, None)
    e = P(GRID, None, None)
    return jax.shard_map(body, mesh=grid, in_specs=(r, r, r, e, e, e), out_specs=r, check_vma=False)
```

```python
import jax
import jax.numpy as jnp
from jax import lax
from jax.experimental import pallas as pl
from jax.experimental.pallas import tpu as pltpu
from jax.sharding import Mesh, PartitionSpec as P

BF16 = jnp.bfloat16
F32 = jnp.float32
MESH = pl.DeviceIdType.MESH
GRID = ('z', 'y', 'x', 'c')
SIZES = (4, 4, 4, 2)
ROW_CAP = 64
EXPERTS = 8
BLOCKS = 16
TILE = 8
MIB = 1024 * 1024


def expert_ids(place, x, c, line):
    dx = jnp.where((place == 2) | (place == 4), 3, 0) + jnp.where((place == 3) | (place == 5), 1, 0)
    dx += jnp.where(place >= 6, 2, 0)
    core = jnp.where(place == 0, c, 0) + jnp.where(place == 1, 1 - c, 0)
    core += jnp.where((place == 4) | (place == 5) | (place == 7), 1, 0)
    return line * EXPERTS + lax.rem(x + dx, 4) * 2 + core


def moe_kernel(hid, meta, wg, wu, wd, out, o_hbm, x_hbm, rows_in, relay, hg, hu, hd,
               tok, metas, slots, tabs, acc, rf2, rn2, stage, xt, hbuf, bg, bu, bd,
               tsend, trecv, msend, mrecv, isend, irecv, fsend, frecv, dsend, drecv, psend, precv,
               nrsend, nrrecv, frsend, frrecv, fwsend, fwrecv, f2send, f2recv, n2send, n2recv,
               lsem, ssem, wsem, xsem, csem):
    z, y, x, c = (lax.axis_index(a) for a in GRID)
    right, left = lax.rem(x + 1, 4), lax.rem(x + 3, 4)
    tokens, d = hid.shape
    half, cols = tokens // 2, d // 2
    rows = TILE * ROW_CAP
    own = (wg, wu, wd)
    held = (hg, hu, hd)
    partner = {'c': 1 - c}

    def remote(src, dst, send, recv, where):
        return pltpu.make_async_remote_copy(src_ref=src, dst_ref=dst, send_sem=send, recv_sem=recv, device_id=where, device_id_type=MESH)

    def along(dim, step):
        return {'z': lax.rem(z + (1 - dim) * step, 4), 'y': lax.rem(y + dim * step, 4)}

    def quarter(ref, m, lane, q, count=1):
        n = own[m].shape[0] // 4
        return ref.at[pl.ds(pl.multiple_of((2 * lane + q) * n, n), count * n), :]

    def line_copy(way, k, m, q, src):
        dst = held[m].at[2 + 2 * k + way]
        return remote(quarter(src, m, c, q), quarter(dst, m, c, q), isend.at[way, k, m, q], irecv.at[way, k, m, q], {'x': right if way == 0 else left})

    def far_copy(k, m, q):
        src, dst = held[m].at[2 + 2 * k + q], held[m].at[6 + k]
        return remote(quarter(src, m, c, q), quarter(dst, m, c, q), fsend.at[k, m, q], frecv.at[k, m, q], {'x': right if q == 0 else left})

    def hand_own(m, n):
        lane = 1 - c if n == 0 else c
        return remote(quarter(own[m], m, lane, 0, 2), quarter(held[m].at[c], m, lane, 0, 2), dsend.at[m, n], drecv.at[m, n], partner)

    def hand_on(slot, m):
        ref = quarter(held[m].at[slot], m, c, 0, 2)
        return remote(ref, ref, psend.at[slot - 2, m], precv.at[slot - 2, m], partner)

    def start_line(k, srcs):
        for n in (0, 1):
            for m in range(3):
                line_copy(0, k, m, n, srcs[m]).start()
                line_copy(1, k, m, 1 - n, srcs[m]).start()

    def place(k, a, b):
        return a * 4 + b if k == 0 else b * 4 + a

    def part(k, a, b, h=None):
        r = pl.ds(0, tokens) if h is None else pl.ds(h * half, half)
        return tok.at[place(k, a, b), r, pl.ds(k * cols, cols)]

    def first_copy(k, way):
        sems = tsend.at[k, 4, way], trecv.at[k, 4, way], along(k, 1 + 2 * (way % 2))
        if way < 2:
            return remote(part(k, 0, 0), part(k, 3 - 2 * way, 0), *sems)
        return remote(part(k, 7 - 2 * way, 0, way - 2), part(k, 2, 0, way - 2), *sems)

    def second_copy(k, a, way):
        sems = tsend.at[k, a, way], trecv.at[k, a, way], along(1 - k, 1 + 2 * (way % 2))
        if way < 2:
            return remote(part(k, a, 0), part(k, a, 3 - 2 * way), *sems)
        return remote(part(k, a, 7 - 2 * way, way - 2), part(k, a, 2, way - 2), *sems)

    def meta_copy(dz, dy):
        s = ((4 - dz) % 4) * 4 + (4 - dy) % 4
        return remote(metas.at[0], metas.at[s], msend.at[s], mrecv.at[s], {'z': lax.rem(z + dz, 4), 'y': lax.rem(y + dy, 4)})

    peers = [(dz, dy) for dz in range(4) for dy in range(4) if dz or dy]

    def spread(color, i, ring, m, n):
        if color == 0:
            return o_hbm.at[i, pl.ds(m, n), ring, :, pl.ds(0, cols)]
        return o_hbm.at[i, ring, pl.ds(m, n), :, pl.ds(cols, cols)]

    def near_rows(i, color, h):
        return remote(spread(color, i, 1 + 2 * h, 0, 4), rows_in.at[i, color, 2 - 2 * h], nrsend.at[i, color, h], nrrecv.at[i, color, h], along(1 - color, 1 + 2 * h))

    def far_rows(i, color, h):
        return remote(spread(color, i, 2, 2 * h, 2), relay.at[i, color, h], frsend.at[i, color, h], frrecv.at[i, color, h], along(1 - color, 1 + 2 * h))

    def pass_rows(i, color, h):
        return remote(relay.at[i, color, h], rows_in.at[i, color, 1, pl.ds(2 * h, 2)], fwsend.at[i, color, h], fwrecv.at[i, color, h], along(1 - color, 1 + 2 * h))

    def far_sum(color, h):
        return remote(acc.at[color, 2, pl.ds(h * half, half), :], rf2.at[color, h], f2send.at[color, h], f2recv.at[color, h], along(color, 1 + 2 * h))

    def near_sum(color, h):
        return remote(acc.at[color, 1 + 2 * h], rn2.at[color, h], n2send.at[color, h], n2recv.at[color, h], along(color, 1 + 2 * h))

    both = [(color, h) for color in (0, 1) for h in (0, 1)]

    own_tok = pltpu.make_async_copy(hid, tok.at[0], lsem.at[0])
    own_tok.start()
    own_meta = pltpu.make_async_copy(meta, metas.at[0], lsem.at[1])
    own_meta.start()

    barrier = pltpu.get_barrier_semaphore()
    for where in [partner, {'x': right}, {'x': left}] + [{'z': lax.rem(z + dz, 4), 'y': lax.rem(y + dy, 4)} for dz, dy in peers]:
        pl.semaphore_signal(barrier, inc=1, device_id=where, device_id_type=MESH)
    pl.semaphore_wait(barrier, 3 + len(peers))

    for n in (0, 1):
        for m in range(3):
            hand_own(m, n).start()

    @pl.when(c == 0)
    def _():
        start_line(0, own)

    own_tok.wait()
    for k in (0, 1):
        for way in (0, 1):
            first_copy(k, way).start()
            second_copy(k, 0, way).start()
    own_meta.wait()
    for dz, dy in peers:
        meta_copy(dz, dy).start()
    for m in range(3):
        hand_own(m, 0).wait_recv()

    @pl.when(c == 0)
    def _():
        start_line(1, [ref.at[1] for ref in held])

    @pl.when(c == 1)
    def _():
        start_line(0, [ref.at[0] for ref in held])
        start_line(1, own)

    for k in (0, 1):
        first_copy(k, 0).wait_recv()
        first_copy(k, 2).start()
        second_copy(k, 3, 0).start()
        second_copy(k, 3, 1).start()
        first_copy(k, 1).wait_recv()
        first_copy(k, 3).start()
        second_copy(k, 1, 0).start()
        second_copy(k, 1, 1).start()
    for k in (0, 1):
        for way in (0, 1):
            second_copy(k, 0, way).wait_recv()
            second_copy(k, 0, 2 + way).start()
    for k in (0, 1):
        first_copy(k, 2).wait_recv()
        first_copy(k, 3).wait_recv()
        second_copy(k, 2, 0).start()
        second_copy(k, 2, 1).start()

    for dz, dy in peers:
        meta_copy(dz, dy).wait_recv()
    order = lax.broadcasted_iota(jnp.int32, (EXPERTS, tokens), 0)
    earlier = lax.broadcasted_iota(jnp.int32, (tokens, tokens), 0) < lax.broadcasted_iota(jnp.int32, (tokens, tokens), 1)
    earlier = jnp.where(earlier, 1.0, 0.0).astype(BF16)

    def table(s, line, terms):
        mine = expert_ids(order, x, c, line).astype(F32)
        rec = metas[s]
        top = rec.shape[0] // 4
        sums = [jnp.zeros((EXPERTS, tokens), F32) for _ in range(1 + terms)]
        for k in range(top):
            hit = rec[k:k + 1, :] == mine
            sums[0] += jnp.where(hit, 1.0, 0.0)
            for p in range(1, 1 + terms):
                sums[p] += jnp.where(hit, rec[p * top + k:p * top + k + 1, :], 0.0)
        rank = jnp.dot(sums[0].astype(BF16), earlier, preferred_element_type=F32)
        return [jnp.where(sums[0] > 0.5, rank, -1.0)] + sums[1:]

    def own_table(s, carry):
        slots[s], = table(s, z * 4 + y, 0)
        return carry

    lax.fori_loop(0, BLOCKS, own_table, 0)

    def ring_table(n, carry):
        color, m, s = n // 16, lax.rem(n // 4, 4), lax.rem(n, 4)
        line = lax.rem(z + color * s, 4) * 4 + lax.rem(y + (1 - color) * s, 4)
        for p, t in enumerate(table((4 - 3 * color) * m, line, 3)):
            tabs[color, m, s, p] = t
        return carry

    def turn(a):
        for k in (0, 1):
            for way in (0, 1):
                second_copy(k, a, way).wait_recv()
                second_copy(k, a, 2 + way).start()

    turn(3)
    turn(1)
    turn(2)
    lax.fori_loop(0, 32, ring_table, 0)
    for a in range(4):
        for k in (0, 1):
            for way in (2, 3):
                second_copy(k, a, way).wait_recv()

    def x_store(s, b):
        return pltpu.make_async_copy(stage.at[b], x_hbm.at[:, s], ssem.at[b])

    lanes = lax.broadcasted_iota(jnp.int32, (ROW_CAP, tokens), 0).astype(F32)

    def gather(s, carry):
        b = lax.rem(s, 2)
        pick = jnp.concatenate([jnp.where(slots[s, pl.ds(e, 1), :] == lanes, 1.0, 0.0).astype(BF16) for e in range(EXPERTS)], axis=0)
        got = jnp.dot(pick, tok[s], preferred_element_type=F32).astype(BF16)

        @pl.when(s >= 2)
        def _():
            x_store(s, b).wait()

        stage[b] = got.reshape(EXPERTS, ROW_CAP, d)
        x_store(s, b).start()
        return carry

    lax.fori_loop(0, BLOCKS, gather, 0)
    acc[...] = jnp.zeros(acc.shape, F32)
    x_store(0, 0).wait()
    x_store(0, 1).wait()
    for k in (0, 1):
        for way in range(4):
            first_copy(k, way).wait_send()
            for a in range(4):
                second_copy(k, a, way).wait_send()

    def load(i, m, go):
        dst = (bg, bu, bd)[m]

        @pl.when(i == 0)
        def _():
            go(pltpu.make_async_copy(own[m], dst, wsem.at[m]))

        @pl.when(i == 1)
        def _():
            go(pltpu.make_async_copy(held[m].at[1 - c], dst, wsem.at[m]))

        @pl.when(i >= 2)
        def _():
            go(pltpu.make_async_copy(held[m].at[i], dst, wsem.at[m]))

    def arrive(i, ms):
        @pl.when(i == 1)
        def _():
            for m in ms:
                hand_own(m, 1).wait_recv()

        for k in (0, 1):
            @pl.when(i == 2 + 2 * k)
            def _():
                for m in ms:
                    for way in (0, 1):
                        for q in (way, 1 - way):
                            line_copy(way, k, m, q, held[m].at[k]).wait_recv()
                        far_copy(k, m, way).start()
                        hand_on(2 + 2 * k + way, m).start()
                for m in ms:
                    hand_on(2 + 2 * k, m).wait_recv()

            @pl.when(i == 3 + 2 * k)
            def _():
                for m in ms:
                    hand_on(3 + 2 * k, m).wait_recv()

            @pl.when(i == 6 + k)
            def _():
                for m in ms:
                    far_copy(k, m, 0).wait_recv()
                    far_copy(k, m, 1).wait_recv()
                    hand_on(6 + k, m).start()
                for m in ms:
                    hand_on(6 + k, m).wait_recv()

    def x_load(i, t):
        return pltpu.make_async_copy(x_hbm.at[i, pl.ds(t * TILE, TILE)], xt.at[t], xsem.at[t])

    def o_store(i, t):
        return pltpu.make_async_copy(stage.at[t].reshape(2, 4, ROW_CAP, d), o_hbm.at[i, pl.ds(2 * t, 2)], ssem.at[t])

    def begin(cp):
        cp.start()

    def finish(cp):
        cp.wait()

    def relay_rows(i):
        for color, h in both:
            far_rows(i, color, h).wait_recv()
            pass_rows(i, color, h).start()

    def row_loads(i, color):
        at = pl.ds(8 * lax.rem(i, 2) + 4 * color, 4)
        srcs = [spread(color, i, 0, 0, 4)] + [rows_in.at[i, color, s] for s in range(3)]
        return [pltpu.make_async_copy(src, tok.at[at, pl.ds(s * ROW_CAP, ROW_CAP), pl.ds(0, cols)], csem.at[color, s]) for s, src in enumerate(srcs)]

    def combine(i):
        for color in (0, 1):
            for h in (0, 1):
                near_rows(i, color, h).wait_recv()
                pass_rows(i, color, h).wait_recv()
            for cp in row_loads(i, color):
                cp.start()
        for color in (0, 1):
            for cp in row_loads(i, color):
                cp.wait()

        def one(n, carry):
            j, color = n // 2, lax.rem(n, 2)
            m = lax.rem(2 + 3 * j + 3 * (j * (j - 1) // 2), 4)
            got = tok[8 * lax.rem(i, 2) + 4 * color + m, :, pl.ds(0, cols)]
            total = acc[color, m]
            for p in range(1, 4):
                g = jnp.concatenate([
                    jnp.where(tabs[color, m, s, 0, pl.ds(i, 1), :] == lanes, tabs[color, m, s, p, pl.ds(i, 1), :], 0.0).astype(BF16)
                    for s in range(4)], axis=0)
                total += lax.dot_general(g, got, (((0,), (0,)), ((), ())), preferred_element_type=F32)
            acc[color, m] = total
            for k in (0, 1):
                @pl.when((i == EXPERTS - 1) & (n == k))
                def _():
                    far_sum(k, 0).start()
                    far_sum(k, 1).start()
            return carry

        lax.fori_loop(0, 8, one, 0)

    def expert(i, carry):
        @pl.when(i < EXPERTS)
        def _():
            for t in (0, 1):
                x_load(i, t).start()

        @pl.when((i >= 1) & (i <= EXPERTS))
        def _():
            relay_rows(i - 1)

        @pl.when(i < EXPERTS)
        def _():
            arrive(i, (0, 1))
            load(i, 0, begin)
            load(i, 1, begin)
            load(i, 0, finish)
            load(i, 1, finish)

            def up(t, carry):
                x_load(i, t).wait()
                xs = xt[t].reshape(rows, d)
                a = jnp.dot(xs, bg[...], preferred_element_type=F32)
                u = jnp.dot(xs, bu[...], preferred_element_type=F32)
                hbuf[t] = (jax.nn.silu(a) * u).astype(BF16)
                return carry

            lax.fori_loop(0, 2, up, 0)

        @pl.when(i >= 2)
        def _():
            combine(i - 2)

        @pl.when(i < EXPERTS)
        def _():
            arrive(i, (2,))
            load(i, 2, begin)
            load(i, 2, finish)

            def down(t, carry):
                o = jnp.dot(hbuf[t], bd[...], preferred_element_type=F32).astype(BF16)
                stage[t] = o.reshape(TILE, ROW_CAP, d)
                o_store(i, t).start()
                return carry

            lax.fori_loop(0, 2, down, 0)
            for t in (0, 1):
                o_store(i, t).wait()
            for color, h in both:
                far_rows(i, color, h).start()
            for color, h in both:
                near_rows(i, color, h).start()

        return carry

    lax.fori_loop(0, EXPERTS + 2, expert, 0)

    for color, h in both:
        far_sum(color, h).wait_recv()
        r = pl.ds(h * half, half)
        acc[color, 1 + 2 * h, r, :] = acc[color, 1 + 2 * h, r, :] + rf2[color, h]
        near_sum(color, h).start()
    for color in (0, 1):
        for h in (0, 1):
            near_sum(color, h).wait_recv()
        out[:, color * cols:(color + 1) * cols] = (acc[color, 0] + rn2[color, 0] + rn2[color, 1]).astype(out.dtype)

    for color, h in both:
        far_sum(color, h).wait_send()
        near_sum(color, h).wait_send()

    def drain(i, carry):
        for color, h in both:
            near_rows(i, color, h).wait_send()
            far_rows(i, color, h).wait_send()
            pass_rows(i, color, h).wait_send()
        return carry

    lax.fori_loop(0, EXPERTS, drain, 0)
    for dz, dy in peers:
        meta_copy(dz, dy).wait_send()
    for m in range(3):
        for n in (0, 1):
            hand_own(m, n).wait_send()
            for k in (0, 1):
                far_copy(k, m, n).wait_send()
                for way in (0, 1):
                    line_copy(way, k, m, n, held[m].at[k]).wait_send()
        for slot in range(2, 8):
            hand_on(slot, m).wait_send()


def run_moe(hidden, meta, w_gate, w_up, w_down):
    tokens, d = hidden.shape
    f = w_gate.shape[1]
    half, cols = tokens // 2, d // 2
    hbm = pl.BlockSpec(memory_space=pl.ANY)
    dma = pltpu.SemaphoreType.DMA
    flops = 2 * EXPERTS * BLOCKS * ROW_CAP * d * (3 * f + 4 * tokens)

    def both_ways(*shape):
        return [dma(shape), dma(shape)]

    return pl.pallas_call(
        moe_kernel,
        in_specs=[hbm] * 5,
        out_specs=[pl.BlockSpec(memory_space=pltpu.VMEM)] + [hbm] * 7,
        out_shape=[
            jax.ShapeDtypeStruct((tokens, d), BF16),
            jax.ShapeDtypeStruct((EXPERTS, 4, 4, ROW_CAP, d), BF16),
            jax.ShapeDtypeStruct((EXPERTS, BLOCKS, ROW_CAP, d), BF16),
            jax.ShapeDtypeStruct((EXPERTS, 2, 3, 4, ROW_CAP, cols), BF16),
            jax.ShapeDtypeStruct((EXPERTS, 2, 2, 2, ROW_CAP, cols), BF16),
            jax.ShapeDtypeStruct((8, d, f), BF16),
            jax.ShapeDtypeStruct((8, d, f), BF16),
            jax.ShapeDtypeStruct((8, f, d), BF16),
        ],
        scratch_shapes=[
            pltpu.VMEM((BLOCKS, tokens, d), BF16),
            pltpu.VMEM((BLOCKS,) + meta.shape, F32),
            pltpu.VMEM((BLOCKS, EXPERTS, tokens), F32),
            pltpu.VMEM((2, 4, 4, 4, EXPERTS, tokens), F32),
            pltpu.VMEM((2, 4, tokens, cols), F32),
            pltpu.VMEM((2, 2, half, cols), F32),
            pltpu.VMEM((2, 2, tokens, cols), F32),
            pltpu.VMEM((2, TILE, ROW_CAP, d), BF16),
            pltpu.VMEM((2, TILE, ROW_CAP, d), BF16),
            pltpu.VMEM((2, TILE * ROW_CAP, f), BF16),
            pltpu.VMEM((d, f), BF16),
            pltpu.VMEM((d, f), BF16),
            pltpu.VMEM((f, d), BF16),
            *both_ways(2, 5, 4), *both_ways(BLOCKS), *both_ways(2, 2, 3, 2), *both_ways(2, 3, 2), *both_ways(3, 2), *both_ways(6, 3),
            *both_ways(EXPERTS, 2, 2), *both_ways(EXPERTS, 2, 2), *both_ways(EXPERTS, 2, 2), *both_ways(2, 2), *both_ways(2, 2),
            dma((2,)), dma((2,)), dma((3,)), dma((2,)), dma((2, 4)),
        ],
        compiler_params=pltpu.CompilerParams(collective_id=0, has_side_effects=True, vmem_limit_bytes=63 * MIB),
        cost_estimate=pl.CostEstimate(flops=flops, bytes_accessed=400 * MIB, transcendentals=0),
        name='run_moe',
    )(hidden, meta, w_gate, w_up, w_down)[0]


def split3(g):
    a = lax.reduce_precision(g, 8, 7)
    b = lax.reduce_precision(g - a, 8, 7)
    return a, b, g - a - b


def solution(mesh):
    grid = Mesh(mesh.devices.reshape((mesh.shape['dp'],) + SIZES), ('dp',) + GRID)

    def body(hidden, route_idx, gate_weights, w_gate, w_up, w_down):
        meta = jnp.concatenate((route_idx.T.astype(F32),) + split3(gate_weights.T), axis=0)
        return run_moe(hidden, meta, w_gate[0], w_up[0], w_down[0])

    r = P(('dp',) + GRID, None)
    e = P(GRID, None, None)
    return jax.shard_map(body, mesh=grid, in_specs=(r, r, r, e, e, e), out_specs=r, check_vma=False)
```

```python
import jax
import jax.numpy as jnp
from jax import lax
from jax.experimental import pallas as pl
from jax.experimental.pallas import tpu as pltpu
from jax.sharding import Mesh, PartitionSpec as P

BF16 = jnp.bfloat16
F32 = jnp.float32
MESH = pl.DeviceIdType.MESH
GRID = ('z', 'y', 'x', 'c')
SIZES = (4, 4, 4, 2)
ROW_CAP = 64
EXPERTS = 8
BLOCKS = 16
TILE = 8
MIB = 1024 * 1024
scope = jax.named_scope


def expert_ids(place, x, c, line):
    dx = jnp.where((place == 2) | (place == 4), 3, 0) + jnp.where((place == 3) | (place == 5), 1, 0)
    dx += jnp.where(place >= 6, 2, 0)
    core = jnp.where(place == 0, c, 0) + jnp.where(place == 1, 1 - c, 0)
    core += jnp.where((place == 4) | (place == 5) | (place == 7), 1, 0)
    return line * EXPERTS + lax.rem(x + dx, 4) * 2 + core


def moe_kernel(hid, meta, wg, wu, wd, out, o_hbm, x_hbm, rows_in, relay, hg, hu, hd,
               tok, metas, slots, tabs, acc, rf2, rn2, stage, xt, hbuf, bg, bu, bd,
               tsend, trecv, msend, mrecv, isend, irecv, fsend, frecv, dsend, drecv, psend, precv,
               nrsend, nrrecv, frsend, frrecv, fwsend, fwrecv, f2send, f2recv, n2send, n2recv,
               lsem, ssem, wsem, xsem, csem):
    z, y, x, c = (lax.axis_index(a) for a in GRID)
    right, left = lax.rem(x + 1, 4), lax.rem(x + 3, 4)
    tokens, d = hid.shape
    half, cols = tokens // 2, d // 2
    rows = TILE * ROW_CAP
    own = (wg, wu, wd)
    held = (hg, hu, hd)
    partner = {'c': 1 - c}

    def remote(src, dst, send, recv, where):
        return pltpu.make_async_remote_copy(src_ref=src, dst_ref=dst, send_sem=send, recv_sem=recv, device_id=where, device_id_type=MESH)

    def along(dim, step):
        return {'z': lax.rem(z + (1 - dim) * step, 4), 'y': lax.rem(y + dim * step, 4)}

    def quarter(ref, m, lane, q, count=1):
        n = own[m].shape[0] // 4
        return ref.at[pl.ds(pl.multiple_of((2 * lane + q) * n, n), count * n), :]

    def line_copy(way, k, m, q, src):
        dst = held[m].at[2 + 2 * k + way]
        return remote(quarter(src, m, c, q), quarter(dst, m, c, q), isend.at[way, k, m, q], irecv.at[way, k, m, q], {'x': right if way == 0 else left})

    def far_copy(k, m, q):
        src, dst = held[m].at[2 + 2 * k + q], held[m].at[6 + k]
        return remote(quarter(src, m, c, q), quarter(dst, m, c, q), fsend.at[k, m, q], frecv.at[k, m, q], {'x': right if q == 0 else left})

    def hand_own(m, n):
        lane = 1 - c if n == 0 else c
        return remote(quarter(own[m], m, lane, 0, 2), quarter(held[m].at[c], m, lane, 0, 2), dsend.at[m, n], drecv.at[m, n], partner)

    def hand_on(slot, m):
        ref = quarter(held[m].at[slot], m, c, 0, 2)
        return remote(ref, ref, psend.at[slot - 2, m], precv.at[slot - 2, m], partner)

    def start_line(k, srcs):
        for n in (0, 1):
            for m in range(3):
                line_copy(0, k, m, n, srcs[m]).start()
                line_copy(1, k, m, 1 - n, srcs[m]).start()

    def place(k, a, b):
        return a * 4 + b if k == 0 else b * 4 + a

    def part(k, a, b, h=None):
        r = pl.ds(0, tokens) if h is None else pl.ds(h * half, half)
        return tok.at[place(k, a, b), r, pl.ds(k * cols, cols)]

    def first_copy(k, way):
        sems = tsend.at[k, 4, way], trecv.at[k, 4, way], along(k, 1 + 2 * (way % 2))
        if way < 2:
            return remote(part(k, 0, 0), part(k, 3 - 2 * way, 0), *sems)
        return remote(part(k, 7 - 2 * way, 0, way - 2), part(k, 2, 0, way - 2), *sems)

    def second_copy(k, a, way):
        sems = tsend.at[k, a, way], trecv.at[k, a, way], along(1 - k, 1 + 2 * (way % 2))
        if way < 2:
            return remote(part(k, a, 0), part(k, a, 3 - 2 * way), *sems)
        return remote(part(k, a, 7 - 2 * way, way - 2), part(k, a, 2, way - 2), *sems)

    def meta_copy(dz, dy):
        s = ((4 - dz) % 4) * 4 + (4 - dy) % 4
        return remote(metas.at[0], metas.at[s], msend.at[s], mrecv.at[s], {'z': lax.rem(z + dz, 4), 'y': lax.rem(y + dy, 4)})

    peers = [(dz, dy) for dz in range(4) for dy in range(4) if dz or dy]

    def spread(color, i, ring, m, n):
        if color == 0:
            return o_hbm.at[i, pl.ds(m, n), ring, :, pl.ds(0, cols)]
        return o_hbm.at[i, ring, pl.ds(m, n), :, pl.ds(cols, cols)]

    def near_rows(i, color, h):
        return remote(spread(color, i, 1 + 2 * h, 0, 4), rows_in.at[i, color, 2 - 2 * h], nrsend.at[i, color, h], nrrecv.at[i, color, h], along(1 - color, 1 + 2 * h))

    def far_rows(i, color, h):
        return remote(spread(color, i, 2, 2 * h, 2), relay.at[i, color, h], frsend.at[i, color, h], frrecv.at[i, color, h], along(1 - color, 1 + 2 * h))

    def pass_rows(i, color, h):
        return remote(relay.at[i, color, h], rows_in.at[i, color, 1, pl.ds(2 * h, 2)], fwsend.at[i, color, h], fwrecv.at[i, color, h], along(1 - color, 1 + 2 * h))

    def far_sum(color, h):
        return remote(acc.at[color, 2, pl.ds(h * half, half), :], rf2.at[color, h], f2send.at[color, h], f2recv.at[color, h], along(color, 1 + 2 * h))

    def near_sum(color, h):
        return remote(acc.at[color, 1 + 2 * h], rn2.at[color, h], n2send.at[color, h], n2recv.at[color, h], along(color, 1 + 2 * h))

    both = [(color, h) for color in (0, 1) for h in (0, 1)]

    own_tok = pltpu.make_async_copy(hid, tok.at[0], lsem.at[0])
    own_tok.start()
    own_meta = pltpu.make_async_copy(meta, metas.at[0], lsem.at[1])
    own_meta.start()

    barrier = pltpu.get_barrier_semaphore()
    for where in [partner, {'x': right}, {'x': left}] + [{'z': lax.rem(z + dz, 4), 'y': lax.rem(y + dy, 4)} for dz, dy in peers]:
        pl.semaphore_signal(barrier, inc=1, device_id=where, device_id_type=MESH)
    pl.semaphore_wait(barrier, 3 + len(peers))

    for n in (0, 1):
        for m in range(3):
            hand_own(m, n).start()

    @pl.when(c == 0)
    def _():
        start_line(0, own)

    own_tok.wait()
    for k in (0, 1):
        for way in (0, 1):
            first_copy(k, way).start()
            second_copy(k, 0, way).start()
    own_meta.wait()
    for dz, dy in peers:
        meta_copy(dz, dy).start()
    for m in range(3):
        hand_own(m, 0).wait_recv()

    @pl.when(c == 0)
    def _():
        start_line(1, [ref.at[1] for ref in held])

    @pl.when(c == 1)
    def _():
        start_line(0, [ref.at[0] for ref in held])
        start_line(1, own)

    for k in (0, 1):
        first_copy(k, 0).wait_recv()
        first_copy(k, 2).start()
        second_copy(k, 3, 0).start()
        second_copy(k, 3, 1).start()
        first_copy(k, 1).wait_recv()
        first_copy(k, 3).start()
        second_copy(k, 1, 0).start()
        second_copy(k, 1, 1).start()
    for k in (0, 1):
        for way in (0, 1):
            second_copy(k, 0, way).wait_recv()
            second_copy(k, 0, 2 + way).start()
    for k in (0, 1):
        first_copy(k, 2).wait_recv()
        first_copy(k, 3).wait_recv()
        second_copy(k, 2, 0).start()
        second_copy(k, 2, 1).start()

    for dz, dy in peers:
        meta_copy(dz, dy).wait_recv()
    order = lax.broadcasted_iota(jnp.int32, (EXPERTS, tokens), 0)
    earlier = lax.broadcasted_iota(jnp.int32, (tokens, tokens), 0) < lax.broadcasted_iota(jnp.int32, (tokens, tokens), 1)
    earlier = jnp.where(earlier, 1.0, 0.0).astype(BF16)

    def table(s, line, terms):
        mine = expert_ids(order, x, c, line).astype(F32)
        rec = metas[s]
        top = rec.shape[0] // 4
        sums = [jnp.zeros((EXPERTS, tokens), F32) for _ in range(1 + terms)]
        for k in range(top):
            hit = rec[k:k + 1, :] == mine
            sums[0] += jnp.where(hit, 1.0, 0.0)
            for p in range(1, 1 + terms):
                sums[p] += jnp.where(hit, rec[p * top + k:p * top + k + 1, :], 0.0)
        rank = jnp.dot(sums[0].astype(BF16), earlier, preferred_element_type=F32)
        return [jnp.where(sums[0] > 0.5, rank, -1.0)] + sums[1:]

    def own_table(s, carry):
        slots[s], = table(s, z * 4 + y, 0)
        return carry

    lax.fori_loop(0, BLOCKS, own_table, 0)

    def ring_table(n, carry):
        color, m, s = n // 16, lax.rem(n // 4, 4), lax.rem(n, 4)
        line = lax.rem(z + color * s, 4) * 4 + lax.rem(y + (1 - color) * s, 4)
        for p, t in enumerate(table((4 - 3 * color) * m, line, 3)):
            tabs[color, m, s, p] = t
        return carry

    def turn(a):
        for k in (0, 1):
            for way in (0, 1):
                second_copy(k, a, way).wait_recv()
                second_copy(k, a, 2 + way).start()

    turn(3)
    turn(1)
    turn(2)
    lax.fori_loop(0, 32, ring_table, 0)
    for a in range(4):
        for k in (0, 1):
            for way in (2, 3):
                second_copy(k, a, way).wait_recv()

    def x_store(s, b):
        return pltpu.make_async_copy(stage.at[b], x_hbm.at[:, s], ssem.at[b])

    lanes = lax.broadcasted_iota(jnp.int32, (ROW_CAP, tokens), 0).astype(F32)

    def gather(s, carry):
        b = lax.rem(s, 2)
        pick = jnp.concatenate([jnp.where(slots[s, pl.ds(e, 1), :] == lanes, 1.0, 0.0).astype(BF16) for e in range(EXPERTS)], axis=0)
        got = jnp.dot(pick, tok[s], preferred_element_type=F32).astype(BF16)

        @pl.when(s >= 2)
        def _():
            x_store(s, b).wait()

        stage[b] = got.reshape(EXPERTS, ROW_CAP, d)
        x_store(s, b).start()
        return carry

    lax.fori_loop(0, BLOCKS, gather, 0)
    acc[...] = jnp.zeros(acc.shape, F32)
    x_store(0, 0).wait()
    x_store(0, 1).wait()
    for k in (0, 1):
        for way in range(4):
            first_copy(k, way).wait_send()
            for a in range(4):
                second_copy(k, a, way).wait_send()

    def load(i, m, go):
        dst = (bg, bu, bd)[m]

        @pl.when(i == 0)
        def _():
            go(pltpu.make_async_copy(own[m], dst, wsem.at[m]))

        @pl.when(i == 1)
        def _():
            go(pltpu.make_async_copy(held[m].at[1 - c], dst, wsem.at[m]))

        @pl.when(i >= 2)
        def _():
            go(pltpu.make_async_copy(held[m].at[i], dst, wsem.at[m]))

    def line_arrived(k, ms):
        for m in ms:
            for way in (0, 1):
                for q in (way, 1 - way):
                    line_copy(way, k, m, q, held[m].at[k]).wait_recv()
                far_copy(k, m, way).start()
                hand_on(2 + 2 * k + way, m).start()

    def far_arrived(k, ms):
        for m in ms:
            far_copy(k, m, 0).wait_recv()
            far_copy(k, m, 1).wait_recv()
            hand_on(6 + k, m).start()

    def handed(i, ms):
        @pl.when(i == 1)
        def _():
            for m in ms:
                hand_own(m, 1).wait_recv()

        @pl.when(i >= 2)
        def _():
            for m in ms:
                hand_on(i, m).wait_recv()

    def x_load(i, t):
        return pltpu.make_async_copy(x_hbm.at[i, pl.ds(t * TILE, TILE)], xt.at[t], xsem.at[t])

    def o_store(i, t):
        return pltpu.make_async_copy(stage.at[t].reshape(2, 4, ROW_CAP, d), o_hbm.at[i, pl.ds(2 * t, 2)], ssem.at[t])

    def begin(cp):
        cp.start()

    def finish(cp):
        cp.wait()

    def relay_rows(i):
        for color, h in both:
            far_rows(i, color, h).wait_recv()
            pass_rows(i, color, h).start()

    def row_loads(i, color):
        at = pl.ds(8 * lax.rem(i, 2) + 4 * color, 4)
        srcs = [spread(color, i, 0, 0, 4)] + [rows_in.at[i, color, s] for s in range(3)]
        return [pltpu.make_async_copy(src, tok.at[at, pl.ds(s * ROW_CAP, ROW_CAP), pl.ds(0, cols)], csem.at[color, s]) for s, src in enumerate(srcs)]

    def combine(i):
        for color in (0, 1):
            with scope('rows_wait'):
                for h in (0, 1):
                    near_rows(i, color, h).wait_recv()
                    pass_rows(i, color, h).wait_recv()
            for cp in row_loads(i, color):
                cp.start()
        with scope('rowload_wait'):
            for color in (0, 1):
                for cp in row_loads(i, color):
                    cp.wait()

        def one(n, carry):
            j, color = n // 2, lax.rem(n, 2)
            m = lax.rem(2 + 3 * j + 3 * (j * (j - 1) // 2), 4)
            got = tok[8 * lax.rem(i, 2) + 4 * color + m, :, pl.ds(0, cols)]
            total = acc[color, m]
            for p in range(1, 4):
                g = jnp.concatenate([
                    jnp.where(tabs[color, m, s, 0, pl.ds(i, 1), :] == lanes, tabs[color, m, s, p, pl.ds(i, 1), :], 0.0).astype(BF16)
                    for s in range(4)], axis=0)
                total += lax.dot_general(g, got, (((0,), (0,)), ((), ())), preferred_element_type=F32)
            acc[color, m] = total
            for k in (0, 1):
                @pl.when((i == EXPERTS - 1) & (n == k))
                def _():
                    far_sum(k, 0).start()
                    far_sum(k, 1).start()
            return carry

        lax.fori_loop(0, 8, one, 0)

    def load_up(i):
        handed(i, (0, 1))
        load(i, 0, begin)
        load(i, 1, begin)

    def load_down(i):
        handed(i, (2,))
        load(i, 2, begin)

    def expert(i, carry):
        late = (i == 4) | (i == 6) | (i == 7)

        @pl.when(i < EXPERTS)
        def _():
            for t in (0, 1):
                x_load(i, t).start()

            @pl.when(jnp.logical_not(late))
            def _():
                load_down(i)

            @pl.when(i == 7)
            def _():
                with scope('far1_gu'):
                    far_arrived(1, (0, 1))

            @pl.when(late)
            def _():
                with scope('late_gu'):
                    load_up(i)

            with scope('load_gu'):
                load(i, 0, finish)
                load(i, 1, finish)

            def up(t, carry):
                x_load(i, t).wait()
                xs = xt[t].reshape(rows, d)
                a = jnp.dot(xs, bg[...], preferred_element_type=F32)
                u = jnp.dot(xs, bu[...], preferred_element_type=F32)
                hbuf[t] = (jax.nn.silu(a) * u).astype(BF16)
                return carry

            with scope('up'):
                lax.fori_loop(0, 2, up, 0)

            @pl.when((i < 3) | (i == 4))
            def _():
                with scope('next_gu'):
                    load_up(i + 1)

        @pl.when(i == 4)
        def _():
            with scope('line1_d'):
                line_arrived(1, (2,))

        for k in (0, 1):
            @pl.when(i == 6 + k)
            def _():
                with scope('far_d'):
                    far_arrived(k, (2,))

        @pl.when((i >= 1) & (i < EXPERTS))
        def _():
            with scope('relay'):
                relay_rows(i - 1)

        @pl.when(i >= 2)
        def _():
            with scope('combine'):
                combine(i - 2)

        @pl.when(i == EXPERTS)
        def _():
            with scope('relay'):
                relay_rows(i - 1)

        @pl.when(i == 3)
        def _():
            with scope('line1_gu'):
                line_arrived(1, (0, 1))

        @pl.when(i == 5)
        def _():
            with scope('far0_gu'):
                far_arrived(0, (0, 1))

        @pl.when(i < EXPERTS)
        def _():
            @pl.when(late)
            def _():
                with scope('late_d'):
                    load_down(i)

            with scope('load_d'):
                load(i, 2, finish)

            def down(t, carry):
                o = jnp.dot(hbuf[t], bd[...], preferred_element_type=F32).astype(BF16)
                stage[t] = o.reshape(TILE, ROW_CAP, d)
                o_store(i, t).start()
                return carry

            with scope('down'):
                lax.fori_loop(0, 2, down, 0)
                for t in (0, 1):
                    o_store(i, t).wait()
            for color, h in both:
                far_rows(i, color, h).start()
            for color, h in both:
                near_rows(i, color, h).start()

        return carry

    with scope('line0'):
        line_arrived(0, (0, 1, 2))
    load_up(0)
    lax.fori_loop(0, EXPERTS + 2, expert, 0)

    for color, h in both:
        with scope('farsum_wait'):
            far_sum(color, h).wait_recv()
        r = pl.ds(h * half, half)
        acc[color, 1 + 2 * h, r, :] = acc[color, 1 + 2 * h, r, :] + rf2[color, h]
        near_sum(color, h).start()
    for color in (0, 1):
        for h in (0, 1):
            with scope('nearsum_wait'):
                near_sum(color, h).wait_recv()
        out[:, color * cols:(color + 1) * cols] = (acc[color, 0] + rn2[color, 0] + rn2[color, 1]).astype(out.dtype)

    for color, h in both:
        far_sum(color, h).wait_send()
        near_sum(color, h).wait_send()

    def drain(i, carry):
        for color, h in both:
            near_rows(i, color, h).wait_send()
            far_rows(i, color, h).wait_send()
            pass_rows(i, color, h).wait_send()
        return carry

    lax.fori_loop(0, EXPERTS, drain, 0)
    for dz, dy in peers:
        meta_copy(dz, dy).wait_send()
    for m in range(3):
        for n in (0, 1):
            hand_own(m, n).wait_send()
            for k in (0, 1):
                far_copy(k, m, n).wait_send()
                for way in (0, 1):
                    line_copy(way, k, m, n, held[m].at[k]).wait_send()
        for slot in range(2, 8):
            hand_on(slot, m).wait_send()


def run_moe(hidden, meta, w_gate, w_up, w_down):
    tokens, d = hidden.shape
    f = w_gate.shape[1]
    half, cols = tokens // 2, d // 2
    hbm = pl.BlockSpec(memory_space=pl.ANY)
    dma = pltpu.SemaphoreType.DMA
    flops = 2 * EXPERTS * BLOCKS * ROW_CAP * d * (3 * f + 4 * tokens)

    def both_ways(*shape):
        return [dma(shape), dma(shape)]

    return pl.pallas_call(
        moe_kernel,
        in_specs=[hbm] * 5,
        out_specs=[pl.BlockSpec(memory_space=pltpu.VMEM)] + [hbm] * 7,
        out_shape=[
            jax.ShapeDtypeStruct((tokens, d), BF16),
            jax.ShapeDtypeStruct((EXPERTS, 4, 4, ROW_CAP, d), BF16),
            jax.ShapeDtypeStruct((EXPERTS, BLOCKS, ROW_CAP, d), BF16),
            jax.ShapeDtypeStruct((EXPERTS, 2, 3, 4, ROW_CAP, cols), BF16),
            jax.ShapeDtypeStruct((EXPERTS, 2, 2, 2, ROW_CAP, cols), BF16),
            jax.ShapeDtypeStruct((8, d, f), BF16),
            jax.ShapeDtypeStruct((8, d, f), BF16),
            jax.ShapeDtypeStruct((8, f, d), BF16),
        ],
        scratch_shapes=[
            pltpu.VMEM((BLOCKS, tokens, d), BF16),
            pltpu.VMEM((BLOCKS,) + meta.shape, F32),
            pltpu.VMEM((BLOCKS, EXPERTS, tokens), F32),
            pltpu.VMEM((2, 4, 4, 4, EXPERTS, tokens), F32),
            pltpu.VMEM((2, 4, tokens, cols), F32),
            pltpu.VMEM((2, 2, half, cols), F32),
            pltpu.VMEM((2, 2, tokens, cols), F32),
            pltpu.VMEM((2, TILE, ROW_CAP, d), BF16),
            pltpu.VMEM((2, TILE, ROW_CAP, d), BF16),
            pltpu.VMEM((2, TILE * ROW_CAP, f), BF16),
            pltpu.VMEM((d, f), BF16),
            pltpu.VMEM((d, f), BF16),
            pltpu.VMEM((f, d), BF16),
            *both_ways(2, 5, 4), *both_ways(BLOCKS), *both_ways(2, 2, 3, 2), *both_ways(2, 3, 2), *both_ways(3, 2), *both_ways(6, 3),
            *both_ways(EXPERTS, 2, 2), *both_ways(EXPERTS, 2, 2), *both_ways(EXPERTS, 2, 2), *both_ways(2, 2), *both_ways(2, 2),
            dma((2,)), dma((2,)), dma((3,)), dma((2,)), dma((2, 4)),
        ],
        compiler_params=pltpu.CompilerParams(collective_id=0, has_side_effects=True, vmem_limit_bytes=63 * MIB),
        cost_estimate=pl.CostEstimate(flops=flops, bytes_accessed=400 * MIB, transcendentals=0),
        name='run_moe',
    )(hidden, meta, w_gate, w_up, w_down)[0]


def split3(g):
    a = lax.reduce_precision(g, 8, 7)
    b = lax.reduce_precision(g - a, 8, 7)
    return a, b, g - a - b


def solution(mesh):
    grid = Mesh(mesh.devices.reshape((mesh.shape['dp'],) + SIZES), ('dp',) + GRID)

    def body(hidden, route_idx, gate_weights, w_gate, w_up, w_down):
        meta = jnp.concatenate((route_idx.T.astype(F32),) + split3(gate_weights.T), axis=0)
        return run_moe(hidden, meta, w_gate[0], w_up[0], w_down[0])

    r = P(('dp',) + GRID, None)
    e = P(GRID, None, None)
    return jax.shard_map(body, mesh=grid, in_specs=(r, r, r, e, e, e), out_specs=r, check_vma=False)
```

```python
import jax
import jax.numpy as jnp
from jax import lax
from jax.experimental import pallas as pl
from jax.experimental.pallas import tpu as pltpu
from jax.sharding import Mesh, PartitionSpec as P

BF16 = jnp.bfloat16
F32 = jnp.float32
MESH = pl.DeviceIdType.MESH
GRID = ('z', 'y', 'x', 'c')
SIZES = (4, 4, 4, 2)
ROW_CAP = 64
EXPERTS = 8
BLOCKS = 16
TILE = 8
MIB = 1024 * 1024
scope = jax.named_scope


def expert_ids(place, x, c, line):
    dx = jnp.where((place == 2) | (place == 4), 3, 0) + jnp.where((place == 3) | (place == 5), 1, 0)
    dx += jnp.where(place >= 6, 2, 0)
    core = jnp.where(place == 0, c, 0) + jnp.where(place == 1, 1 - c, 0)
    core += jnp.where((place == 4) | (place == 5) | (place == 7), 1, 0)
    return line * EXPERTS + lax.rem(x + dx, 4) * 2 + core


def moe_kernel(hid, ids, gates, wg, wu, wd, out, o_hbm, x_hbm, rows_in, relay, hg, hu, hd,
               tok, all_ids, all_gates, slots, tabs, acc, rf2, rn2, stage, xt, abuf, hbuf, bg, bu, bd,
               tsend, trecv, msend, mrecv, isend, irecv, fsend, frecv, dsend, drecv, psend, precv,
               nrsend, nrrecv, frsend, frrecv, fwsend, fwrecv, f2send, f2recv, n2send, n2recv,
               gsend, grecv, qsend, qrecv, lsem, ssem, osem, wsem, xsem, csem):
    z, y, x, c = (lax.axis_index(a) for a in GRID)
    right, left = lax.rem(x + 1, 4), lax.rem(x + 3, 4)
    tokens, d = hid.shape
    half, cols = tokens // 2, d // 2
    rows = TILE * ROW_CAP
    own = (wg, wu, wd)
    held = (hg, hu, hd)
    partner = {'c': 1 - c}

    def remote(src, dst, send, recv, where):
        return pltpu.make_async_remote_copy(src_ref=src, dst_ref=dst, send_sem=send, recv_sem=recv, device_id=where, device_id_type=MESH)

    def along(dim, step):
        return {'z': lax.rem(z + (1 - dim) * step, 4), 'y': lax.rem(y + dim * step, 4)}

    def quarter(ref, m, lane, q, count=1):
        n = own[m].shape[0] // 4
        return ref.at[pl.ds(pl.multiple_of((2 * lane + q) * n, n), count * n), :]

    def line_copy(way, k, m, q, src):
        dst = held[m].at[2 + 2 * k + way]
        return remote(quarter(src, m, c, q), quarter(dst, m, c, q), isend.at[way, k, m, q], irecv.at[way, k, m, q], {'x': right if way == 0 else left})

    def far_copy(k, m, q):
        src, dst = held[m].at[2 + 2 * k + q], held[m].at[6 + k]
        return remote(quarter(src, m, c, q), quarter(dst, m, c, q), fsend.at[k, m, q], frecv.at[k, m, q], {'x': right if q == 0 else left})

    def hand_own(m, n):
        lane = 1 - c if n == 0 else c
        return remote(quarter(own[m], m, lane, 0, 2), quarter(held[m].at[c], m, lane, 0, 2), dsend.at[m, n], drecv.at[m, n], partner)

    def hand_on(slot, m):
        ref = quarter(held[m].at[slot], m, c, 0, 2)
        return remote(ref, ref, psend.at[slot - 2, m], precv.at[slot - 2, m], partner)

    def start_line(k, srcs, skip=0):
        for n, m in [(n, m) for n in (0, 1) for m in range(3)][skip:]:
            line_copy(0, k, m, n, srcs[m]).start()
            line_copy(1, k, m, 1 - n, srcs[m]).start()

    def piece(color, part):
        return pl.ds(color * cols + part * (cols // 2), cols // 2)

    def piece_of(ref, lane, q, count, color, part):
        n = ref.shape[0] // 4
        return ref.at[pl.ds(pl.multiple_of((2 * lane + q) * n, n), count * n), piece(color, part)]

    def far_piece(q, part, color):
        src, dst = hd.at[4 + q], hd.at[7]
        return remote(piece_of(src, c, q, 1, color, part), piece_of(dst, c, q, 1, color, part), gsend.at[q, part, color], grecv.at[q, part, color], {'x': right if q == 0 else left})

    def hand_piece(part, color):
        ref = piece_of(hd.at[7], c, 0, 2, color, part)
        return remote(ref, ref, qsend.at[part, color], qrecv.at[part, color], partner)

    def place(k, a, b):
        return a * 4 + b if k == 0 else b * 4 + a

    def part(k, a, b, h=None):
        r = pl.ds(0, tokens) if h is None else pl.ds(h * half, half)
        return tok.at[place(k, a, b), r, pl.ds(k * cols, cols)]

    def first_copy(k, way):
        sems = tsend.at[k, 4, way], trecv.at[k, 4, way], along(k, 1 + 2 * (way % 2))
        if way < 2:
            return remote(part(k, 0, 0), part(k, 3 - 2 * way, 0), *sems)
        return remote(part(k, 7 - 2 * way, 0, way - 2), part(k, 2, 0, way - 2), *sems)

    def second_copy(k, a, way):
        sems = tsend.at[k, a, way], trecv.at[k, a, way], along(1 - k, 1 + 2 * (way % 2))
        if way < 2:
            return remote(part(k, a, 0), part(k, a, 3 - 2 * way), *sems)
        return remote(part(k, a, 7 - 2 * way, way - 2), part(k, a, 2, way - 2), *sems)

    def route_copies(dz, dy):
        s = ((4 - dz) % 4) * 4 + (4 - dy) % 4
        where = {'z': lax.rem(z + dz, 4), 'y': lax.rem(y + dy, 4)}
        return [remote(ref.at[0], ref.at[s], msend.at[n, s], mrecv.at[n, s], where) for n, ref in enumerate((all_ids, all_gates))]

    peers = [(dz, dy) for dz in range(4) for dy in range(4) if dz or dy]

    def spread(color, i, ring, m, n, part=None):
        w = pl.ds(color * cols, cols) if part is None else piece(color, part)
        if color == 0:
            return o_hbm.at[i, pl.ds(m, n), ring, :, w]
        return o_hbm.at[i, ring, pl.ds(m, n), :, w]

    def within(part):
        return pl.ds(0, cols) if part is None else pl.ds(part * (cols // 2), cols // 2)

    def row_sems(send, recv, i, part, color, h):
        n = i if part is None else i + part
        return send.at[n, color, h], recv.at[n, color, h], along(1 - color, 1 + 2 * h)

    def near_rows(i, color, h, part=None):
        return remote(spread(color, i, 1 + 2 * h, 0, 4, part), rows_in.at[i, color, 2 - 2 * h, :, :, within(part)], *row_sems(nrsend, nrrecv, i, part, color, h))

    def far_rows(i, color, h, part=None):
        return remote(spread(color, i, 2, 2 * h, 2, part), relay.at[i, color, h, :, :, within(part)], *row_sems(frsend, frrecv, i, part, color, h))

    def pass_rows(i, color, h, part=None):
        return remote(relay.at[i, color, h, :, :, within(part)], rows_in.at[i, color, 1, pl.ds(2 * h, 2), :, within(part)], *row_sems(fwsend, fwrecv, i, part, color, h))

    def far_sum(color, h, part):
        r, w = pl.ds(h * half, half), within(part)
        return remote(acc.at[color, 2, r, w], rf2.at[color, h, :, w], f2send.at[color, h, part], f2recv.at[color, h, part], along(color, 1 + 2 * h))

    def near_sum(color, h, waits, part):
        r, w = pl.ds((h if waits else 1 - h) * half, half), within(part)
        return remote(acc.at[color, 1 + 2 * h, r, w], rn2.at[color, h, r, w], n2send.at[color, h, waits, part], n2recv.at[color, h, waits, part], along(color, 1 + 2 * h))

    both = [(color, h) for color in (0, 1) for h in (0, 1)]

    own_tok = pltpu.make_async_copy(hid, tok.at[0], lsem.at[0])
    own_tok.start()
    own_routes = [pltpu.make_async_copy(ids, all_ids.at[0], lsem.at[1]), pltpu.make_async_copy(gates, all_gates.at[0], lsem.at[2])]
    for cp in own_routes:
        cp.start()

    barrier = pltpu.get_barrier_semaphore()
    for where in [partner, {'x': right}, {'x': left}] + [{'z': lax.rem(z + dz, 4), 'y': lax.rem(y + dy, 4)} for dz, dy in peers]:
        pl.semaphore_signal(barrier, inc=1, device_id=where, device_id_type=MESH)
    pl.semaphore_wait(barrier, 3 + len(peers))

    for n in (0, 1):
        for m in range(3):
            hand_own(m, n).start()

    @pl.when(c == 0)
    def _():
        start_line(0, own)

    @pl.when(c == 1)
    def _():
        line_copy(0, 1, 0, 0, own[0]).start()
        line_copy(1, 1, 0, 1, own[0]).start()

    own_tok.wait()
    for k in (0, 1):
        for way in (0, 1):
            first_copy(k, way).start()
            second_copy(k, 0, way).start()
    for cp in own_routes:
        cp.wait()
    for dz, dy in peers:
        for cp in route_copies(dz, dy):
            cp.start()
    for m in range(3):
        hand_own(m, 0).wait_recv()

    @pl.when(c == 0)
    def _():
        start_line(1, [ref.at[1] for ref in held])

    @pl.when(c == 1)
    def _():
        start_line(0, [ref.at[0] for ref in held])
        start_line(1, own, 1)

    for k in (0, 1):
        first_copy(k, 0).wait_recv()
        first_copy(k, 2).start()
        second_copy(k, 3, 0).start()
        second_copy(k, 3, 1).start()
        first_copy(k, 1).wait_recv()
        first_copy(k, 3).start()
        second_copy(k, 1, 0).start()
        second_copy(k, 1, 1).start()
    for k in (0, 1):
        for way in (0, 1):
            second_copy(k, 0, way).wait_recv()
            second_copy(k, 0, 2 + way).start()
    for k in (0, 1):
        first_copy(k, 2).wait_recv()
        first_copy(k, 3).wait_recv()
        second_copy(k, 2, 0).start()
        second_copy(k, 2, 1).start()

    for dz, dy in peers:
        for cp in route_copies(dz, dy):
            cp.wait_recv()
    order = lax.broadcasted_iota(jnp.int32, (EXPERTS, tokens), 0)
    earlier = lax.broadcasted_iota(jnp.int32, (tokens, tokens), 0) < lax.broadcasted_iota(jnp.int32, (tokens, tokens), 1)
    earlier = jnp.where(earlier, 1.0, 0.0).astype(BF16)

    def table(s, line):
        mine = expert_ids(order, x, c, line)
        rec, weight = all_ids[s], all_gates[s]
        chosen = jnp.zeros((EXPERTS, tokens), F32)
        gate = jnp.zeros((EXPERTS, tokens), F32)
        for k in range(rec.shape[0]):
            hit = rec[k:k + 1, :] == mine
            chosen += jnp.where(hit, 1.0, 0.0)
            gate += jnp.where(hit, weight[k:k + 1, :], 0.0)
        rank = jnp.dot(chosen.astype(BF16), earlier, preferred_element_type=F32)
        return jnp.where(chosen > 0.5, rank, -1.0), gate

    def own_table(s, carry):
        slots[s] = table(s, z * 4 + y)[0]
        return carry

    lax.fori_loop(0, BLOCKS, own_table, 0)

    def ring_table(n, carry):
        color, m, s = n // 16, lax.rem(n // 4, 4), lax.rem(n, 4)
        line = lax.rem(z + color * s, 4) * 4 + lax.rem(y + (1 - color) * s, 4)
        slot, gate = table((4 - 3 * color) * m, line)
        tabs[color, m, s, 0] = slot
        for p in range(1, 4):
            term = gate.astype(BF16).astype(F32)
            tabs[color, m, s, p] = term
            gate = gate - term
        return carry

    def turn(a):
        for k in (0, 1):
            for way in (0, 1):
                second_copy(k, a, way).wait_recv()
                second_copy(k, a, 2 + way).start()

    turn(3)
    turn(1)
    turn(2)
    lax.fori_loop(0, 32, ring_table, 0)
    for a in range(4):
        for k in (0, 1):
            for way in (2, 3):
                second_copy(k, a, way).wait_recv()

    def x_store(s, b):
        return pltpu.make_async_copy(stage.at[b].reshape(EXPERTS, ROW_CAP, d), x_hbm.at[:, s], ssem.at[b])

    lanes = lax.broadcasted_iota(jnp.int32, (ROW_CAP, tokens), 0).astype(F32)

    def gather(s, carry):
        b = lax.rem(s, 2)
        pick = jnp.concatenate([jnp.where(slots[s, pl.ds(e, 1), :] == lanes, 1.0, 0.0).astype(BF16) for e in range(EXPERTS)], axis=0)
        got = jnp.dot(pick, tok[s], preferred_element_type=F32).astype(BF16)

        @pl.when(s >= 2)
        def _():
            x_store(s, b).wait()

        stage[b] = got.reshape(2, 4, ROW_CAP, d)
        x_store(s, b).start()
        return carry

    lax.fori_loop(0, BLOCKS, gather, 0)
    acc[...] = jnp.zeros(acc.shape, F32)
    x_store(0, 0).wait()
    x_store(0, 1).wait()
    for k in (0, 1):
        for way in range(4):
            first_copy(k, way).wait_send()
            for a in range(4):
                second_copy(k, a, way).wait_send()

    def load(i, m, go):
        dst = (bg, bu, bd)[m]

        @pl.when(i == 0)
        def _():
            go(pltpu.make_async_copy(own[m], dst, wsem.at[m]))

        @pl.when(i == 1)
        def _():
            go(pltpu.make_async_copy(held[m].at[1 - c], dst, wsem.at[m]))

        @pl.when(i >= 2)
        def _():
            go(pltpu.make_async_copy(held[m].at[i], dst, wsem.at[m]))

    def line_arrived(k, ms):
        for m in ms:
            for way in (0, 1):
                for q in (way, 1 - way):
                    line_copy(way, k, m, q, held[m].at[k]).wait_recv()
                if (k, m) == (1, 2):
                    for part in (0, 1):
                        for color in (0, 1):
                            far_piece(way, part, color).start()
                else:
                    far_copy(k, m, way).start()
                hand_on(2 + 2 * k + way, m).start()

    def far_arrived(k, ms):
        for m in ms:
            far_copy(k, m, 0).wait_recv()
            far_copy(k, m, 1).wait_recv()
            hand_on(6 + k, m).start()

    def handed(i, ms):
        @pl.when(i == 1)
        def _():
            for m in ms:
                hand_own(m, 1).wait_recv()

        @pl.when(i >= 2)
        def _():
            for m in ms:
                hand_on(i, m).wait_recv()

    def x_load(i, t):
        return pltpu.make_async_copy(x_hbm.at[i, pl.ds(t * TILE, TILE)], xt.at[t], xsem.at[t])

    def o_store(i, t, w):
        n = 0 if w.size == d else w.start // cols
        return pltpu.make_async_copy(stage.at[t, :, :, :, w], o_hbm.at[i, pl.ds(2 * t, 2), :, :, w], osem.at[t, n])

    def begin(cp):
        cp.start()

    def finish(cp):
        cp.wait()

    def relay_rows(i, part=None):
        for color, h in both:
            far_rows(i, color, h, part).wait_recv()
            pass_rows(i, color, h, part).start()

    def row_loads(i, color, part):
        at = pl.ds(8 * lax.rem(i, 2) + 4 * color, 4)
        srcs = [spread(color, i, 0, 0, 4, part)] + [rows_in.at[i, color, s, :, :, within(part)] for s in range(3)]
        return [pltpu.make_async_copy(src, tok.at[at, pl.ds(s * ROW_CAP, ROW_CAP), within(part)], csem.at[color, s]) for s, src in enumerate(srcs)]

    def combine(i, part=None, then=None):
        for color in (0, 1):
            with scope('rows_wait'):
                for h in (0, 1):
                    near_rows(i, color, h, part).wait_recv()
                    pass_rows(i, color, h, part).wait_recv()
            for cp in row_loads(i, color, part):
                cp.start()
        with scope('rowload_wait'):
            for color in (0, 1):
                for cp in row_loads(i, color, part):
                    cp.wait()

        def one(n, carry):
            j, color = n // 2, lax.rem(n, 2)
            m = lax.rem(2 + 3 * j + 3 * (j * (j - 1) // 2), 4)
            got = tok[8 * lax.rem(i, 2) + 4 * color + m, :, within(part)]
            total = acc[color, m, :, within(part)]
            for p in range(1, 4):
                g = jnp.concatenate([
                    jnp.where(tabs[color, m, s, 0, pl.ds(i, 1), :] == lanes, tabs[color, m, s, p, pl.ds(i, 1), :], 0.0).astype(BF16)
                    for s in range(4)], axis=0)
                total += lax.dot_general(g, got, (((0,), (0,)), ((), ())), preferred_element_type=F32)
            acc[color, m, :, within(part)] = total
            if then is not None:
                then(j, color)
            return carry

        lax.fori_loop(0, 8, one, 0)

    def load_up(i):
        handed(i, (0, 1))
        load(i, 0, begin)
        load(i, 1, begin)

    def load_down(i):
        handed(i, (2,))
        load(i, 2, begin)

    def down(i, ws):
        def one(t, carry):
            for w in ws:
                o = jnp.dot(hbuf[t], bd[:, w], preferred_element_type=F32).astype(BF16)
                stage[t, :, :, :, w] = o.reshape(2, 4, ROW_CAP, o.shape[-1])
                o_store(i, t, w).start()
            return carry

        with scope('down'):
            lax.fori_loop(0, 2, one, 0)
            for t in (0, 1):
                for w in ws:
                    o_store(i, t, w).wait()

    def send(i, part=None):
        for color, h in both:
            far_rows(i, color, h, part).start()
        for color, h in both:
            near_rows(i, color, h, part).start()

    def expert(i, carry):
        late = (i == 4) | (i == 6)
        for t in (0, 1):
            x_load(i, t).start()

        @pl.when(jnp.logical_not(late))
        def _():
            load_down(i)

        @pl.when(late)
        def _():
            with scope('late_gu'):
                load_up(i)

        with scope('load_gu'):
            load(i, 0, finish)
            load(i, 1, finish)

        def up(t, carry):
            x_load(i, t).wait()
            xs = xt[t].reshape(rows, d)
            a = jnp.dot(xs, bg[...], preferred_element_type=F32)
            u = jnp.dot(xs, bu[...], preferred_element_type=F32)
            hbuf[t] = (jax.nn.silu(a) * u).astype(BF16)
            return carry

        with scope('up'):
            lax.fori_loop(0, 2, up, 0)

        @pl.when((i < 3) | (i == 4))
        def _():
            with scope('next_gu'):
                load_up(i + 1)

        @pl.when(i == 4)
        def _():
            with scope('line1_d'):
                line_arrived(1, (2,))

        @pl.when(i == 6)
        def _():
            with scope('far0_d'):
                far_arrived(0, (2,))

        @pl.when(i >= 1)
        def _():
            with scope('relay'):
                relay_rows(i - 1)

        @pl.when(i >= 2)
        def _():
            with scope('combine'):
                combine(i - 2)

        @pl.when(i == 3)
        def _():
            with scope('line1_gu'):
                line_arrived(1, (0, 1))

        @pl.when(i == 5)
        def _():
            with scope('far0_gu'):
                far_arrived(0, (0, 1))

        @pl.when(late)
        def _():
            with scope('late_d'):
                load_down(i)

        with scope('load_d'):
            load(i, 2, finish)
        down(i, [pl.ds(0, d)])
        send(i)
        return carry

    with scope('line0'):
        line_arrived(0, (0, 1, 2))
    load_up(0)
    lax.fori_loop(0, EXPERTS - 1, expert, 0)

    last = EXPERTS - 1
    for t in (0, 1):
        x_load(last, t).start()
    with scope('combine'):
        combine(last - 2)
    with scope('last_g'):
        far_arrived(1, (0,))
        hand_on(last, 0).wait_recv()
        g_load = pltpu.make_async_copy(hg.at[last], bg, wsem.at[0])
        g_load.start()
        g_load.wait()

    def gate_half(t, carry):
        x_load(last, t).wait()
        a = jnp.dot(xt[t].reshape(rows, d), bg[...], preferred_element_type=F32)
        abuf[t] = jax.nn.silu(a)
        return carry

    with scope('gate_half'):
        lax.fori_loop(0, 2, gate_half, 0)
    with scope('relay'):
        relay_rows(last - 1)
    with scope('last_u'):
        far_arrived(1, (1,))
        hand_on(last, 1).wait_recv()
        u_load = pltpu.make_async_copy(hu.at[last], bu, wsem.at[1])
        u_load.start()
        u_load.wait()

    def up_half(t, carry):
        u = jnp.dot(xt[t].reshape(rows, d), bu[...], preferred_element_type=F32)
        hbuf[t] = (abuf[t] * u).astype(BF16)
        return carry

    with scope('up_half'):
        lax.fori_loop(0, 2, up_half, 0)
    for part in (0, 1):
        with scope('last_d'):
            for color in (0, 1):
                for q in (0, 1):
                    far_piece(q, part, color).wait_recv()
                hand_piece(part, color).start()
            d_loads = []
            for color in (0, 1):
                hand_piece(part, color).wait_recv()
                d_loads.append(pltpu.make_async_copy(hd.at[last, :, piece(color, part)], bd.at[:, piece(color, part)], wsem.at[color]))
                d_loads[-1].start()
            for cp in d_loads:
                cp.wait()
        down(last, [piece(0, part), piece(1, part)])
        send(last, part)
    with scope('relay'):
        relay_rows(last, 0)
    with scope('combine'):
        combine(last - 1)
    with scope('relay'):
        relay_rows(last, 1)

    for part in (0, 1):
        def then(j, color):
            @pl.when(j == 0)
            def _():
                far_sum(color, 0, part).start()
                far_sum(color, 1, part).start()

            for h in (0, 1):
                @pl.when(j == 1 + h)
                def _():
                    near_sum(color, h, 0, part).start()

        with scope('combine'):
            combine(last, part, then)
    for part in (0, 1):
        for color, h in both:
            with scope('farsum_wait'):
                far_sum(color, h, part).wait_recv()
            r, w = pl.ds(h * half, half), within(part)
            acc[color, 1 + 2 * h, r, w] = acc[color, 1 + 2 * h, r, w] + rf2[color, h, :, w]
            near_sum(color, h, 1, part).start()
    for part in (0, 1):
        w = within(part)
        for color in (0, 1):
            with scope('nearsum_wait'):
                for h in (0, 1):
                    for waits in (0, 1):
                        near_sum(color, h, waits, part).wait_recv()
            out[:, piece(color, part)] = (acc[color, 0, :, w] + rn2[color, 0, :, w] + rn2[color, 1, :, w]).astype(out.dtype)

    for part in (0, 1):
        for color, h in both:
            far_sum(color, h, part).wait_send()
            near_sum(color, h, 0, part).wait_send()
            near_sum(color, h, 1, part).wait_send()
            near_rows(last, color, h, part).wait_send()
            far_rows(last, color, h, part).wait_send()
            pass_rows(last, color, h, part).wait_send()
            far_piece(h, part, color).wait_send()
        for color in (0, 1):
            hand_piece(part, color).wait_send()

    def drain(i, carry):
        for color, h in both:
            near_rows(i, color, h).wait_send()
            far_rows(i, color, h).wait_send()
            pass_rows(i, color, h).wait_send()
        return carry

    lax.fori_loop(0, EXPERTS - 1, drain, 0)
    for dz, dy in peers:
        for cp in route_copies(dz, dy):
            cp.wait_send()
    for m in range(3):
        for n in (0, 1):
            hand_own(m, n).wait_send()
            for k in (0, 1):
                if (k, m) != (1, 2):
                    far_copy(k, m, n).wait_send()
                for way in (0, 1):
                    line_copy(way, k, m, n, held[m].at[k]).wait_send()
        for slot in range(2, 8 if m < 2 else 7):
            hand_on(slot, m).wait_send()


def run_moe(hidden, ids, gates, w_gate, w_up, w_down):
    tokens, d = hidden.shape
    f = w_gate.shape[1]
    half, cols = tokens // 2, d // 2
    hbm = pl.BlockSpec(memory_space=pl.ANY)
    dma = pltpu.SemaphoreType.DMA
    flops = 2 * EXPERTS * BLOCKS * ROW_CAP * d * (3 * f + 4 * tokens)

    def both_ways(*shape):
        return [dma(shape), dma(shape)]

    return pl.pallas_call(
        moe_kernel,
        in_specs=[hbm] * 6,
        out_specs=[pl.BlockSpec(memory_space=pltpu.VMEM)] + [hbm] * 7,
        out_shape=[
            jax.ShapeDtypeStruct((tokens, d), BF16),
            jax.ShapeDtypeStruct((EXPERTS, 4, 4, ROW_CAP, d), BF16),
            jax.ShapeDtypeStruct((EXPERTS, BLOCKS, ROW_CAP, d), BF16),
            jax.ShapeDtypeStruct((EXPERTS, 2, 3, 4, ROW_CAP, cols), BF16),
            jax.ShapeDtypeStruct((EXPERTS, 2, 2, 2, ROW_CAP, cols), BF16),
            jax.ShapeDtypeStruct((8, d, f), BF16),
            jax.ShapeDtypeStruct((8, d, f), BF16),
            jax.ShapeDtypeStruct((8, f, d), BF16),
        ],
        scratch_shapes=[
            pltpu.VMEM((BLOCKS, tokens, d), BF16),
            pltpu.VMEM((BLOCKS,) + ids.shape, jnp.int32),
            pltpu.VMEM((BLOCKS,) + gates.shape, F32),
            pltpu.VMEM((BLOCKS, EXPERTS, tokens), F32),
            pltpu.VMEM((2, 4, 4, 4, EXPERTS, tokens), F32),
            pltpu.VMEM((2, 4, tokens, cols), F32),
            pltpu.VMEM((2, 2, half, cols), F32),
            pltpu.VMEM((2, 2, tokens, cols), F32),
            pltpu.VMEM((2, 2, 4, ROW_CAP, d), BF16),
            pltpu.VMEM((2, TILE, ROW_CAP, d), BF16),
            pltpu.VMEM((2, TILE * ROW_CAP, f), F32),
            pltpu.VMEM((2, TILE * ROW_CAP, f), BF16),
            pltpu.VMEM((d, f), BF16),
            pltpu.VMEM((d, f), BF16),
            pltpu.VMEM((f, d), BF16),
            *both_ways(2, 5, 4), *both_ways(2, BLOCKS), *both_ways(2, 2, 3, 2), *both_ways(2, 3, 2), *both_ways(3, 2), *both_ways(6, 3),
            *both_ways(EXPERTS + 1, 2, 2), *both_ways(EXPERTS + 1, 2, 2), *both_ways(EXPERTS + 1, 2, 2), *both_ways(2, 2, 2), *both_ways(2, 2, 2, 2),
            *both_ways(2, 2, 2), *both_ways(2, 2), dma((3,)), dma((2,)), dma((2, 2)), dma((3,)), dma((2,)), dma((2, 4)),
        ],
        compiler_params=pltpu.CompilerParams(collective_id=0, has_side_effects=True, vmem_limit_bytes=63 * MIB),
        cost_estimate=pl.CostEstimate(flops=flops, bytes_accessed=400 * MIB, transcendentals=0),
        name='run_moe',
    )(hidden, ids, gates, w_gate, w_up, w_down)[0]


def solution(mesh):
    grid = Mesh(mesh.devices.reshape((mesh.shape['dp'],) + SIZES), ('dp',) + GRID)

    def body(hidden, route_idx, gate_weights, w_gate, w_up, w_down):
        return run_moe(hidden, route_idx.T, gate_weights.T, w_gate[0], w_up[0], w_down[0])

    r = P(('dp',) + GRID, None)
    e = P(GRID, None, None)
    return jax.shard_map(body, mesh=grid, in_specs=(r, r, r, e, e, e), out_specs=r, check_vma=False)
```

```python
import jax
import jax.numpy as jnp
from jax import lax
from jax.experimental import pallas as pl
from jax.experimental.pallas import tpu as pltpu
from jax.sharding import Mesh, PartitionSpec as P

BF16 = jnp.bfloat16
F32 = jnp.float32
MESH = pl.DeviceIdType.MESH
GRID = ('z', 'y', 'x', 'c')
SIZES = (4, 4, 4, 2)
ROW_CAP = 64
EXPERTS = 8
BLOCKS = 16
TILE = 8
PARTS = 4
SUMS = 2
UPS = 2
MIB = 1024 * 1024
scope = jax.named_scope


def expert_ids(place, x, c, line):
    dx = jnp.where((place == 2) | (place == 4), 3, 0) + jnp.where((place == 3) | (place == 5), 1, 0)
    dx += jnp.where(place >= 6, 2, 0)
    core = jnp.where(place == 0, c, 0) + jnp.where(place == 1, 1 - c, 0)
    core += jnp.where((place == 4) | (place == 5) | (place == 7), 1, 0)
    return line * EXPERTS + lax.rem(x + dx, 4) * 2 + core


def moe_kernel(hid, ids, gates, wg, wu, wd, out, o_hbm, x_hbm, rows_in, relay, hg, hu, hd,
               tok, all_ids, all_gates, slots, tabs, acc, rf2, rn2, stage, xt, abuf, hbuf, bg, bu, bd,
               tsend, trecv, msend, mrecv, isend, irecv, fsend, frecv, dsend, drecv, psend, precv,
               nrsend, nrrecv, frsend, frrecv, fwsend, fwrecv, f2send, f2recv, n2send, n2recv,
               gsend, grecv, qsend, qrecv, usend, urecv, vsend, vrecv, lsem, ssem, osem, wsem, xsem, csem):
    z, y, x, c = (lax.axis_index(a) for a in GRID)
    right, left = lax.rem(x + 1, 4), lax.rem(x + 3, 4)
    tokens, d = hid.shape
    half, cols = tokens // 2, d // 2
    rows = TILE * ROW_CAP
    own = (wg, wu, wd)
    held = (hg, hu, hd)
    partner = {'c': 1 - c}

    def remote(src, dst, send, recv, where):
        return pltpu.make_async_remote_copy(src_ref=src, dst_ref=dst, send_sem=send, recv_sem=recv, device_id=where, device_id_type=MESH)

    def along(dim, step):
        return {'z': lax.rem(z + (1 - dim) * step, 4), 'y': lax.rem(y + dim * step, 4)}

    def quarter(ref, m, lane, q, count=1):
        n = own[m].shape[0] // 4
        return ref.at[pl.ds(pl.multiple_of((2 * lane + q) * n, n), count * n), :]

    def line_copy(way, k, m, q, src):
        dst = held[m].at[2 + 2 * k + way]
        return remote(quarter(src, m, c, q), quarter(dst, m, c, q), isend.at[way, k, m, q], irecv.at[way, k, m, q], {'x': right if way == 0 else left})

    def far_copy(k, m, q):
        src, dst = held[m].at[2 + 2 * k + q], held[m].at[6 + k]
        return remote(quarter(src, m, c, q), quarter(dst, m, c, q), fsend.at[k, m, q], frecv.at[k, m, q], {'x': right if q == 0 else left})

    def hand_own(m, n):
        lane = 1 - c if n == 0 else c
        return remote(quarter(own[m], m, lane, 0, 2), quarter(held[m].at[c], m, lane, 0, 2), dsend.at[m, n], drecv.at[m, n], partner)

    def hand_on(slot, m):
        ref = quarter(held[m].at[slot], m, c, 0, 2)
        return remote(ref, ref, psend.at[slot - 2, m], precv.at[slot - 2, m], partner)

    def start_line(k, srcs, skip=0):
        for n, m in [(n, m) for n in (0, 1) for m in range(3)][skip:]:
            line_copy(0, k, m, n, srcs[m]).start()
            line_copy(1, k, m, 1 - n, srcs[m]).start()

    def piece(color, part):
        return pl.ds(color * cols + part * (cols // PARTS), cols // PARTS)

    def piece_of(ref, lane, q, count, color, part):
        n = ref.shape[0] // 4
        return ref.at[pl.ds(pl.multiple_of((2 * lane + q) * n, n), count * n), piece(color, part)]

    def far_piece(q, part, color):
        src, dst = hd.at[4 + q], hd.at[7]
        return remote(piece_of(src, c, q, 1, color, part), piece_of(dst, c, q, 1, color, part), gsend.at[q, part, color], grecv.at[q, part, color], {'x': right if q == 0 else left})

    def hand_piece(part, color):
        ref = piece_of(hd.at[7], c, 0, 2, color, part)
        return remote(ref, ref, qsend.at[part, color], qrecv.at[part, color], partner)

    def strip(part):
        n = wu.shape[1] // UPS
        return pl.ds(part * n, n)

    def strip_of(ref, lane, q, count, part):
        n = ref.shape[0] // 4
        return ref.at[pl.ds(pl.multiple_of((2 * lane + q) * n, n), count * n), strip(part)]

    def far_strip(q, part):
        return remote(strip_of(hu.at[4 + q], c, q, 1, part), strip_of(hu.at[7], c, q, 1, part), usend.at[q, part], urecv.at[q, part], {'x': right if q == 0 else left})

    def hand_strip(part):
        ref = strip_of(hu.at[7], c, 0, 2, part)
        return remote(ref, ref, vsend.at[part], vrecv.at[part], partner)

    def place(k, a, b):
        return a * 4 + b if k == 0 else b * 4 + a

    def part(k, a, b, h=None):
        r = pl.ds(0, tokens) if h is None else pl.ds(h * half, half)
        return tok.at[place(k, a, b), r, pl.ds(k * cols, cols)]

    def first_copy(k, way):
        sems = tsend.at[k, 4, way], trecv.at[k, 4, way], along(k, 1 + 2 * (way % 2))
        if way < 2:
            return remote(part(k, 0, 0), part(k, 3 - 2 * way, 0), *sems)
        return remote(part(k, 7 - 2 * way, 0, way - 2), part(k, 2, 0, way - 2), *sems)

    def second_copy(k, a, way):
        sems = tsend.at[k, a, way], trecv.at[k, a, way], along(1 - k, 1 + 2 * (way % 2))
        if way < 2:
            return remote(part(k, a, 0), part(k, a, 3 - 2 * way), *sems)
        return remote(part(k, a, 7 - 2 * way, way - 2), part(k, a, 2, way - 2), *sems)

    def route_copies(dz, dy):
        s = ((4 - dz) % 4) * 4 + (4 - dy) % 4
        where = {'z': lax.rem(z + dz, 4), 'y': lax.rem(y + dy, 4)}
        return [remote(ref.at[0], ref.at[s], msend.at[n, s], mrecv.at[n, s], where) for n, ref in enumerate((all_ids, all_gates))]

    peers = [(dz, dy) for dz in range(4) for dy in range(4) if dz or dy]

    def spread(color, i, ring, m, n, part=None):
        w = pl.ds(color * cols, cols) if part is None else piece(color, part)
        if color == 0:
            return o_hbm.at[i, pl.ds(m, n), ring, :, w]
        return o_hbm.at[i, ring, pl.ds(m, n), :, w]

    def within(part, parts=PARTS):
        return pl.ds(0, cols) if part is None else pl.ds(part * (cols // parts), cols // parts)

    def row_sems(send, recv, i, part, color, h):
        n = i if part is None else i + part
        return send.at[n, color, h], recv.at[n, color, h], along(1 - color, 1 + 2 * h)

    def near_rows(i, color, h, part=None):
        return remote(spread(color, i, 1 + 2 * h, 0, 4, part), rows_in.at[i, color, 2 - 2 * h, :, :, within(part)], *row_sems(nrsend, nrrecv, i, part, color, h))

    def far_rows(i, color, h, part=None):
        return remote(spread(color, i, 2, 2 * h, 2, part), relay.at[i, color, h, :, :, within(part)], *row_sems(frsend, frrecv, i, part, color, h))

    def pass_rows(i, color, h, part=None):
        return remote(relay.at[i, color, h, :, :, within(part)], rows_in.at[i, color, 1, pl.ds(2 * h, 2), :, within(part)], *row_sems(fwsend, fwrecv, i, part, color, h))

    def far_sum(color, h, part):
        r, w = pl.ds(h * half, half), within(part, SUMS)
        return remote(acc.at[color, 2, r, w], rf2.at[color, h, :, w], f2send.at[color, h, part], f2recv.at[color, h, part], along(color, 1 + 2 * h))

    def near_sum(color, h, waits, part):
        r, w = pl.ds((h if waits else 1 - h) * half, half), within(part, SUMS)
        return remote(acc.at[color, 1 + 2 * h, r, w], rn2.at[color, h, r, w], n2send.at[color, h, waits, part], n2recv.at[color, h, waits, part], along(color, 1 + 2 * h))

    both = [(color, h) for color in (0, 1) for h in (0, 1)]

    own_tok = pltpu.make_async_copy(hid, tok.at[0], lsem.at[0])
    own_tok.start()
    own_routes = [pltpu.make_async_copy(ids, all_ids.at[0], lsem.at[1]), pltpu.make_async_copy(gates, all_gates.at[0], lsem.at[2])]
    for cp in own_routes:
        cp.start()

    barrier = pltpu.get_barrier_semaphore()
    for where in [partner, {'x': right}, {'x': left}] + [{'z': lax.rem(z + dz, 4), 'y': lax.rem(y + dy, 4)} for dz, dy in peers]:
        pl.semaphore_signal(barrier, inc=1, device_id=where, device_id_type=MESH)
    pl.semaphore_wait(barrier, 3 + len(peers))

    for n in (0, 1):
        for m in range(3):
            hand_own(m, n).start()

    @pl.when(c == 0)
    def _():
        start_line(0, own)

    @pl.when(c == 1)
    def _():
        line_copy(0, 1, 0, 0, own[0]).start()
        line_copy(1, 1, 0, 1, own[0]).start()

    own_tok.wait()
    for k in (0, 1):
        for way in (0, 1):
            first_copy(k, way).start()
            second_copy(k, 0, way).start()
    for cp in own_routes:
        cp.wait()
    for dz, dy in peers:
        for cp in route_copies(dz, dy):
            cp.start()
    for m in range(3):
        hand_own(m, 0).wait_recv()

    @pl.when(c == 0)
    def _():
        start_line(1, [ref.at[1] for ref in held])

    @pl.when(c == 1)
    def _():
        start_line(0, [ref.at[0] for ref in held])
        start_line(1, own, 1)

    for k in (0, 1):
        first_copy(k, 0).wait_recv()
        first_copy(k, 2).start()
        second_copy(k, 3, 0).start()
        second_copy(k, 3, 1).start()
        first_copy(k, 1).wait_recv()
        first_copy(k, 3).start()
        second_copy(k, 1, 0).start()
        second_copy(k, 1, 1).start()
    for k in (0, 1):
        for way in (0, 1):
            second_copy(k, 0, way).wait_recv()
            second_copy(k, 0, 2 + way).start()
    for k in (0, 1):
        first_copy(k, 2).wait_recv()
        first_copy(k, 3).wait_recv()
        second_copy(k, 2, 0).start()
        second_copy(k, 2, 1).start()

    for dz, dy in peers:
        for cp in route_copies(dz, dy):
            cp.wait_recv()
    order = lax.broadcasted_iota(jnp.int32, (EXPERTS, tokens), 0)
    earlier = lax.broadcasted_iota(jnp.int32, (tokens, tokens), 0) < lax.broadcasted_iota(jnp.int32, (tokens, tokens), 1)
    earlier = jnp.where(earlier, 1.0, 0.0).astype(BF16)

    def table(s, line):
        mine = expert_ids(order, x, c, line)
        rec, weight = all_ids[s], all_gates[s]
        chosen = jnp.zeros((EXPERTS, tokens), F32)
        gate = jnp.zeros((EXPERTS, tokens), F32)
        for k in range(rec.shape[0]):
            hit = rec[k:k + 1, :] == mine
            chosen += jnp.where(hit, 1.0, 0.0)
            gate += jnp.where(hit, weight[k:k + 1, :], 0.0)
        rank = jnp.dot(chosen.astype(BF16), earlier, preferred_element_type=F32)
        return jnp.where(chosen > 0.5, rank, -1.0), gate

    def own_table(s, carry):
        slots[s] = table(s, z * 4 + y)[0]
        return carry

    lax.fori_loop(0, BLOCKS, own_table, 0)

    def ring_table(n, carry):
        color, m, s = n // 16, lax.rem(n // 4, 4), lax.rem(n, 4)
        line = lax.rem(z + color * s, 4) * 4 + lax.rem(y + (1 - color) * s, 4)
        slot, gate = table((4 - 3 * color) * m, line)
        tabs[color, m, s, 0] = slot
        for p in range(1, 4):
            term = gate.astype(BF16).astype(F32)
            tabs[color, m, s, p] = term
            gate = gate - term
        return carry

    def turn(a):
        for k in (0, 1):
            for way in (0, 1):
                second_copy(k, a, way).wait_recv()
                second_copy(k, a, 2 + way).start()

    turn(3)
    turn(1)
    turn(2)
    lax.fori_loop(0, 32, ring_table, 0)
    for a in range(4):
        for k in (0, 1):
            for way in (2, 3):
                second_copy(k, a, way).wait_recv()

    def x_store(s, b):
        return pltpu.make_async_copy(stage.at[b].reshape(EXPERTS, ROW_CAP, d), x_hbm.at[:, s], ssem.at[b])

    lanes = lax.broadcasted_iota(jnp.int32, (ROW_CAP, tokens), 0).astype(F32)

    def gather(s, carry):
        b = lax.rem(s, 2)
        pick = jnp.concatenate([jnp.where(slots[s, pl.ds(e, 1), :] == lanes, 1.0, 0.0).astype(BF16) for e in range(EXPERTS)], axis=0)
        got = jnp.dot(pick, tok[s], preferred_element_type=F32).astype(BF16)

        @pl.when(s >= 2)
        def _():
            x_store(s, b).wait()

        stage[b] = got.reshape(2, 4, ROW_CAP, d)
        x_store(s, b).start()
        return carry

    lax.fori_loop(0, BLOCKS, gather, 0)
    acc[...] = jnp.zeros(acc.shape, F32)
    x_store(0, 0).wait()
    x_store(0, 1).wait()
    for k in (0, 1):
        for way in range(4):
            first_copy(k, way).wait_send()
            for a in range(4):
                second_copy(k, a, way).wait_send()

    def load(i, m, go):
        dst = (bg, bu, bd)[m]

        @pl.when(i == 0)
        def _():
            go(pltpu.make_async_copy(own[m], dst, wsem.at[m]))

        @pl.when(i == 1)
        def _():
            go(pltpu.make_async_copy(held[m].at[1 - c], dst, wsem.at[m]))

        @pl.when(i >= 2)
        def _():
            go(pltpu.make_async_copy(held[m].at[i], dst, wsem.at[m]))

    def line_arrived(k, ms):
        for m in ms:
            for way in (0, 1):
                for q in (way, 1 - way):
                    line_copy(way, k, m, q, held[m].at[k]).wait_recv()
                if (k, m) == (1, 1):
                    for part in range(UPS):
                        far_strip(way, part).start()
                elif (k, m) == (1, 2):
                    for part in range(PARTS):
                        for color in (0, 1):
                            far_piece(way, part, color).start()
                else:
                    far_copy(k, m, way).start()
                hand_on(2 + 2 * k + way, m).start()

    def far_arrived(k, ms):
        for m in ms:
            far_copy(k, m, 0).wait_recv()
            far_copy(k, m, 1).wait_recv()
            hand_on(6 + k, m).start()

    def handed(i, ms):
        @pl.when(i == 1)
        def _():
            for m in ms:
                hand_own(m, 1).wait_recv()

        @pl.when(i >= 2)
        def _():
            for m in ms:
                hand_on(i, m).wait_recv()

    def x_load(i, t):
        return pltpu.make_async_copy(x_hbm.at[i, pl.ds(t * TILE, TILE)], xt.at[t], xsem.at[t])

    def o_store(i, t, w):
        n = 0 if w.size == d else w.start // cols
        return pltpu.make_async_copy(stage.at[t, :, :, :, w], o_hbm.at[i, pl.ds(2 * t, 2), :, :, w], osem.at[t, n])

    def begin(cp):
        cp.start()

    def finish(cp):
        cp.wait()

    def relay_rows(i, part=None):
        for color, h in both:
            far_rows(i, color, h, part).wait_recv()
            pass_rows(i, color, h, part).start()

    def row_loads(i, color, w):
        at = pl.ds(8 * lax.rem(i, 2) + 4 * color, 4)
        here = pl.ds(color * cols + w.start, w.size)
        srcs = [o_hbm.at[i, :, 0, :, here] if color == 0 else o_hbm.at[i, 0, :, :, here]] + [rows_in.at[i, color, s, :, :, w] for s in range(3)]
        return [pltpu.make_async_copy(src, tok.at[at, pl.ds(s * ROW_CAP, ROW_CAP), w], csem.at[color, s]) for s, src in enumerate(srcs)]

    def fetch_rows(i, w, parts=(None,)):
        for color in (0, 1):
            with scope('rows_wait'):
                for part in parts:
                    for h in (0, 1):
                        near_rows(i, color, h, part).wait_recv()
                        pass_rows(i, color, h, part).wait_recv()
            for cp in row_loads(i, color, w):
                cp.start()

    def await_rows(i, w):
        with scope('rowload_wait'):
            for color in (0, 1):
                for cp in row_loads(i, color, w):
                    cp.wait()

    def add_rows(i, w, start=0, stop=8, then=None):
        def one(n, carry):
            j, color = n // 2, lax.rem(n, 2)
            m = lax.rem(2 + 3 * j + 3 * (j * (j - 1) // 2), 4)
            got = tok[8 * lax.rem(i, 2) + 4 * color + m, :, w]
            total = acc[color, m, :, w]
            for p in range(1, 4):
                g = jnp.concatenate([
                    jnp.where(tabs[color, m, s, 0, pl.ds(i, 1), :] == lanes, tabs[color, m, s, p, pl.ds(i, 1), :], 0.0).astype(BF16)
                    for s in range(4)], axis=0)
                total += lax.dot_general(g, got, (((0,), (0,)), ((), ())), preferred_element_type=F32)
            acc[color, m, :, w] = total
            if then is not None:
                then(j, color)
            return carry

        lax.fori_loop(start, stop, one, 0)

    def combine(i, w, parts=(None,), then=None):
        fetch_rows(i, w, parts)
        await_rows(i, w)
        add_rows(i, w, then=then)

    def load_up(i):
        handed(i, (0, 1))
        load(i, 0, begin)
        load(i, 1, begin)

    def load_down(i):
        handed(i, (2,))
        load(i, 2, begin)

    def down(i, ws):
        def one(t, carry):
            for w in ws:
                o = jnp.dot(hbuf[t], bd[:, w], preferred_element_type=F32).astype(BF16)
                stage[t, :, :, :, w] = o.reshape(2, 4, ROW_CAP, o.shape[-1])
                o_store(i, t, w).start()
            return carry

        with scope('down'):
            lax.fori_loop(0, 2, one, 0)
            for t in (0, 1):
                for w in ws:
                    o_store(i, t, w).wait()

    def send(i, part=None):
        for color, h in both:
            far_rows(i, color, h, part).start()
        for color, h in both:
            near_rows(i, color, h, part).start()

    def expert(i, carry):
        late = (i == 4) | (i == 6)
        for t in (0, 1):
            x_load(i, t).start()

        @pl.when(jnp.logical_not(late))
        def _():
            load_down(i)

        @pl.when(late)
        def _():
            with scope('late_gu'):
                load_up(i)

        with scope('load_gu'):
            load(i, 0, finish)
            load(i, 1, finish)

        def up(t, carry):
            x_load(i, t).wait()
            xs = xt[t].reshape(rows, d)
            a = jnp.dot(xs, bg[...], preferred_element_type=F32)
            u = jnp.dot(xs, bu[...], preferred_element_type=F32)
            hbuf[t] = (jax.nn.silu(a) * u).astype(BF16)
            return carry

        with scope('up'):
            lax.fori_loop(0, 2, up, 0)

        @pl.when((i < 3) | (i == 4))
        def _():
            with scope('next_gu'):
                load_up(i + 1)

        @pl.when(i == 4)
        def _():
            with scope('line1_d'):
                line_arrived(1, (2,))

        @pl.when(i == 6)
        def _():
            with scope('far0_d'):
                far_arrived(0, (2,))

        @pl.when(i >= 1)
        def _():
            with scope('relay'):
                relay_rows(i - 1)

        @pl.when(i >= 2)
        def _():
            with scope('combine'):
                combine(i - 2, within(None))

        @pl.when(i == 3)
        def _():
            with scope('line1_gu'):
                line_arrived(1, (0, 1))

        @pl.when(i == 5)
        def _():
            with scope('far0_gu'):
                far_arrived(0, (0, 1))

        @pl.when(late)
        def _():
            with scope('late_d'):
                load_down(i)

        with scope('load_d'):
            load(i, 2, finish)
        down(i, [pl.ds(0, d)])
        send(i)
        return carry

    with scope('line0'):
        line_arrived(0, (0, 1, 2))
    load_up(0)
    lax.fori_loop(0, EXPERTS - 1, expert, 0)

    last = EXPERTS - 1
    for t in (0, 1):
        x_load(last, t).start()
    def strip_arrived(part):
        far_strip(0, part).wait_recv()
        far_strip(1, part).wait_recv()
        hand_strip(part).start()

    with scope('last_g'):
        far_arrived(1, (0,))
    with scope('combine'):
        combine(last - 2, within(None))
    with scope('last_g'):
        hand_on(last, 0).wait_recv()
        g_load = pltpu.make_async_copy(hg.at[last], bg, wsem.at[0])
        g_load.start()
        strip_arrived(0)
        g_load.wait()

    def gate_half(t, carry):
        x_load(last, t).wait()
        a = jnp.dot(xt[t].reshape(rows, d), bg[...], preferred_element_type=F32)
        abuf[t] = jax.nn.silu(a)
        return carry

    with scope('gate_half'):
        lax.fori_loop(0, 2, gate_half, 0)
    with scope('relay'):
        relay_rows(last - 1)
    def piece_arrived(part):
        for color in (0, 1):
            for q in (0, 1):
                far_piece(q, part, color).wait_recv()
            hand_piece(part, color).start()

    for part in range(UPS):
        with scope('last_u'):
            hand_strip(part).wait_recv()
            u_load = pltpu.make_async_copy(hu.at[last, :, strip(part)], bu.at[:, strip(part)], wsem.at[1])
            u_load.start()
            u_load.wait()
        if part + 1 == UPS:
            with scope('piece'):
                piece_arrived(0)

        def up_half(t, carry):
            u = jnp.dot(xt[t].reshape(rows, d), bu[:, strip(part)], preferred_element_type=F32)
            hbuf[t, :, strip(part)] = (abuf[t, :, strip(part)] * u).astype(BF16)
            return carry

        with scope('up_half'):
            lax.fori_loop(0, 2, up_half, 0)
        if part + 1 < UPS:
            with scope('strip'):
                strip_arrived(part + 1)

    every = within(None)
    first, second = within(0, SUMS), within(1, SUMS)

    def then_first(j, color):
        spread_sums(j, color, 0)

    def then_second(j, color):
        spread_sums(j, color, 1)

    def spread_sums(j, color, part):
        @pl.when(j == 0)
        def _():
            far_sum(color, 0, part).start()
            far_sum(color, 1, part).start()

        for h in (0, 1):
            @pl.when(j == 1 + h)
            def _():
                near_sum(color, h, 0, part).start()

    for part in range(PARTS):
        with scope('last_d'):
            d_loads = []
            for color in (0, 1):
                hand_piece(part, color).wait_recv()
                d_loads.append(pltpu.make_async_copy(hd.at[last, :, piece(color, part)], bd.at[:, piece(color, part)], wsem.at[color]))
                d_loads[-1].start()
            for cp in d_loads:
                cp.wait()
        if part + 1 < PARTS:
            with scope('piece'):
                piece_arrived(part + 1)
        down(last, [piece(0, part), piece(1, part)])
        if part:
            with scope('relay'):
                relay_rows(last, part - 1)
        send(last, part)
        with scope('between'):
            if part == 0:
                fetch_rows(last - 1, every)
            if part == 1:
                await_rows(last - 1, every)
                add_rows(last - 1, every, 0, 3)
            if part == 2:
                add_rows(last - 1, every, 3, 6)
            if part == 3:
                fetch_rows(last, first, range(PARTS // SUMS))
                add_rows(last - 1, every, 6, 8)
    with scope('first_sums'):
        await_rows(last, first)
        add_rows(last, first, 0, 2, then_first)
    with scope('relay'):
        relay_rows(last, PARTS - 1)
    with scope('first_sums'):
        add_rows(last, first, 2, 8, then_first)
    with scope('second_sums'):
        combine(last, second, range(PARTS // SUMS, PARTS), then_second)
    for part in range(SUMS):
        for color, h in both:
            with scope('farsum_wait'):
                far_sum(color, h, part).wait_recv()
            r, w = pl.ds(h * half, half), within(part, SUMS)
            acc[color, 1 + 2 * h, r, w] = acc[color, 1 + 2 * h, r, w] + rf2[color, h, :, w]
            near_sum(color, h, 1, part).start()
    for part in range(SUMS):
        w = within(part, SUMS)
        for color in (0, 1):
            with scope('nearsum_wait'):
                for h in (0, 1):
                    for waits in (0, 1):
                        near_sum(color, h, waits, part).wait_recv()
            here = pl.ds(color * cols + w.start, w.size)
            out[:, here] = (acc[color, 0, :, w] + rn2[color, 0, :, w] + rn2[color, 1, :, w]).astype(out.dtype)

    for color, h in both:
        for part in range(SUMS):
            far_sum(color, h, part).wait_send()
            near_sum(color, h, 0, part).wait_send()
            near_sum(color, h, 1, part).wait_send()
        for part in range(PARTS):
            near_rows(last, color, h, part).wait_send()
            far_rows(last, color, h, part).wait_send()
            pass_rows(last, color, h, part).wait_send()
            far_piece(h, part, color).wait_send()
    for color in (0, 1):
        for part in range(PARTS):
            hand_piece(part, color).wait_send()
    for part in range(UPS):
        far_strip(0, part).wait_send()
        far_strip(1, part).wait_send()
        hand_strip(part).wait_send()

    def drain(i, carry):
        for color, h in both:
            near_rows(i, color, h).wait_send()
            far_rows(i, color, h).wait_send()
            pass_rows(i, color, h).wait_send()
        return carry

    lax.fori_loop(0, EXPERTS - 1, drain, 0)
    for dz, dy in peers:
        for cp in route_copies(dz, dy):
            cp.wait_send()
    for m in range(3):
        for n in (0, 1):
            hand_own(m, n).wait_send()
            for k in (0, 1):
                if k == 0 or m == 0:
                    far_copy(k, m, n).wait_send()
                for way in (0, 1):
                    line_copy(way, k, m, n, held[m].at[k]).wait_send()
        for slot in range(2, 8 if m == 0 else 7):
            hand_on(slot, m).wait_send()


def run_moe(hidden, ids, gates, w_gate, w_up, w_down):
    tokens, d = hidden.shape
    f = w_gate.shape[1]
    half, cols = tokens // 2, d // 2
    hbm = pl.BlockSpec(memory_space=pl.ANY)
    dma = pltpu.SemaphoreType.DMA
    flops = 2 * EXPERTS * BLOCKS * ROW_CAP * d * (3 * f + 4 * tokens)

    def both_ways(*shape):
        return [dma(shape), dma(shape)]

    return pl.pallas_call(
        moe_kernel,
        in_specs=[hbm] * 6,
        out_specs=[pl.BlockSpec(memory_space=pltpu.VMEM)] + [hbm] * 7,
        out_shape=[
            jax.ShapeDtypeStruct((tokens, d), BF16),
            jax.ShapeDtypeStruct((EXPERTS, 4, 4, ROW_CAP, d), BF16),
            jax.ShapeDtypeStruct((EXPERTS, BLOCKS, ROW_CAP, d), BF16),
            jax.ShapeDtypeStruct((EXPERTS, 2, 3, 4, ROW_CAP, cols), BF16),
            jax.ShapeDtypeStruct((EXPERTS, 2, 2, 2, ROW_CAP, cols), BF16),
            jax.ShapeDtypeStruct((8, d, f), BF16),
            jax.ShapeDtypeStruct((8, d, f), BF16),
            jax.ShapeDtypeStruct((8, f, d), BF16),
        ],
        scratch_shapes=[
            pltpu.VMEM((BLOCKS, tokens, d), BF16),
            pltpu.VMEM((BLOCKS,) + ids.shape, jnp.int32),
            pltpu.VMEM((BLOCKS,) + gates.shape, F32),
            pltpu.VMEM((BLOCKS, EXPERTS, tokens), F32),
            pltpu.VMEM((2, 4, 4, 4, EXPERTS, tokens), F32),
            pltpu.VMEM((2, 4, tokens, cols), F32),
            pltpu.VMEM((2, 2, half, cols), F32),
            pltpu.VMEM((2, 2, tokens, cols), F32),
            pltpu.VMEM((2, 2, 4, ROW_CAP, d), BF16),
            pltpu.VMEM((2, TILE, ROW_CAP, d), BF16),
            pltpu.VMEM((2, TILE * ROW_CAP, f), F32),
            pltpu.VMEM((2, TILE * ROW_CAP, f), BF16),
            pltpu.VMEM((d, f), BF16),
            pltpu.VMEM((d, f), BF16),
            pltpu.VMEM((f, d), BF16),
            *both_ways(2, 5, 4), *both_ways(2, BLOCKS), *both_ways(2, 2, 3, 2), *both_ways(2, 3, 2), *both_ways(3, 2), *both_ways(6, 3),
            *[sem for _ in range(3) for sem in both_ways(EXPERTS - 1 + PARTS, 2, 2)], *both_ways(2, 2, SUMS), *both_ways(2, 2, 2, SUMS),
            *both_ways(2, PARTS, 2), *both_ways(PARTS, 2), *both_ways(2, UPS), *both_ways(UPS), dma((3,)), dma((2,)), dma((2, 2)), dma((3,)), dma((2,)), dma((2, 4)),
        ],
        compiler_params=pltpu.CompilerParams(collective_id=0, has_side_effects=True, vmem_limit_bytes=63 * MIB),
        cost_estimate=pl.CostEstimate(flops=flops, bytes_accessed=400 * MIB, transcendentals=0),
        name='run_moe',
    )(hidden, ids, gates, w_gate, w_up, w_down)[0]


def solution(mesh):
    grid = Mesh(mesh.devices.reshape((mesh.shape['dp'],) + SIZES), ('dp',) + GRID)

    def body(hidden, route_idx, gate_weights, w_gate, w_up, w_down):
        return run_moe(hidden, route_idx.T, gate_weights.T, w_gate[0], w_up[0], w_down[0])

    r = P(('dp',) + GRID, None)
    e = P(GRID, None, None)
    return jax.shard_map(body, mesh=grid, in_specs=(r, r, r, e, e, e), out_specs=r, check_vma=False)
```

```python
import jax
import jax.numpy as jnp
from jax import lax
from jax.experimental import pallas as pl
from jax.experimental.pallas import tpu as pltpu
from jax.sharding import Mesh, PartitionSpec as P

BF16 = jnp.bfloat16
F32 = jnp.float32
MESH = pl.DeviceIdType.MESH
GRID = ('z', 'y', 'x', 'c')
SIZES = (4, 4, 4, 2)
ROW_CAP = 64
EXPERTS = 8
BLOCKS = 16
TILE = 8
EDGES = (0, 256, 512, 768, 1024)
PARTS = len(EDGES) - 1
SUMS = 2
FIRST = 2
OPENING = 128
UPS = 3
MIB = 1024 * 1024
scope = jax.named_scope


def expert_ids(place, x, c, line):
    dx = jnp.where((place == 2) | (place == 4), 3, 0) + jnp.where((place == 3) | (place == 5), 1, 0)
    dx += jnp.where(place >= 6, 2, 0)
    core = jnp.where(place == 0, c, 0) + jnp.where(place == 1, 1 - c, 0)
    core += jnp.where((place == 4) | (place == 5) | (place == 7), 1, 0)
    return line * EXPERTS + lax.rem(x + dx, 4) * 2 + core


def moe_kernel(hid, ids, gates, wg, wu, wd, out, o_hbm, x_hbm, rows_in, relay, hg, hu, hd,
               tok, all_ids, all_gates, slots, tabs, acc, rf2, rn2, stage, xt, abuf, hbuf, bg, bu, bd,
               tsend, trecv, msend, mrecv, isend, irecv, fsend, frecv, dsend, drecv, psend, precv,
               nrsend, nrrecv, frsend, frrecv, fwsend, fwrecv, f2send, f2recv, n2send, n2recv,
               gsend, grecv, qsend, qrecv, usend, urecv, vsend, vrecv, lsem, ssem, osem, wsem, xsem, csem):
    z, y, x, c = (lax.axis_index(a) for a in GRID)
    right, left = lax.rem(x + 1, 4), lax.rem(x + 3, 4)
    tokens, d = hid.shape
    half, cols = tokens // 2, d // 2
    rows = TILE * ROW_CAP
    own = (wg, wu, wd)
    held = (hg, hu, hd)
    partner = {'c': 1 - c}

    def remote(src, dst, send, recv, where):
        return pltpu.make_async_remote_copy(src_ref=src, dst_ref=dst, send_sem=send, recv_sem=recv, device_id=where, device_id_type=MESH)

    def along(dim, step):
        return {'z': lax.rem(z + (1 - dim) * step, 4), 'y': lax.rem(y + dim * step, 4)}

    def quarter(ref, m, lane, q, count=1):
        n = own[m].shape[0] // 4
        return ref.at[pl.ds(pl.multiple_of((2 * lane + q) * n, n), count * n), :]

    def line_copies(way, k, m, src):
        n = own[m].shape[0] // 2
        cuts = (0, OPENING, n) if (k, m) == (1, 0) else (0, n)
        dst, where = held[m].at[2 + 2 * k + way], {'x': right if way == 0 else left}
        copies = []
        for j, (a, b) in enumerate(zip(cuts, cuts[1:])):
            at = pl.ds(pl.multiple_of(c * n + a, 64), b - a)
            copies.append(remote(src.at[at, :], dst.at[at, :], isend.at[way, k, m, j], irecv.at[way, k, m, j], where))
        return copies

    def far_copy(k, m, q):
        src, dst = held[m].at[2 + 2 * k + q], held[m].at[6 + k]
        return remote(quarter(src, m, c, q), quarter(dst, m, c, q), fsend.at[k, m, q], frecv.at[k, m, q], {'x': right if q == 0 else left})

    def hand_own(m, n):
        lane = 1 - c if n == 0 else c
        return remote(quarter(own[m], m, lane, 0, 2), quarter(held[m].at[c], m, lane, 0, 2), dsend.at[m, n], drecv.at[m, n], partner)

    def hand_on(slot, m):
        ref = quarter(held[m].at[slot], m, c, 0, 2)
        return remote(ref, ref, psend.at[slot - 2, m], precv.at[slot - 2, m], partner)

    def start_line(k, m, src, which=(0, 1)):
        for way in (0, 1):
            for j, cp in enumerate(line_copies(way, k, m, src)):
                if j in which:
                    cp.start()

    def piece(color, part):
        return pl.ds(pl.multiple_of(color * cols + EDGES[part], 128), EDGES[part + 1] - EDGES[part])

    def far_piece(q, part):
        n = wd.shape[0] // 2
        at = pl.ds(q * n, n), piece(c, part)
        return remote(hd.at[4 + q, *at], hd.at[7, *at], gsend.at[q, part], grecv.at[q, part], {'x': right if q == 0 else left})

    def hand_piece(part):
        ref = hd.at[7, :, piece(c, part)]
        return remote(ref, ref, qsend.at[part], qrecv.at[part], partner)

    def strip(part):
        n = wu.shape[1] // UPS
        return pl.ds(part * n, n)

    def strip_of(ref, lane, q, count, part):
        n = ref.shape[0] // 4
        return ref.at[pl.ds(pl.multiple_of((2 * lane + q) * n, n), count * n), strip(part)]

    def far_strip(q, part):
        return remote(strip_of(hu.at[4 + q], c, q, 1, part), strip_of(hu.at[7], c, q, 1, part), usend.at[q, part], urecv.at[q, part], {'x': right if q == 0 else left})

    def hand_strip(part):
        ref = strip_of(hu.at[7], c, 0, 2, part)
        return remote(ref, ref, vsend.at[part], vrecv.at[part], partner)

    def place(k, a, b):
        return a * 4 + b if k == 0 else b * 4 + a

    def part(k, a, b, h=None):
        r = pl.ds(0, tokens) if h is None else pl.ds(h * half, half)
        return tok.at[place(k, a, b), r, pl.ds(k * cols, cols)]

    def first_copy(k, way):
        sems = tsend.at[k, 4, way], trecv.at[k, 4, way], along(k, 1 + 2 * (way % 2))
        if way < 2:
            return remote(part(k, 0, 0), part(k, 3 - 2 * way, 0), *sems)
        return remote(part(k, 7 - 2 * way, 0, way - 2), part(k, 2, 0, way - 2), *sems)

    def second_copy(k, a, way):
        sems = tsend.at[k, a, way], trecv.at[k, a, way], along(1 - k, 1 + 2 * (way % 2))
        if way < 2:
            return remote(part(k, a, 0), part(k, a, 3 - 2 * way), *sems)
        return remote(part(k, a, 7 - 2 * way, way - 2), part(k, a, 2, way - 2), *sems)

    def route_copies(dz, dy):
        s = ((4 - dz) % 4) * 4 + (4 - dy) % 4
        where = {'z': lax.rem(z + dz, 4), 'y': lax.rem(y + dy, 4)}
        return [remote(ref.at[0], ref.at[s], msend.at[n, s], mrecv.at[n, s], where) for n, ref in enumerate((all_ids, all_gates))]

    peers = [(dz, dy) for dz in range(4) for dy in range(4) if dz or dy]

    def spread(color, i, ring, m, n, part=None):
        w = pl.ds(color * cols, cols) if part is None else piece(color, part)
        if color == 0:
            return o_hbm.at[i, pl.ds(m, n), ring, :, w]
        return o_hbm.at[i, ring, pl.ds(m, n), :, w]

    def within(part):
        return pl.ds(0, cols) if part is None else pl.ds(EDGES[part], EDGES[part + 1] - EDGES[part])

    def sums(part):
        return pl.ds(part * (cols // SUMS), cols // SUMS)

    def row_sems(send, recv, i, part, color, h):
        n = i if part is None else i + part
        return send.at[n, color, h], recv.at[n, color, h], along(1 - color, 1 + 2 * h)

    def near_rows(i, color, h, part=None):
        return remote(spread(color, i, 1 + 2 * h, 0, 4, part), rows_in.at[i, color, 2 - 2 * h, :, :, within(part)], *row_sems(nrsend, nrrecv, i, part, color, h))

    def far_rows(i, color, h, part=None):
        return remote(spread(color, i, 2, 2 * h, 2, part), relay.at[i, color, h, :, :, within(part)], *row_sems(frsend, frrecv, i, part, color, h))

    def pass_rows(i, color, h, part=None):
        return remote(relay.at[i, color, h, :, :, within(part)], rows_in.at[i, color, 1, pl.ds(2 * h, 2), :, within(part)], *row_sems(fwsend, fwrecv, i, part, color, h))

    def far_sum(color, h, part):
        r, w = pl.ds(h * half, half), sums(part)
        return remote(acc.at[color, 2, r, w], rf2.at[color, h, :, w], f2send.at[color, h, part], f2recv.at[color, h, part], along(color, 1 + 2 * h))

    def near_sum(color, h, waits, part):
        r, w = pl.ds((h if waits else 1 - h) * half, half), sums(part)
        return remote(acc.at[color, 1 + 2 * h, r, w], rn2.at[color, h, r, w], n2send.at[color, h, waits, part], n2recv.at[color, h, waits, part], along(color, 1 + 2 * h))

    both = [(color, h) for color in (0, 1) for h in (0, 1)]

    own_tok = pltpu.make_async_copy(hid, tok.at[0], lsem.at[0])
    own_tok.start()
    own_routes = [pltpu.make_async_copy(ids, all_ids.at[0], lsem.at[1]), pltpu.make_async_copy(gates, all_gates.at[0], lsem.at[2])]
    for cp in own_routes:
        cp.start()

    barrier = pltpu.get_barrier_semaphore()
    for where in [partner, {'x': right}, {'x': left}] + [{'z': lax.rem(z + dz, 4), 'y': lax.rem(y + dy, 4)} for dz, dy in peers]:
        pl.semaphore_signal(barrier, inc=1, device_id=where, device_id_type=MESH)
    pl.semaphore_wait(barrier, 3 + len(peers))

    for n in (0, 1):
        for m in range(3):
            hand_own(m, n).start()

    @pl.when(c == 0)
    def _():
        for m in range(3):
            start_line(0, m, own[m])

    @pl.when(c == 1)
    def _():
        start_line(1, 0, own[0], (0,))

    own_tok.wait()
    for k in (0, 1):
        for way in (0, 1):
            first_copy(k, way).start()
            second_copy(k, 0, way).start()
    for cp in own_routes:
        cp.wait()
    for dz, dy in peers:
        for cp in route_copies(dz, dy):
            cp.start()
    for m in range(3):
        hand_own(m, 0).wait_recv()

        @pl.when(c == 1)
        def _():
            start_line(0, m, held[m].at[0])

    for m in range(3):
        @pl.when(c == 0)
        def _():
            start_line(1, m, held[m].at[1])

        @pl.when(c == 1)
        def _():
            start_line(1, m, own[m], (1,) if m == 0 else (0,))

    for k in (0, 1):
        first_copy(k, 0).wait_recv()
        first_copy(k, 2).start()
        second_copy(k, 3, 0).start()
        second_copy(k, 3, 1).start()
        first_copy(k, 1).wait_recv()
        first_copy(k, 3).start()
        second_copy(k, 1, 0).start()
        second_copy(k, 1, 1).start()
    for k in (0, 1):
        for way in (0, 1):
            second_copy(k, 0, way).wait_recv()
            second_copy(k, 0, 2 + way).start()
    for k in (0, 1):
        first_copy(k, 2).wait_recv()
        first_copy(k, 3).wait_recv()
        second_copy(k, 2, 0).start()
        second_copy(k, 2, 1).start()

    for dz, dy in peers:
        for cp in route_copies(dz, dy):
            cp.wait_recv()
    order = lax.broadcasted_iota(jnp.int32, (EXPERTS, tokens), 0)
    earlier = lax.broadcasted_iota(jnp.int32, (tokens, tokens), 0) < lax.broadcasted_iota(jnp.int32, (tokens, tokens), 1)
    earlier = jnp.where(earlier, 1.0, 0.0).astype(BF16)

    def table(s, line):
        mine = expert_ids(order, x, c, line)
        rec, weight = all_ids[s], all_gates[s]
        chosen = jnp.zeros((EXPERTS, tokens), F32)
        gate = jnp.zeros((EXPERTS, tokens), F32)
        for k in range(rec.shape[0]):
            hit = rec[k:k + 1, :] == mine
            chosen += jnp.where(hit, 1.0, 0.0)
            gate += jnp.where(hit, weight[k:k + 1, :], 0.0)
        rank = jnp.dot(chosen.astype(BF16), earlier, preferred_element_type=F32)
        return jnp.where(chosen > 0.5, rank, -1.0), gate

    def own_table(s, carry):
        slots[s] = table(s, z * 4 + y)[0]
        return carry

    lax.fori_loop(0, BLOCKS, own_table, 0)

    def ring_table(n, carry):
        color, m, s = n // 16, lax.rem(n // 4, 4), lax.rem(n, 4)
        line = lax.rem(z + color * s, 4) * 4 + lax.rem(y + (1 - color) * s, 4)
        slot, gate = table((4 - 3 * color) * m, line)
        tabs[color, m, s, 0] = slot
        for p in range(1, 4):
            term = gate.astype(BF16).astype(F32)
            tabs[color, m, s, p] = term
            gate = gate - term
        return carry

    def turn(a):
        for k in (0, 1):
            for way in (0, 1):
                second_copy(k, a, way).wait_recv()
                second_copy(k, a, 2 + way).start()

    turn(3)
    turn(1)
    turn(2)
    lax.fori_loop(0, 32, ring_table, 0)
    for a in range(4):
        for k in (0, 1):
            for way in (2, 3):
                second_copy(k, a, way).wait_recv()

    def x_store(s, b):
        return pltpu.make_async_copy(stage.at[b].reshape(EXPERTS, ROW_CAP, d), x_hbm.at[:, s], ssem.at[b])

    lanes = lax.broadcasted_iota(jnp.int32, (ROW_CAP, tokens), 0).astype(F32)

    def gather(s, carry):
        b = lax.rem(s, 2)
        pick = jnp.concatenate([jnp.where(slots[s, pl.ds(e, 1), :] == lanes, 1.0, 0.0).astype(BF16) for e in range(EXPERTS)], axis=0)
        got = jnp.dot(pick, tok[s], preferred_element_type=F32).astype(BF16)

        @pl.when(s >= 2)
        def _():
            x_store(s, b).wait()

        stage[b] = got.reshape(2, 4, ROW_CAP, d)
        x_store(s, b).start()
        return carry

    lax.fori_loop(0, BLOCKS, gather, 0)
    acc[...] = jnp.zeros(acc.shape, F32)
    x_store(0, 0).wait()
    x_store(0, 1).wait()
    for k in (0, 1):
        for way in range(4):
            first_copy(k, way).wait_send()
            for a in range(4):
                second_copy(k, a, way).wait_send()

    def load(i, m, go):
        dst = (bg, bu, bd)[m]

        @pl.when(i == 0)
        def _():
            go(pltpu.make_async_copy(own[m], dst, wsem.at[m]))

        @pl.when(i == 1)
        def _():
            go(pltpu.make_async_copy(held[m].at[1 - c], dst, wsem.at[m]))

        @pl.when(i >= 2)
        def _():
            go(pltpu.make_async_copy(held[m].at[i], dst, wsem.at[m]))

    def line_arrived(k, ms):
        for m in ms:
            for way in (0, 1):
                for cp in line_copies(way, k, m, held[m].at[k]):
                    cp.wait_recv()
                if (k, m) == (1, 1):
                    for part in range(UPS):
                        far_strip(way, part).start()
                elif (k, m) != (1, 2):
                    far_copy(k, m, way).start()
                hand_on(2 + 2 * k + way, m).start()

    def far_arrived(k, ms):
        for m in ms:
            far_copy(k, m, 0).wait_recv()
            far_copy(k, m, 1).wait_recv()
            hand_on(6 + k, m).start()

    def handed(i, ms):
        @pl.when(i == 1)
        def _():
            for m in ms:
                hand_own(m, 1).wait_recv()

        @pl.when(i >= 2)
        def _():
            for m in ms:
                hand_on(i, m).wait_recv()

    def x_load(i, t):
        return pltpu.make_async_copy(x_hbm.at[i, pl.ds(t * TILE, TILE)], xt.at[t], xsem.at[t])

    def o_store(i, t, w, n):
        return pltpu.make_async_copy(stage.at[t, :, :, :, w], o_hbm.at[i, pl.ds(2 * t, 2), :, :, w], osem.at[t, n])

    def begin(cp):
        cp.start()

    def finish(cp):
        cp.wait()

    def relay_rows(i, part=None):
        for color, h in both:
            far_rows(i, color, h, part).wait_recv()
            pass_rows(i, color, h, part).start()

    def row_loads(i, color, w):
        at = pl.ds(8 * lax.rem(i, 2) + 4 * color, 4)
        here = pl.ds(color * cols + w.start, w.size)
        srcs = [o_hbm.at[i, :, 0, :, here] if color == 0 else o_hbm.at[i, 0, :, :, here]] + [rows_in.at[i, color, s, :, :, w] for s in range(3)]
        return [pltpu.make_async_copy(src, tok.at[at, pl.ds(s * ROW_CAP, ROW_CAP), w], csem.at[color, s]) for s, src in enumerate(srcs)]

    def fetch_rows(i, w, parts=(None,)):
        for color in (0, 1):
            with scope('rows_wait'):
                for part in parts:
                    for h in (0, 1):
                        near_rows(i, color, h, part).wait_recv()
                        pass_rows(i, color, h, part).wait_recv()
            for cp in row_loads(i, color, w):
                cp.start()

    def await_rows(i, w):
        with scope('rowload_wait'):
            for color in (0, 1):
                for cp in row_loads(i, color, w):
                    cp.wait()

    def add_rows(i, w, start=0, stop=8, then=None):
        def one(n, carry):
            j, color = n // 2, lax.rem(n, 2)
            m = lax.rem(2 + 3 * j + 3 * (j * (j - 1) // 2), 4)
            got = tok[8 * lax.rem(i, 2) + 4 * color + m, :, w]
            total = acc[color, m, :, w]
            for p in range(1, 4):
                g = jnp.concatenate([
                    jnp.where(tabs[color, m, s, 0, pl.ds(i, 1), :] == lanes, tabs[color, m, s, p, pl.ds(i, 1), :], 0.0).astype(BF16)
                    for s in range(4)], axis=0)
                total += lax.dot_general(g, got, (((0,), (0,)), ((), ())), preferred_element_type=F32)
            acc[color, m, :, w] = total
            if then is not None:
                then(j, color)
            return carry

        lax.fori_loop(start, stop, one, 0)

    def combine(i, w, parts=(None,), then=None):
        fetch_rows(i, w, parts)
        await_rows(i, w)
        add_rows(i, w, then=then)

    def load_up(i):
        handed(i, (0, 1))
        load(i, 0, begin)
        load(i, 1, begin)

    def load_down(i):
        handed(i, (2,))
        load(i, 2, begin)

    def down(i, ws):
        def one(t, carry):
            for n, w in enumerate(ws):
                o = jnp.dot(hbuf[t], bd[:, w], preferred_element_type=F32).astype(BF16)
                stage[t, :, :, :, w] = o.reshape(2, 4, ROW_CAP, o.shape[-1])
                o_store(i, t, w, n).start()
            return carry

        with scope('down'):
            lax.fori_loop(0, 2, one, 0)
            for t in (0, 1):
                for n, w in enumerate(ws):
                    o_store(i, t, w, n).wait()

    def send(i, part=None, colors=(0, 1)):
        for color in colors:
            for h in (0, 1):
                far_rows(i, color, h, part).start()
        for color in colors:
            for h in (0, 1):
                near_rows(i, color, h, part).start()

    def expert(i, carry):
        late = (i == 4) | (i == 6)
        for t in (0, 1):
            x_load(i, t).start()

        @pl.when(jnp.logical_not(late))
        def _():
            load_down(i)

        @pl.when(i == 5)
        def _():
            for part in range(PARTS):
                for q in (0, 1):
                    far_piece(q, part).start()

        @pl.when(late)
        def _():
            with scope('late_gu'):
                load_up(i)

        with scope('load_gu'):
            load(i, 0, finish)
            load(i, 1, finish)

        def up(t, carry):
            x_load(i, t).wait()
            xs = xt[t].reshape(rows, d)
            a = jnp.dot(xs, bg[...], preferred_element_type=F32)
            u = jnp.dot(xs, bu[...], preferred_element_type=F32)
            hbuf[t] = (jax.nn.silu(a) * u).astype(BF16)
            return carry

        with scope('up'):
            lax.fori_loop(0, 2, up, 0)

        @pl.when(i == 1)
        def _():
            with scope('line0'):
                line_arrived(0, (0, 1, 2))

        @pl.when((i == 0) | (i == 2) | (i == 4))
        def _():
            with scope('next_gu'):
                load_up(i + 1)

        @pl.when(i == 4)
        def _():
            with scope('line1_d'):
                line_arrived(1, (2,))

        @pl.when(i == 6)
        def _():
            with scope('far0_d'):
                far_arrived(0, (2,))

        @pl.when(i >= 1)
        def _():
            with scope('relay'):
                relay_rows(i - 1)

        @pl.when(i >= 2)
        def _():
            with scope('combine'):
                combine(i - 2, within(None))

        @pl.when(i == 1)
        def _():
            with scope('next_gu'):
                load_up(i + 1)

        @pl.when(i == 3)
        def _():
            with scope('line1_gu'):
                line_arrived(1, (0, 1))

        @pl.when(i == 5)
        def _():
            with scope('far0_gu'):
                far_arrived(0, (0, 1))

        @pl.when(late)
        def _():
            with scope('late_d'):
                load_down(i)

        with scope('load_d'):
            load(i, 2, finish)
        down(i, [pl.ds(0, d)])
        send(i)
        return carry

    load_up(0)
    lax.fori_loop(0, EXPERTS - 1, expert, 0)

    last = EXPERTS - 1
    for t in (0, 1):
        x_load(last, t).start()
    def strip_arrived(part):
        far_strip(0, part).wait_recv()
        far_strip(1, part).wait_recv()
        hand_strip(part).start()

    def strip_arrived(part):
        with scope('strip'):
            far_strip(0, part).wait_recv()
            far_strip(1, part).wait_recv()
            hand_strip(part).start()

    def gate_half(t, carry):
        x_load(last, t).wait()
        a = jnp.dot(xt[t].reshape(rows, d), bg[...], preferred_element_type=F32)
        abuf[t] = jax.nn.silu(a)
        return carry

    with scope('last_g'):
        far_arrived(1, (0,))
    with scope('combine'):
        combine(last - 2, within(None))
    with scope('last_g'):
        hand_on(last, 0).wait_recv()
        g_load = pltpu.make_async_copy(hg.at[last], bg, wsem.at[0])
        g_load.start()
    strip_arrived(0)
    with scope('last_g'):
        g_load.wait()
    with scope('gate_half'):
        lax.fori_loop(0, 2, gate_half, 0)
    strip_arrived(1)
    with scope('relay'):
        relay_rows(last - 1)

    def piece_arrived(part):
        with scope('piece'):
            for q in (0, 1):
                far_piece(q, part).wait_recv()
            hand_piece(part).start()

    def piece_load(color, part):
        at = piece(color, part)
        return pltpu.make_async_copy(hd.at[last, :, at], bd.at[:, at], wsem.at[color])

    for part in range(UPS):
        with scope('last_u'):
            hand_strip(part).wait_recv()
            u_load = pltpu.make_async_copy(hu.at[last, :, strip(part)], bu.at[:, strip(part)], wsem.at[1])
            u_load.start()
            u_load.wait()

        def up_half(t, carry):
            u = jnp.dot(xt[t].reshape(rows, d), bu[:, strip(part)], preferred_element_type=F32)
            hbuf[t, :, strip(part)] = (abuf[t, :, strip(part)] * u).astype(BF16)
            return carry

        with scope('up_half'):
            lax.fori_loop(0, 2, up_half, 0)
        if part + 2 < UPS:
            strip_arrived(part + 2)
    piece_arrived(0)

    every = within(None)
    first, second = sums(0), sums(1)

    def then_first(j, color):
        spread_sums(j, color, 0)

    def then_second(j, color):
        spread_sums(j, color, 1)

    def spread_sums(j, color, part):
        @pl.when(j == 0)
        def _():
            far_sum(color, 0, part).start()
            far_sum(color, 1, part).start()

        for h in (0, 1):
            @pl.when(j == 1 + h)
            def _():
                near_sum(color, h, 0, part).start()

    for step in (0, 1):
        with scope('last_d'):
            if step:
                hand_piece(0).wait_recv()
            color = c if step == 0 else 1 - c
            piece_load(color, 0).start()
            piece_load(color, 0).wait()
        if step:
            piece_arrived(1)
        down(last, [piece(color, 0)])
        for k in (0, 1):
            @pl.when(color == k)
            def _():
                send(last, 0, (k,))

    for part in range(1, PARTS):
        with scope('last_d'):
            hand_piece(part).wait_recv()
            for color in (0, 1):
                piece_load(color, part).start()
            for color in (0, 1):
                piece_load(color, part).wait()
        if part + 1 < PARTS:
            piece_arrived(part + 1)
        down(last, [piece(0, part), piece(1, part)])
        with scope('relay'):
            relay_rows(last, part - 1)
        send(last, part)
        with scope('between'):
            if part == 1:
                fetch_rows(last - 1, every)
            if part == 2:
                await_rows(last - 1, every)
                add_rows(last - 1, every, 0, 4)
            if part == 3:
                fetch_rows(last, first, range(FIRST))
                add_rows(last - 1, every, 4, 8)
    with scope('first_sums'):
        await_rows(last, first)
        add_rows(last, first, 0, 2, then_first)
    with scope('relay'):
        relay_rows(last, PARTS - 1)
    with scope('first_sums'):
        add_rows(last, first, 2, 8, then_first)
    with scope('second_sums'):
        combine(last, second, range(FIRST, PARTS), then_second)
    for part in range(SUMS):
        for color, h in both:
            with scope('farsum_wait'):
                far_sum(color, h, part).wait_recv()
            r, w = pl.ds(h * half, half), sums(part)
            acc[color, 1 + 2 * h, r, w] = acc[color, 1 + 2 * h, r, w] + rf2[color, h, :, w]
            near_sum(color, h, 1, part).start()
    for part in range(SUMS):
        w = sums(part)
        for color in (0, 1):
            with scope('nearsum_wait'):
                for h in (0, 1):
                    for waits in (0, 1):
                        near_sum(color, h, waits, part).wait_recv()
            here = pl.ds(color * cols + w.start, w.size)
            out[:, here] = (acc[color, 0, :, w] + rn2[color, 0, :, w] + rn2[color, 1, :, w]).astype(out.dtype)

    for color, h in both:
        for part in range(SUMS):
            far_sum(color, h, part).wait_send()
            near_sum(color, h, 0, part).wait_send()
            near_sum(color, h, 1, part).wait_send()
        for part in range(PARTS):
            near_rows(last, color, h, part).wait_send()
            far_rows(last, color, h, part).wait_send()
            pass_rows(last, color, h, part).wait_send()
    for part in range(PARTS):
        far_piece(0, part).wait_send()
        far_piece(1, part).wait_send()
        hand_piece(part).wait_send()
    for part in range(UPS):
        far_strip(0, part).wait_send()
        far_strip(1, part).wait_send()
        hand_strip(part).wait_send()

    def drain(i, carry):
        for color, h in both:
            near_rows(i, color, h).wait_send()
            far_rows(i, color, h).wait_send()
            pass_rows(i, color, h).wait_send()
        return carry

    lax.fori_loop(0, EXPERTS - 1, drain, 0)
    for dz, dy in peers:
        for cp in route_copies(dz, dy):
            cp.wait_send()
    for m in range(3):
        for n in (0, 1):
            hand_own(m, n).wait_send()
            for k in (0, 1):
                if k == 0 or m == 0:
                    far_copy(k, m, n).wait_send()
                for cp in line_copies(n, k, m, held[m].at[k]):
                    cp.wait_send()
        for slot in range(2, 8 if m == 0 else 7):
            hand_on(slot, m).wait_send()


def run_moe(hidden, ids, gates, w_gate, w_up, w_down):
    tokens, d = hidden.shape
    f = w_gate.shape[1]
    half, cols = tokens // 2, d // 2
    hbm = pl.BlockSpec(memory_space=pl.ANY)
    dma = pltpu.SemaphoreType.DMA
    flops = 2 * EXPERTS * BLOCKS * ROW_CAP * d * (3 * f + 4 * tokens)

    def both_ways(*shape):
        return [dma(shape), dma(shape)]

    return pl.pallas_call(
        moe_kernel,
        in_specs=[hbm] * 6,
        out_specs=[pl.BlockSpec(memory_space=pltpu.VMEM)] + [hbm] * 7,
        out_shape=[
            pltpu.VMEM((tokens, d), BF16),
            jax.ShapeDtypeStruct((EXPERTS, 4, 4, ROW_CAP, d), BF16),
            jax.ShapeDtypeStruct((EXPERTS, BLOCKS, ROW_CAP, d), BF16),
            jax.ShapeDtypeStruct((EXPERTS, 2, 3, 4, ROW_CAP, cols), BF16),
            jax.ShapeDtypeStruct((EXPERTS, 2, 2, 2, ROW_CAP, cols), BF16),
            jax.ShapeDtypeStruct((8, d, f), BF16),
            jax.ShapeDtypeStruct((8, d, f), BF16),
            jax.ShapeDtypeStruct((8, f, d), BF16),
        ],
        scratch_shapes=[
            pltpu.VMEM((BLOCKS, tokens, d), BF16),
            pltpu.VMEM((BLOCKS,) + ids.shape, jnp.int32),
            pltpu.VMEM((BLOCKS,) + gates.shape, F32),
            pltpu.VMEM((BLOCKS, EXPERTS, tokens), F32),
            pltpu.VMEM((2, 4, 4, 4, EXPERTS, tokens), F32),
            pltpu.VMEM((2, 4, tokens, cols), F32),
            pltpu.VMEM((2, 2, half, cols), F32),
            pltpu.VMEM((2, 2, tokens, cols), F32),
            pltpu.VMEM((2, 2, 4, ROW_CAP, d), BF16),
            pltpu.VMEM((2, TILE, ROW_CAP, d), BF16),
            pltpu.VMEM((2, TILE * ROW_CAP, f), F32),
            pltpu.VMEM((2, TILE * ROW_CAP, f), BF16),
            pltpu.VMEM((d, f), BF16),
            pltpu.VMEM((d, f), BF16),
            pltpu.VMEM((f, d), BF16),
            *both_ways(2, 5, 4), *both_ways(2, BLOCKS), *both_ways(2, 2, 3, 2), *both_ways(2, 3, 2), *both_ways(3, 2), *both_ways(6, 3),
            *[sem for _ in range(3) for sem in both_ways(EXPERTS - 1 + PARTS, 2, 2)], *both_ways(2, 2, SUMS), *both_ways(2, 2, 2, SUMS),
            *both_ways(2, PARTS), *both_ways(PARTS), *both_ways(2, UPS), *both_ways(UPS), dma((3,)), dma((2,)), dma((2, 2)), dma((3,)), dma((2,)), dma((2, 4)),
        ],
        compiler_params=pltpu.CompilerParams(collective_id=0, has_side_effects=True, vmem_limit_bytes=60 * MIB),
        cost_estimate=pl.CostEstimate(flops=flops, bytes_accessed=400 * MIB, transcendentals=0),
        name='run_moe',
    )(hidden, ids, gates, w_gate, w_up, w_down)[0]


def solution(mesh):
    grid = Mesh(mesh.devices.reshape((mesh.shape['dp'],) + SIZES), ('dp',) + GRID)

    def body(hidden, route_idx, gate_weights, w_gate, w_up, w_down):
        return run_moe(hidden, route_idx.T, gate_weights.T, w_gate[0], w_up[0], w_down[0])

    r = P(('dp',) + GRID, None)
    e = P(GRID, None, None)
    return jax.shard_map(body, mesh=grid, in_specs=(r, r, r, e, e, e), out_specs=r, check_vma=False)
```

```python
import jax
import jax.numpy as jnp
from jax import lax
from jax.experimental import pallas as pl
from jax.experimental.pallas import tpu as pltpu
from jax.sharding import Mesh, PartitionSpec as P

BF16 = jnp.bfloat16
F32 = jnp.float32
MESH = pl.DeviceIdType.MESH
GRID = ('z', 'y', 'x', 'c')
SIZES = (4, 4, 4, 2)
ROW_CAP = 64
EXPERTS = 8
BLOCKS = 16
TILE = 8
EDGES = (0, 256, 512, 768, 1024)
PARTS = len(EDGES) - 1
SUMS = 2
FIRST = 2
OPENING = 128
UPS = 3
MIB = 1024 * 1024
scope = jax.named_scope


def expert_ids(place, x, c, line):
    dx = jnp.where((place == 2) | (place == 4), 3, 0) + jnp.where((place == 3) | (place == 5), 1, 0)
    dx += jnp.where(place >= 6, 2, 0)
    core = jnp.where(place == 0, c, 0) + jnp.where(place == 1, 1 - c, 0)
    core += jnp.where((place == 4) | (place == 5) | (place == 7), 1, 0)
    return line * EXPERTS + lax.rem(x + dx, 4) * 2 + core


def moe_kernel(hid, ids, gates, wg, wu, wd, out, o_hbm, x_hbm, rows_in, relay, hg, hu, hd,
               tok, all_ids, all_gates, slots, tabs, acc, rf2, rn2, last_relay, last_in, stage, xt, abuf, hbuf, bg, bu, bd,
               tsend, trecv, msend, mrecv, wsend, irecv, frecv, drecv, precv, grecv, qrecv, urecv, vrecv,
               rsend, rrecv, hrecv, ssend, f2recv, n2recv, lsem, ssem, wsem, xsem, csem):
    z, y, x, c = (lax.axis_index(a) for a in GRID)
    right, left = lax.rem(x + 1, 4), lax.rem(x + 3, 4)
    tokens, d = hid.shape
    half, cols = tokens // 2, d // 2
    rows = TILE * ROW_CAP
    own = (wg, wu, wd)
    held = (hg, hu, hd)
    partner = {'c': 1 - c}

    def remote(src, dst, send, recv, where):
        return pltpu.make_async_remote_copy(src_ref=src, dst_ref=dst, send_sem=send, recv_sem=recv, device_id=where, device_id_type=MESH)

    def received(ref, sem):
        remote(ref, ref, sem, sem, partner).wait_recv()

    def sent(ref, sem):
        remote(ref, ref, sem, sem, partner).wait_send()

    def along(dim, step):
        return {'z': lax.rem(z + (1 - dim) * step, 4), 'y': lax.rem(y + dim * step, 4)}

    def quarter(ref, m, lane, q, count=1):
        n = own[m].shape[0] // 4
        return ref.at[pl.ds(pl.multiple_of((2 * lane + q) * n, n), count * n), :]

    def line_copies(way, k, m, src, which=(0, 1)):
        n = own[m].shape[0] // 2
        cuts = (0, OPENING, n) if (k, m) == (1, 0) else (0, n)
        dst, where = held[m].at[2 + 2 * k + way], {'x': right if way == 0 else left}
        copies = []
        for j in which[:len(cuts) - 1]:
            a, b = cuts[j:j + 2]
            at = pl.ds(pl.multiple_of(c * n + a, 64), b - a)
            copies.append(remote(src.at[at, :], dst.at[at, :], wsend.at[m], irecv.at[way, k, m], where))
        return copies

    def far_copy(k, m, q):
        src, dst = held[m].at[2 + 2 * k + q], held[m].at[6 + k]
        return remote(quarter(src, m, c, q), quarter(dst, m, c, q), wsend.at[m], frecv.at[3 * k + m], {'x': right if q == 0 else left})

    def hand_own(m, n):
        lane = 1 - c if n == 0 else c
        return remote(quarter(own[m], m, lane, 0, 2), quarter(held[m].at[c], m, lane, 0, 2), wsend.at[m], drecv.at[m, n], partner)

    def hand_on(slot, m):
        ref = quarter(held[m].at[slot], m, c, 0, 2)
        return remote(ref, ref, wsend.at[m], precv.at[3 * (slot - 2) + m], partner)

    def start_line(k, m, src, which=(0, 1)):
        for way in (0, 1):
            for cp in line_copies(way, k, m, src, which):
                cp.start()

    def piece(color, part):
        return pl.ds(pl.multiple_of(color * cols + EDGES[part], 128), EDGES[part + 1] - EDGES[part])

    def far_piece(q, part):
        n = wd.shape[0] // 2
        at = pl.ds(q * n, n), piece(c, part)
        return remote(hd.at[4 + q, *at], hd.at[7, *at], wsend.at[2], grecv.at[part], {'x': right if q == 0 else left})

    def hand_piece(part):
        ref = hd.at[7, :, piece(c, part)]
        return remote(ref, ref, wsend.at[2], qrecv.at[part], partner)

    def strip(part):
        n = wu.shape[1] // UPS
        return pl.ds(part * n, n)

    def strip_of(ref, lane, q, count, part):
        n = ref.shape[0] // 4
        return ref.at[pl.ds(pl.multiple_of((2 * lane + q) * n, n), count * n), strip(part)]

    def far_strip(q, part):
        return remote(strip_of(hu.at[4 + q], c, q, 1, part), strip_of(hu.at[7], c, q, 1, part), wsend.at[1], urecv.at[part], {'x': right if q == 0 else left})

    def hand_strip(part):
        ref = strip_of(hu.at[7], c, 0, 2, part)
        return remote(ref, ref, wsend.at[1], vrecv.at[part], partner)

    def place(k, a, b):
        return a * 4 + b if k == 0 else b * 4 + a

    def part(k, a, b, h=None):
        r = pl.ds(0, tokens) if h is None else pl.ds(h * half, half)
        return tok.at[place(k, a, b), r, pl.ds(k * cols, cols)]

    def first_copy(k, way):
        sems = tsend, trecv.at[k, 4, min(way, 2)], along(k, 1 + 2 * (way % 2))
        if way < 2:
            return remote(part(k, 0, 0), part(k, 3 - 2 * way, 0), *sems)
        return remote(part(k, 7 - 2 * way, 0, way - 2), part(k, 2, 0, way - 2), *sems)

    def second_copy(k, a, way):
        sems = tsend, trecv.at[k, a, min(way, 2)], along(1 - k, 1 + 2 * (way % 2))
        if way < 2:
            return remote(part(k, a, 0), part(k, a, 3 - 2 * way), *sems)
        return remote(part(k, a, 7 - 2 * way, way - 2), part(k, a, 2, way - 2), *sems)

    def route_copies(dz, dy):
        s = ((4 - dz) % 4) * 4 + (4 - dy) % 4
        where = {'z': lax.rem(z + dz, 4), 'y': lax.rem(y + dy, 4)}
        return [remote(ref.at[0], ref.at[s], msend.at[n], mrecv.at[n], where) for n, ref in enumerate((all_ids, all_gates))]

    peers = [(dz, dy) for dz in range(4) for dy in range(4) if dz or dy]

    def spread(color, i, ring, m, n, part=None):
        ref, w = (o_hbm.at[i], pl.ds(color * cols, cols)) if part is None else (stage, piece(color, part))
        if color == 0:
            return ref.at[pl.ds(m, n), ring, :, w]
        return ref.at[ring, pl.ds(m, n), :, w]

    def landing(i, color, s, m, n, part):
        if part is None:
            return rows_in.at[i, color, s - 1, pl.ds(m, n)]
        return last_in.at[color, s - 1, pl.ds(m, n), :, within(part)]

    def halfway(i, color, h, part):
        return relay.at[i, color, h] if part is None else last_relay.at[color, h, :, :, within(part)]

    def within(part):
        return pl.ds(0, cols) if part is None else pl.ds(EDGES[part], EDGES[part + 1] - EDGES[part])

    def sums(part):
        return pl.ds(part * (cols // SUMS), cols // SUMS)

    def row_sems(send, recv, i, part, color, h):
        return send.at[i], recv.at[i if part is None else i + part], along(1 - color, 1 + 2 * h)

    def near_rows(i, color, h, part=None):
        return remote(spread(color, i, 1 + 2 * h, 0, 4, part), landing(i, color, 3 - 2 * h, 0, 4, part), *row_sems(rsend, rrecv, i, part, color, h))

    def far_rows(i, color, h, part=None):
        return remote(spread(color, i, 2, 2 * h, 2, part), halfway(i, color, h, part), *row_sems(rsend, hrecv, i, part, color, h))

    def pass_rows(i, color, h, part=None):
        return remote(halfway(i, color, h, part), landing(i, color, 2, 2 * h, 2, part), *row_sems(rsend, rrecv, i, part, color, h))

    def far_sum(color, h, part):
        r, w = pl.ds(h * half, half), sums(part)
        return remote(acc.at[color, 2, r, w], rf2.at[color, h, :, w], ssend, f2recv.at[color, h, part], along(color, 1 + 2 * h))

    def near_sum(color, h, waits, part):
        r, w = pl.ds((h if waits else 1 - h) * half, half), sums(part)
        return remote(acc.at[color, 1 + 2 * h, r, w], rn2.at[color, h, r, w], ssend, n2recv.at[color, part], along(color, 1 + 2 * h))

    both = [(color, h) for color in (0, 1) for h in (0, 1)]

    own_tok = pltpu.make_async_copy(hid, tok.at[0], lsem.at[0])
    own_tok.start()
    own_routes = [pltpu.make_async_copy(ids, all_ids.at[0], lsem.at[1]), pltpu.make_async_copy(gates, all_gates.at[0], lsem.at[2])]
    for cp in own_routes:
        cp.start()

    barrier = pltpu.get_barrier_semaphore()
    for where in [partner, {'x': right}, {'x': left}] + [{'z': lax.rem(z + dz, 4), 'y': lax.rem(y + dy, 4)} for dz, dy in peers]:
        pl.semaphore_signal(barrier, inc=1, device_id=where, device_id_type=MESH)
    pl.semaphore_wait(barrier, 3 + len(peers))

    for n in (0, 1):
        for m in range(3):
            hand_own(m, n).start()

    @pl.when(c == 0)
    def _():
        for m in range(3):
            start_line(0, m, own[m])

    @pl.when(c == 1)
    def _():
        start_line(1, 0, own[0], (0,))

    own_tok.wait()
    for k in (0, 1):
        for way in (0, 1):
            first_copy(k, way).start()
            second_copy(k, 0, way).start()
    for cp in own_routes:
        cp.wait()
    for dz, dy in peers:
        for cp in route_copies(dz, dy):
            cp.start()
    for m in range(3):
        hand_own(m, 0).wait_recv()

        @pl.when(c == 1)
        def _():
            start_line(0, m, held[m].at[0])

    for m in range(3):
        @pl.when(c == 0)
        def _():
            start_line(1, m, held[m].at[1])

        @pl.when(c == 1)
        def _():
            start_line(1, m, own[m], (1,) if m == 0 else (0,))

    for k in (0, 1):
        first_copy(k, 0).wait_recv()
        first_copy(k, 2).start()
        second_copy(k, 3, 0).start()
        second_copy(k, 3, 1).start()
        first_copy(k, 1).wait_recv()
        first_copy(k, 3).start()
        second_copy(k, 1, 0).start()
        second_copy(k, 1, 1).start()
    for k in (0, 1):
        for way in (0, 1):
            second_copy(k, 0, way).wait_recv()
            second_copy(k, 0, 2 + way).start()
    for k in (0, 1):
        received(part(k, 2, 0), trecv.at[k, 4, 2])
        second_copy(k, 2, 0).start()
        second_copy(k, 2, 1).start()

    for n, ref in enumerate((all_ids, all_gates)):
        received(ref.at[pl.ds(1, BLOCKS - 1)], mrecv.at[n])
    order = lax.broadcasted_iota(jnp.int32, (EXPERTS, tokens), 0)
    earlier = lax.broadcasted_iota(jnp.int32, (tokens, tokens), 0) < lax.broadcasted_iota(jnp.int32, (tokens, tokens), 1)
    earlier = jnp.where(earlier, 1.0, 0.0).astype(BF16)

    def table(s, line):
        mine = expert_ids(order, x, c, line)
        rec, weight = all_ids[s], all_gates[s]
        chosen = jnp.zeros((EXPERTS, tokens), F32)
        gate = jnp.zeros((EXPERTS, tokens), F32)
        for k in range(rec.shape[0]):
            hit = rec[k:k + 1, :] == mine
            chosen += jnp.where(hit, 1.0, 0.0)
            gate += jnp.where(hit, weight[k:k + 1, :], 0.0)
        rank = jnp.dot(chosen.astype(BF16), earlier, preferred_element_type=F32)
        return jnp.where(chosen > 0.5, rank, -1.0), gate

    def own_table(s, carry):
        slots[s] = table(s, z * 4 + y)[0]
        return carry

    lax.fori_loop(0, BLOCKS, own_table, 0)

    def ring_table(n, carry):
        color, m, s = n // 16, lax.rem(n // 4, 4), lax.rem(n, 4)
        line = lax.rem(z + color * s, 4) * 4 + lax.rem(y + (1 - color) * s, 4)
        slot, gate = table((4 - 3 * color) * m, line)
        tabs[color, m, s, 0] = slot
        for p in range(1, 4):
            term = gate.astype(BF16).astype(F32)
            tabs[color, m, s, p] = term
            gate = gate - term
        return carry

    def turn(a):
        for k in (0, 1):
            for way in (0, 1):
                second_copy(k, a, way).wait_recv()
                second_copy(k, a, 2 + way).start()

    turn(3)
    turn(1)
    turn(2)
    lax.fori_loop(0, 32, ring_table, 0)
    for a in range(4):
        for k in (0, 1):
            received(part(k, a, 2), trecv.at[k, a, 2])

    def x_store(s, b):
        return pltpu.make_async_copy(stage.at[pl.ds(2 * b, 2)].reshape(EXPERTS, ROW_CAP, d), x_hbm.at[:, s], ssem.at[b])

    lanes = lax.broadcasted_iota(jnp.int32, (ROW_CAP, tokens), 0).astype(F32)

    def gather(s, carry):
        b = lax.rem(s, 2)
        pick = jnp.concatenate([jnp.where(slots[s, pl.ds(e, 1), :] == lanes, 1.0, 0.0).astype(BF16) for e in range(EXPERTS)], axis=0)
        got = jnp.dot(pick, tok[s], preferred_element_type=F32).astype(BF16)

        @pl.when(s >= 2)
        def _():
            x_store(s, b).wait()

        stage[pl.ds(2 * b, 2)] = got.reshape(2, 4, ROW_CAP, d)
        x_store(s, b).start()
        return carry

    lax.fori_loop(0, BLOCKS, gather, 0)
    acc[...] = jnp.zeros(acc.shape, F32)
    x_store(0, 0).wait()
    x_store(0, 1).wait()
    sent(tok.at[pl.ds(1, BLOCKS - 1)], tsend)

    def load(i, m, go):
        dst = (bg, bu, bd)[m]

        @pl.when(i == 0)
        def _():
            go(pltpu.make_async_copy(own[m], dst, wsem.at[m]))

        @pl.when(i == 1)
        def _():
            go(pltpu.make_async_copy(held[m].at[1 - c], dst, wsem.at[m]))

        @pl.when(i >= 2)
        def _():
            go(pltpu.make_async_copy(held[m].at[i], dst, wsem.at[m]))

    def line_arrived(k, ms):
        for m in ms:
            for way in (0, 1):
                received(quarter(held[m].at[2 + 2 * k + way], m, c, 0, 2), irecv.at[way, k, m])
                if (k, m) == (1, 1):
                    for part in range(UPS):
                        far_strip(way, part).start()
                elif (k, m) != (1, 2):
                    far_copy(k, m, way).start()
                hand_on(2 + 2 * k + way, m).start()

    def far_arrived(k, ms):
        for m in ms:
            received(quarter(held[m].at[6 + k], m, c, 0, 2), frecv.at[3 * k + m])
            hand_on(6 + k, m).start()

    def handed(i, ms):
        @pl.when(i == 1)
        def _():
            for m in ms:
                hand_own(m, 1).wait_recv()

        @pl.when(i >= 2)
        def _():
            for m in ms:
                hand_on(i, m).wait_recv()

    def x_load(i, t):
        return pltpu.make_async_copy(x_hbm.at[i, pl.ds(t * TILE, TILE)], xt.at[t], xsem.at[t])

    def o_store(i, t):
        return pltpu.make_async_copy(stage.at[pl.ds(2 * t, 2)], o_hbm.at[i, pl.ds(2 * t, 2)], ssem.at[t])

    def begin(cp):
        cp.start()

    def finish(cp):
        cp.wait()

    def relay_rows(i, part=None):
        if part is None:
            received(relay.at[i], hrecv.at[i])
        else:
            received(last_relay.at[:, :, :, :, within(part)], hrecv.at[i + part])
        for color, h in both:
            pass_rows(i, color, h, part).start()

    def row_loads(i, color):
        at = pl.ds(8 * lax.rem(i, 2) + 4 * color, 4)
        srcs = [spread(color, i, 0, 0, 4)] + [rows_in.at[i, color, s] for s in range(3)]
        return [pltpu.make_async_copy(src, tok.at[at, pl.ds(s * ROW_CAP, ROW_CAP), pl.ds(0, cols)], csem.at[color]) for s, src in enumerate(srcs)]

    def rows_arrived(i, parts=(None,)):
        with scope('rows_wait'):
            for part in parts:
                if part is None:
                    received(rows_in.at[i], rrecv.at[i])
                else:
                    received(last_in.at[:, :, :, :, within(part)], rrecv.at[i + part])

    def fetch_rows(i):
        rows_arrived(i)
        for color in (0, 1):
            for cp in row_loads(i, color):
                cp.start()

    def await_rows(i):
        with scope('rowload_wait'):
            for color in (0, 1):
                ref = tok.at[pl.ds(8 * lax.rem(i, 2) + 4 * color, 4), :, pl.ds(0, cols)]
                pltpu.make_async_copy(ref, ref, csem.at[color]).wait()

    def add_rows(i, w, take, start=0, stop=8, then=None):
        def one(n, carry):
            j, color = n // 2, lax.rem(n, 2)
            m = lax.rem(2 + 3 * j + 3 * (j * (j - 1) // 2), 4)
            got = take(color, m)
            total = acc[color, m, :, w]
            for p in range(1, 4):
                g = jnp.concatenate([
                    jnp.where(tabs[color, m, s, 0, pl.ds(i, 1), :] == lanes, tabs[color, m, s, p, pl.ds(i, 1), :], 0.0).astype(BF16)
                    for s in range(4)], axis=0)
                total += lax.dot_general(g, got, (((0,), (0,)), ((), ())), preferred_element_type=F32)
            acc[color, m, :, w] = total
            if then is not None:
                then(j, color)
            return carry

        lax.fori_loop(start, stop, one, 0)

    def add_fetched(i, start=0, stop=8):
        add_rows(i, pl.ds(0, cols), lambda color, m: tok[8 * lax.rem(i, 2) + 4 * color + m, :, pl.ds(0, cols)], start, stop)

    def add_last(w, start, stop, then):
        def take(color, m):
            here = pl.ds(pl.multiple_of(color * cols + w.start, 128), w.size)
            return jnp.concatenate([stage[(1 - color) * m, color * m, :, here]] + [last_in[color, s, m, :, w] for s in range(3)], axis=0)

        add_rows(EXPERTS - 1, w, take, start, stop, then)

    def combine(i):
        fetch_rows(i)
        await_rows(i)
        add_fetched(i)

    def load_up(i):
        handed(i, (0, 1))
        load(i, 0, begin)
        load(i, 1, begin)

    def load_down(i):
        handed(i, (2,))
        load(i, 2, begin)

    def down(ws):
        def one(t, carry):
            for w in ws:
                o = jnp.dot(hbuf[t], bd[:, w], preferred_element_type=F32).astype(BF16)
                stage[pl.ds(2 * t, 2), :, :, w] = o.reshape(2, 4, ROW_CAP, o.shape[-1])
            return carry

        with scope('down'):
            lax.fori_loop(0, 2, one, 0)

    def send(i, part=None, colors=(0, 1)):
        for color in colors:
            for h in (0, 1):
                far_rows(i, color, h, part).start()
        for color in colors:
            for h in (0, 1):
                near_rows(i, color, h, part).start()

    def expert(i, carry):
        late = (i == 4) | (i == 6)
        for t in (0, 1):
            x_load(i, t).start()

        @pl.when(jnp.logical_not(late))
        def _():
            load_down(i)

        @pl.when(i == 5)
        def _():
            for part in range(PARTS):
                for q in (0, 1):
                    far_piece(q, part).start()

        @pl.when(late)
        def _():
            with scope('late_gu'):
                load_up(i)

        with scope('load_gu'):
            load(i, 0, finish)
            load(i, 1, finish)

        def up(t, carry):
            x_load(i, t).wait()
            xs = xt[t].reshape(rows, d)
            a = jnp.dot(xs, bg[...], preferred_element_type=F32)
            u = jnp.dot(xs, bu[...], preferred_element_type=F32)
            hbuf[t] = (jax.nn.silu(a) * u).astype(BF16)
            return carry

        with scope('up'):
            lax.fori_loop(0, 2, up, 0)

        @pl.when(i == 1)
        def _():
            with scope('line0'):
                line_arrived(0, (0, 1, 2))

        @pl.when((i == 0) | (i == 2) | (i == 4))
        def _():
            with scope('next_gu'):
                load_up(i + 1)

        @pl.when(i == 4)
        def _():
            with scope('line1_d'):
                line_arrived(1, (2,))

        @pl.when(i == 6)
        def _():
            with scope('far0_d'):
                far_arrived(0, (2,))

        @pl.when(i >= 1)
        def _():
            with scope('relay'):
                relay_rows(i - 1)

        @pl.when(i >= 2)
        def _():
            with scope('combine'):
                combine(i - 2)

        @pl.when(i == 1)
        def _():
            with scope('next_gu'):
                load_up(i + 1)

        @pl.when(i == 3)
        def _():
            with scope('line1_gu'):
                line_arrived(1, (0, 1))

        @pl.when(i == 5)
        def _():
            with scope('far0_gu'):
                far_arrived(0, (0, 1))

        @pl.when(late)
        def _():
            with scope('late_d'):
                load_down(i)

        with scope('load_d'):
            load(i, 2, finish)
        down([pl.ds(0, d)])
        with scope('store'):
            for t in (0, 1):
                o_store(i, t).start()
            for t in (0, 1):
                o_store(i, t).wait()
        send(i)
        return carry

    load_up(0)
    lax.fori_loop(0, EXPERTS - 1, expert, 0)

    last = EXPERTS - 1
    for t in (0, 1):
        x_load(last, t).start()
    def strip_arrived(part):
        far_strip(0, part).wait_recv()
        far_strip(1, part).wait_recv()
        hand_strip(part).start()

    def strip_arrived(part):
        with scope('strip'):
            received(strip_of(hu.at[7], c, 0, 2, part), urecv.at[part])
            hand_strip(part).start()

    def gate_half(t, carry):
        x_load(last, t).wait()
        a = jnp.dot(xt[t].reshape(rows, d), bg[...], preferred_element_type=F32)
        abuf[t] = jax.nn.silu(a)
        return carry

    with scope('last_g'):
        far_arrived(1, (0,))
    with scope('combine'):
        combine(last - 2)
    with scope('last_g'):
        hand_on(last, 0).wait_recv()
        g_load = pltpu.make_async_copy(hg.at[last], bg, wsem.at[0])
        g_load.start()
    strip_arrived(0)
    with scope('last_g'):
        g_load.wait()
    with scope('gate_half'):
        lax.fori_loop(0, 2, gate_half, 0)
    strip_arrived(1)
    with scope('relay'):
        relay_rows(last - 1)

    def piece_arrived(part):
        with scope('piece'):
            received(hd.at[7, :, piece(c, part)], grecv.at[part])
            hand_piece(part).start()

    def piece_load(color, part):
        at = piece(color, part)
        return pltpu.make_async_copy(hd.at[last, :, at], bd.at[:, at], wsem.at[color])

    for part in range(UPS):
        with scope('last_u'):
            hand_strip(part).wait_recv()
            u_load = pltpu.make_async_copy(hu.at[last, :, strip(part)], bu.at[:, strip(part)], wsem.at[1])
            u_load.start()
            u_load.wait()

        def up_half(t, carry):
            u = jnp.dot(xt[t].reshape(rows, d), bu[:, strip(part)], preferred_element_type=F32)
            hbuf[t, :, strip(part)] = (abuf[t, :, strip(part)] * u).astype(BF16)
            return carry

        with scope('up_half'):
            lax.fori_loop(0, 2, up_half, 0)
        if part + 2 < UPS:
            strip_arrived(part + 2)
    piece_arrived(0)

    first, second = sums(0), sums(1)

    def then_first(j, color):
        spread_sums(j, color, 0)

    def then_second(j, color):
        spread_sums(j, color, 1)

    def spread_sums(j, color, part):
        @pl.when(j == 0)
        def _():
            far_sum(color, 0, part).start()
            far_sum(color, 1, part).start()

        for h in (0, 1):
            @pl.when(j == 1 + h)
            def _():
                near_sum(color, h, 0, part).start()

    for step in (0, 1):
        with scope('last_d'):
            if step:
                hand_piece(0).wait_recv()
            color = c if step == 0 else 1 - c
            piece_load(color, 0).start()
            piece_load(color, 0).wait()
        if step:
            piece_arrived(1)
        down([piece(color, 0)])
        for k in (0, 1):
            @pl.when(color == k)
            def _():
                send(last, 0, (k,))

    for part in range(1, PARTS):
        with scope('last_d'):
            hand_piece(part).wait_recv()
            for color in (0, 1):
                piece_load(color, part).start()
            for color in (0, 1):
                piece_load(color, part).wait()
        down([piece(0, part), piece(1, part)])
        send(last, part)
        if part + 1 < PARTS:
            piece_arrived(part + 1)
        with scope('relay'):
            relay_rows(last, part - 1)
        with scope('between'):
            if part == 1:
                fetch_rows(last - 1)
            if part == 2:
                await_rows(last - 1)
                add_fetched(last - 1, 0, 4)
            if part == 3:
                add_fetched(last - 1, 4, 8)
    rows_arrived(last, range(FIRST))
    with scope('first_sums'):
        add_last(first, 0, 2, then_first)
    with scope('relay'):
        relay_rows(last, PARTS - 1)
    with scope('first_sums'):
        add_last(first, 2, 8, then_first)
    rows_arrived(last, range(FIRST, PARTS))
    with scope('second_sums'):
        add_last(second, 0, 8, then_second)
    for part in range(SUMS):
        for color, h in both:
            with scope('farsum_wait'):
                far_sum(color, h, part).wait_recv()
            r, w = pl.ds(h * half, half), sums(part)
            acc[color, 1 + 2 * h, r, w] = acc[color, 1 + 2 * h, r, w] + rf2[color, h, :, w]
            near_sum(color, h, 1, part).start()
    for part in range(SUMS):
        w = sums(part)
        for color in (0, 1):
            with scope('nearsum_wait'):
                received(rn2.at[color, :, :, w], n2recv.at[color, part])
            here = pl.ds(color * cols + w.start, w.size)
            out[:, here] = (acc[color, 0, :, w] + rn2[color, 0, :, w] + rn2[color, 1, :, w]).astype(out.dtype)

    sent(acc.at[:, pl.ds(1, 3)], ssend)
    for i in range(EXPERTS - 1):
        sent(o_hbm.at[i], rsend.at[i])
    sent(stage, rsend.at[last])
    for n, ref in enumerate((all_ids, all_gates)):
        sent(ref.at[pl.ds(1, BLOCKS - 1)], msend.at[n])
    for m in range(3):
        sent(held[m].at[pl.ds(0, EXPERTS - 1)], wsend.at[m])


def run_moe(hidden, ids, gates, w_gate, w_up, w_down):
    tokens, d = hidden.shape
    f = w_gate.shape[1]
    half, cols = tokens // 2, d // 2
    hbm = pl.BlockSpec(memory_space=pl.ANY)
    dma = pltpu.SemaphoreType.DMA
    flops = 2 * EXPERTS * BLOCKS * ROW_CAP * d * (3 * f + 4 * tokens)

    return pl.pallas_call(
        moe_kernel,
        in_specs=[hbm] * 6,
        out_specs=[pl.BlockSpec(memory_space=pltpu.VMEM)] + [hbm] * 7,
        out_shape=[
            pltpu.VMEM((tokens, d), BF16),
            jax.ShapeDtypeStruct((EXPERTS, 4, 4, ROW_CAP, d), BF16),
            jax.ShapeDtypeStruct((EXPERTS, BLOCKS, ROW_CAP, d), BF16),
            jax.ShapeDtypeStruct((EXPERTS, 2, 3, 4, ROW_CAP, cols), BF16),
            jax.ShapeDtypeStruct((EXPERTS, 2, 2, 2, ROW_CAP, cols), BF16),
            jax.ShapeDtypeStruct((8, d, f), BF16),
            jax.ShapeDtypeStruct((8, d, f), BF16),
            jax.ShapeDtypeStruct((8, f, d), BF16),
        ],
        scratch_shapes=[
            pltpu.VMEM((BLOCKS, tokens, d), BF16),
            pltpu.VMEM((BLOCKS,) + ids.shape, jnp.int32),
            pltpu.VMEM((BLOCKS,) + gates.shape, F32),
            pltpu.VMEM((BLOCKS, EXPERTS, tokens), F32),
            pltpu.VMEM((2, 4, 4, 4, EXPERTS, tokens), F32),
            pltpu.VMEM((2, 4, tokens, cols), F32),
            pltpu.VMEM((2, 2, half, cols), F32),
            pltpu.VMEM((2, 2, tokens, cols), F32),
            pltpu.VMEM((2, 2, 2, ROW_CAP, cols), BF16),
            pltpu.VMEM((2, 3, 4, ROW_CAP, cols), BF16),
            pltpu.VMEM((4, 4, ROW_CAP, d), BF16),
            pltpu.VMEM((2, TILE, ROW_CAP, d), BF16),
            pltpu.VMEM((2, TILE * ROW_CAP, f), F32),
            pltpu.VMEM((2, TILE * ROW_CAP, f), BF16),
            pltpu.VMEM((d, f), BF16),
            pltpu.VMEM((d, f), BF16),
            pltpu.VMEM((f, d), BF16),
            dma(()), dma((2, 5, 3)), dma((2,)), dma((2,)), dma((3,)), dma((2, 2, 3)), dma((4,)), dma((3, 2)), dma((16,)), dma((PARTS,)), dma((PARTS,)), dma((UPS,)), dma((UPS,)),
            dma((EXPERTS,)), dma((EXPERTS - 1 + PARTS,)), dma((EXPERTS - 1 + PARTS,)), dma(()), dma((2, 2, SUMS)), dma((2, SUMS)), dma((3,)), dma((2,)), dma((3,)), dma((2,)), dma((2,)),
        ],
        compiler_params=pltpu.CompilerParams(collective_id=0, has_side_effects=True, vmem_limit_bytes=62 * MIB),
        cost_estimate=pl.CostEstimate(flops=flops, bytes_accessed=400 * MIB, transcendentals=0),
        name='run_moe',
    )(hidden, ids, gates, w_gate, w_up, w_down)[0]


def solution(mesh):
    grid = Mesh(mesh.devices.reshape((mesh.shape['dp'],) + SIZES), ('dp',) + GRID)

    def body(hidden, route_idx, gate_weights, w_gate, w_up, w_down):
        return run_moe(hidden, route_idx.T, gate_weights.T, w_gate[0], w_up[0], w_down[0])

    r = P(('dp',) + GRID, None)
    e = P(GRID, None, None)
    return jax.shard_map(body, mesh=grid, in_specs=(r, r, r, e, e, e), out_specs=r, check_vma=False)
```

```python
import jax
import jax.numpy as jnp
from jax import lax
from jax.experimental import pallas as pl
from jax.experimental.pallas import tpu as pltpu
from jax.sharding import Mesh, PartitionSpec as P

BF16 = jnp.bfloat16
F32 = jnp.float32
MESH = pl.DeviceIdType.MESH
GRID = ('z', 'y', 'x', 'c')
SIZES = (4, 4, 4, 2)
ROW_CAP = 64
EXPERTS = 8
BLOCKS = 16
TILE = 8
EDGES = (0, 256, 512, 768, 1024)
PARTS = len(EDGES) - 1
SUMS = 2
FIRST = 2
OPENING = 128
UPS = 3
MIB = 1024 * 1024
scope = jax.named_scope


def expert_ids(place, x, c, line):
    dx = jnp.where((place == 2) | (place == 4), 3, 0) + jnp.where((place == 3) | (place == 5), 1, 0)
    dx += jnp.where(place >= 6, 2, 0)
    core = jnp.where(place == 0, c, 0) + jnp.where(place == 1, 1 - c, 0)
    core += jnp.where((place == 4) | (place == 5) | (place == 7), 1, 0)
    return line * EXPERTS + lax.rem(x + dx, 4) * 2 + core


def moe_kernel(hid, ids, gates, wg, wu, wd, out, o_hbm, x_hbm, rows_in, relay, hg, hu, hd,
               tok, all_ids, all_gates, slots, tabs, acc, rf2, rn2, last_relay, last_in, stage, xt, abuf, hbuf, bg, bu, bd,
               tsend, trecv, msend, mrecv, wsend, irecv, frecv, drecv, precv, grecv, qrecv, urecv, vrecv,
               rsend, rrecv, hrecv, ssend, f2recv, n2recv, lsem, ssem, wsem, xsem, csem):
    z, y, x, c = (lax.axis_index(a) for a in GRID)
    right, left = lax.rem(x + 1, 4), lax.rem(x + 3, 4)
    tokens, d = hid.shape
    half, cols = tokens // 2, d // 2
    rows = TILE * ROW_CAP
    own = (wg, wu, wd)
    held = (hg, hu, hd)
    partner = {'c': 1 - c}

    def remote(src, dst, send, recv, where):
        return pltpu.make_async_remote_copy(src_ref=src, dst_ref=dst, send_sem=send, recv_sem=recv, device_id=where, device_id_type=MESH)

    def received(ref, sem):
        remote(ref, ref, sem, sem, partner).wait_recv()

    def sent(ref, sem):
        remote(ref, ref, sem, sem, partner).wait_send()

    def along(dim, step):
        return {'z': lax.rem(z + (1 - dim) * step, 4), 'y': lax.rem(y + dim * step, 4)}

    def quarter(ref, m, lane, q, count=1):
        n = own[m].shape[0] // 4
        return ref.at[pl.ds(pl.multiple_of((2 * lane + q) * n, n), count * n), :]

    def line_copies(way, k, m, src, which=(0, 1)):
        n = own[m].shape[0] // 2
        cuts = (0, OPENING, n) if (k, m) == (1, 0) else (0, n)
        dst, where = held[m].at[2 + 2 * k + way], {'x': right if way == 0 else left}
        copies = []
        for j in which[:len(cuts) - 1]:
            a, b = cuts[j:j + 2]
            at = pl.ds(pl.multiple_of(c * n + a, 64), b - a)
            copies.append(remote(src.at[at, :], dst.at[at, :], wsend.at[m], irecv.at[way, k, m], where))
        return copies

    def far_copy(k, m, q):
        src, dst = held[m].at[2 + 2 * k + q], held[m].at[6 + k]
        return remote(quarter(src, m, c, q), quarter(dst, m, c, q), wsend.at[m], frecv.at[3 * k + m], {'x': right if q == 0 else left})

    def hand_own(m, n):
        lane = 1 - c if n == 0 else c
        return remote(quarter(own[m], m, lane, 0, 2), quarter(held[m].at[c], m, lane, 0, 2), wsend.at[m], drecv.at[m, n], partner)

    def hand_on(slot, m):
        ref = quarter(held[m].at[slot], m, c, 0, 2)
        return remote(ref, ref, wsend.at[m], precv.at[3 * (slot - 2) + m], partner)

    def start_line(k, m, src, which=(0, 1)):
        for way in (0, 1):
            for cp in line_copies(way, k, m, src, which):
                cp.start()

    def piece(color, part):
        return pl.ds(pl.multiple_of(color * cols + EDGES[part], 128), EDGES[part + 1] - EDGES[part])

    def far_piece(q, part):
        n = wd.shape[0] // 2
        at = pl.ds(q * n, n), piece(c, part)
        return remote(hd.at[4 + q, *at], hd.at[7, *at], wsend.at[2], grecv.at[part], {'x': right if q == 0 else left})

    def hand_piece(part):
        ref = hd.at[7, :, piece(c, part)]
        return remote(ref, ref, wsend.at[2], qrecv.at[part], partner)

    def strip(part):
        n = wu.shape[1] // UPS
        return pl.ds(part * n, n)

    def strip_of(ref, lane, q, count, part):
        n = ref.shape[0] // 4
        return ref.at[pl.ds(pl.multiple_of((2 * lane + q) * n, n), count * n), strip(part)]

    def far_strip(q, part):
        return remote(strip_of(hu.at[4 + q], c, q, 1, part), strip_of(hu.at[7], c, q, 1, part), wsend.at[1], urecv.at[part], {'x': right if q == 0 else left})

    def hand_strip(part):
        ref = strip_of(hu.at[7], c, 0, 2, part)
        return remote(ref, ref, wsend.at[1], vrecv.at[part], partner)

    def place(k, a, b):
        return a * 4 + b if k == 0 else b * 4 + a

    def part(k, a, b, h=None):
        r = pl.ds(0, tokens) if h is None else pl.ds(h * half, half)
        return tok.at[place(k, a, b), r, pl.ds(k * cols, cols)]

    def first_copy(k, way):
        sems = tsend, trecv.at[k, 4, min(way, 2)], along(k, 1 + 2 * (way % 2))
        if way < 2:
            return remote(part(k, 0, 0), part(k, 3 - 2 * way, 0), *sems)
        return remote(part(k, 7 - 2 * way, 0, way - 2), part(k, 2, 0, way - 2), *sems)

    def second_copy(k, a, way):
        sems = tsend, trecv.at[k, a, min(way, 2)], along(1 - k, 1 + 2 * (way % 2))
        if way < 2:
            return remote(part(k, a, 0), part(k, a, 3 - 2 * way), *sems)
        return remote(part(k, a, 7 - 2 * way, way - 2), part(k, a, 2, way - 2), *sems)

    def route_copies(dz, dy):
        s = ((4 - dz) % 4) * 4 + (4 - dy) % 4
        where = {'z': lax.rem(z + dz, 4), 'y': lax.rem(y + dy, 4)}
        return [remote(ref.at[0], ref.at[s], msend.at[n], mrecv.at[n], where) for n, ref in enumerate((all_ids, all_gates))]

    peers = [(dz, dy) for dz in range(4) for dy in range(4) if dz or dy]

    def spread(color, i, ring, m, n, part=None):
        ref, w = (o_hbm.at[i], pl.ds(color * cols, cols)) if part is None else (stage, piece(color, part))
        if color == 0:
            return ref.at[pl.ds(m, n), ring, :, w]
        return ref.at[ring, pl.ds(m, n), :, w]

    def landing(i, color, s, m, n, part):
        if part is None:
            return rows_in.at[i, color, s - 1, pl.ds(m, n)]
        return last_in.at[color, s - 1, pl.ds(m, n), :, within(part)]

    def halfway(i, color, h, part):
        return relay.at[i, color, h] if part is None else last_relay.at[color, h, :, :, within(part)]

    def within(part):
        return pl.ds(0, cols) if part is None else pl.ds(EDGES[part], EDGES[part + 1] - EDGES[part])

    def sums(part):
        return pl.ds(part * (cols // SUMS), cols // SUMS)

    def row_sems(send, recv, i, part, color, h):
        return send.at[i], recv.at[i if part is None else i + part], along(1 - color, 1 + 2 * h)

    def near_rows(i, color, h, part=None):
        return remote(spread(color, i, 1 + 2 * h, 0, 4, part), landing(i, color, 3 - 2 * h, 0, 4, part), *row_sems(rsend, rrecv, i, part, color, h))

    def far_rows(i, color, h, part=None):
        return remote(spread(color, i, 2, 2 * h, 2, part), halfway(i, color, h, part), *row_sems(rsend, hrecv, i, part, color, h))

    def pass_rows(i, color, h, part=None):
        return remote(halfway(i, color, h, part), landing(i, color, 2, 2 * h, 2, part), *row_sems(rsend, rrecv, i, part, color, h))

    def far_sum(color, h, part):
        r, w = pl.ds(h * half, half), sums(part)
        return remote(acc.at[color, 2, r, w], rf2.at[color, h, :, w], ssend, f2recv.at[color, h, part], along(color, 1 + 2 * h))

    def near_sum(color, h, waits, part):
        r, w = pl.ds((h if waits else 1 - h) * half, half), sums(part)
        return remote(acc.at[color, 1 + 2 * h, r, w], rn2.at[color, h, r, w], ssend, n2recv.at[color, part], along(color, 1 + 2 * h))

    both = [(color, h) for color in (0, 1) for h in (0, 1)]

    own_tok = pltpu.make_async_copy(hid, tok.at[0], lsem.at[0])
    own_tok.start()
    own_routes = [pltpu.make_async_copy(ids, all_ids.at[0], lsem.at[1]), pltpu.make_async_copy(gates, all_gates.at[0], lsem.at[2])]
    for cp in own_routes:
        cp.start()

    barrier = pltpu.get_barrier_semaphore()
    for where in [partner, {'x': right}, {'x': left}] + [{'z': lax.rem(z + dz, 4), 'y': lax.rem(y + dy, 4)} for dz, dy in peers]:
        pl.semaphore_signal(barrier, inc=1, device_id=where, device_id_type=MESH)
    pl.semaphore_wait(barrier, 3 + len(peers))

    for n in (0, 1):
        for m in range(3):
            hand_own(m, n).start()

    @pl.when(c == 0)
    def _():
        for m in range(3):
            start_line(0, m, own[m])

    @pl.when(c == 1)
    def _():
        start_line(1, 0, own[0], (0,))

    own_tok.wait()
    for k in (0, 1):
        for way in (0, 1):
            first_copy(k, way).start()
            second_copy(k, 0, way).start()
    for cp in own_routes:
        cp.wait()
    for dz, dy in peers:
        for cp in route_copies(dz, dy):
            cp.start()
    for m in range(3):
        hand_own(m, 0).wait_recv()

        @pl.when(c == 1)
        def _():
            start_line(0, m, held[m].at[0])

    for m in range(3):
        @pl.when(c == 0)
        def _():
            start_line(1, m, held[m].at[1])

        @pl.when(c == 1)
        def _():
            start_line(1, m, own[m], (1,) if m == 0 else (0,))

    for k in (0, 1):
        first_copy(k, 0).wait_recv()
        first_copy(k, 2).start()
        second_copy(k, 3, 0).start()
        second_copy(k, 3, 1).start()
        first_copy(k, 1).wait_recv()
        first_copy(k, 3).start()
        second_copy(k, 1, 0).start()
        second_copy(k, 1, 1).start()
    for k in (0, 1):
        for way in (0, 1):
            second_copy(k, 0, way).wait_recv()
            second_copy(k, 0, 2 + way).start()
    for k in (0, 1):
        received(part(k, 2, 0), trecv.at[k, 4, 2])
        second_copy(k, 2, 0).start()
        second_copy(k, 2, 1).start()

    for n, ref in enumerate((all_ids, all_gates)):
        received(ref.at[pl.ds(1, BLOCKS - 1)], mrecv.at[n])
    order = lax.broadcasted_iota(jnp.int32, (EXPERTS, tokens), 0)
    earlier = lax.broadcasted_iota(jnp.int32, (tokens, tokens), 0) < lax.broadcasted_iota(jnp.int32, (tokens, tokens), 1)
    earlier = jnp.where(earlier, 1.0, 0.0).astype(BF16)

    def table(s, line):
        mine = expert_ids(order, x, c, line)
        rec, weight = all_ids[s], all_gates[s]
        chosen = jnp.zeros((EXPERTS, tokens), F32)
        gate = jnp.zeros((EXPERTS, tokens), F32)
        for k in range(rec.shape[0]):
            hit = rec[k:k + 1, :] == mine
            chosen += jnp.where(hit, 1.0, 0.0)
            gate += jnp.where(hit, weight[k:k + 1, :], 0.0)
        rank = jnp.dot(chosen.astype(BF16), earlier, preferred_element_type=F32)
        return jnp.where(chosen > 0.5, rank, -1.0), gate

    def own_table(s, carry):
        slots[s] = table(s, z * 4 + y)[0]
        return carry

    lax.fori_loop(0, BLOCKS, own_table, 0)

    def ring_table(n, carry):
        color, m, s = n // 16, lax.rem(n // 4, 4), lax.rem(n, 4)
        line = lax.rem(z + color * s, 4) * 4 + lax.rem(y + (1 - color) * s, 4)
        slot, gate = table((4 - 3 * color) * m, line)
        tabs[color, m, s, 0] = slot
        for p in range(1, 4):
            term = (gate * (1 - 2.0 ** -8) if p == 1 else gate).astype(BF16).astype(F32)
            tabs[color, m, s, p] = term
            gate = gate - term
        return carry

    def turn(a):
        for k in (0, 1):
            for way in (0, 1):
                second_copy(k, a, way).wait_recv()
                second_copy(k, a, 2 + way).start()

    turn(3)
    turn(1)
    turn(2)
    lax.fori_loop(0, 32, ring_table, 0)
    for a in range(4):
        for k in (0, 1):
            received(part(k, a, 2), trecv.at[k, a, 2])

    def x_store(s, b):
        return pltpu.make_async_copy(stage.at[pl.ds(2 * b, 2)].reshape(EXPERTS, ROW_CAP, d), x_hbm.at[:, s], ssem.at[b])

    lanes = lax.broadcasted_iota(jnp.int32, (ROW_CAP, tokens), 0).astype(F32)

    def gather(s, carry):
        b = lax.rem(s, 2)
        pick = jnp.concatenate([jnp.where(slots[s, pl.ds(e, 1), :] == lanes, 1.0, 0.0).astype(BF16) for e in range(EXPERTS)], axis=0)
        got = jnp.dot(pick, tok[s], preferred_element_type=F32).astype(BF16)

        @pl.when(s >= 2)
        def _():
            x_store(s, b).wait()

        stage[pl.ds(2 * b, 2)] = got.reshape(2, 4, ROW_CAP, d)
        x_store(s, b).start()
        return carry

    lax.fori_loop(0, BLOCKS, gather, 0)
    acc[...] = jnp.zeros(acc.shape, F32)
    x_store(0, 0).wait()
    x_store(0, 1).wait()
    sent(tok.at[pl.ds(1, BLOCKS - 1)], tsend)

    def load(i, m, go):
        dst = (bg, bu, bd)[m]

        @pl.when(i == 0)
        def _():
            go(pltpu.make_async_copy(own[m], dst, wsem.at[m]))

        @pl.when(i == 1)
        def _():
            go(pltpu.make_async_copy(held[m].at[1 - c], dst, wsem.at[m]))

        @pl.when(i >= 2)
        def _():
            go(pltpu.make_async_copy(held[m].at[i], dst, wsem.at[m]))

    def line_arrived(k, ms):
        for m in ms:
            for way in (0, 1):
                received(quarter(held[m].at[2 + 2 * k + way], m, c, 0, 2), irecv.at[way, k, m])
                if (k, m) == (1, 1):
                    for part in range(UPS):
                        far_strip(way, part).start()
                elif (k, m) != (1, 2):
                    far_copy(k, m, way).start()
                hand_on(2 + 2 * k + way, m).start()

    def far_arrived(k, ms):
        for m in ms:
            received(quarter(held[m].at[6 + k], m, c, 0, 2), frecv.at[3 * k + m])
            hand_on(6 + k, m).start()

    def handed(i, ms):
        @pl.when(i == 1)
        def _():
            for m in ms:
                hand_own(m, 1).wait_recv()

        @pl.when(i >= 2)
        def _():
            for m in ms:
                hand_on(i, m).wait_recv()

    def x_load(i, t):
        return pltpu.make_async_copy(x_hbm.at[i, pl.ds(t * TILE, TILE)], xt.at[t], xsem.at[t])

    def o_store(i, t):
        return pltpu.make_async_copy(stage.at[pl.ds(2 * t, 2)], o_hbm.at[i, pl.ds(2 * t, 2)], ssem.at[t])

    def begin(cp):
        cp.start()

    def finish(cp):
        cp.wait()

    def relay_rows(i, part=None):
        if part is None:
            received(relay.at[i], hrecv.at[i])
        else:
            received(last_relay.at[:, :, :, :, within(part)], hrecv.at[i + part])
        for color, h in both:
            pass_rows(i, color, h, part).start()

    def row_loads(i, color):
        at = pl.ds(8 * lax.rem(i, 2) + 4 * color, 4)
        srcs = [spread(color, i, 0, 0, 4)] + [rows_in.at[i, color, s] for s in range(3)]
        return [pltpu.make_async_copy(src, tok.at[at, pl.ds(s * ROW_CAP, ROW_CAP), pl.ds(0, cols)], csem.at[color]) for s, src in enumerate(srcs)]

    def rows_arrived(i, parts=(None,)):
        with scope('rows_wait'):
            for part in parts:
                if part is None:
                    received(rows_in.at[i], rrecv.at[i])
                else:
                    received(last_in.at[:, :, :, :, within(part)], rrecv.at[i + part])

    def fetch_rows(i):
        rows_arrived(i)
        for color in (0, 1):
            for cp in row_loads(i, color):
                cp.start()

    def await_rows(i):
        with scope('rowload_wait'):
            for color in (0, 1):
                ref = tok.at[pl.ds(8 * lax.rem(i, 2) + 4 * color, 4), :, pl.ds(0, cols)]
                pltpu.make_async_copy(ref, ref, csem.at[color]).wait()

    def add_rows(i, w, take, start=0, stop=8, then=None):
        def one(n, carry):
            j, color = n // 2, lax.rem(n, 2)
            m = lax.rem(2 + 3 * j + 3 * (j * (j - 1) // 2), 4)
            got = take(color, m)
            total = acc[color, m, :, w]
            for p in range(1, 4):
                g = jnp.concatenate([
                    jnp.where(tabs[color, m, s, 0, pl.ds(i, 1), :] == lanes, tabs[color, m, s, p, pl.ds(i, 1), :], 0.0).astype(BF16)
                    for s in range(4)], axis=0)
                total += lax.dot_general(g, got, (((0,), (0,)), ((), ())), preferred_element_type=F32)
            acc[color, m, :, w] = total
            if then is not None:
                then(j, color)
            return carry

        lax.fori_loop(start, stop, one, 0)

    def add_fetched(i, start=0, stop=8):
        add_rows(i, pl.ds(0, cols), lambda color, m: tok[8 * lax.rem(i, 2) + 4 * color + m, :, pl.ds(0, cols)], start, stop)

    def add_last(w, start, stop, then):
        def take(color, m):
            here = pl.ds(pl.multiple_of(color * cols + w.start, 128), w.size)
            return jnp.concatenate([stage[(1 - color) * m, color * m, :, here]] + [last_in[color, s, m, :, w] for s in range(3)], axis=0)

        add_rows(EXPERTS - 1, w, take, start, stop, then)

    def combine(i):
        fetch_rows(i)
        await_rows(i)
        add_fetched(i)

    def load_up(i):
        handed(i, (0, 1))
        load(i, 0, begin)
        load(i, 1, begin)

    def load_down(i):
        handed(i, (2,))
        load(i, 2, begin)

    def down(ws):
        def one(t, carry):
            for w in ws:
                o = jnp.dot(hbuf[t], bd[:, w], preferred_element_type=F32).astype(BF16)
                stage[pl.ds(2 * t, 2), :, :, w] = o.reshape(2, 4, ROW_CAP, o.shape[-1])
            return carry

        with scope('down'):
            lax.fori_loop(0, 2, one, 0)

    def send(i, part=None, colors=(0, 1)):
        for color in colors:
            for h in (0, 1):
                far_rows(i, color, h, part).start()
        for color in colors:
            for h in (0, 1):
                near_rows(i, color, h, part).start()

    def expert(i, carry):
        late = (i == 4) | (i == 6)
        for t in (0, 1):
            x_load(i, t).start()

        @pl.when(jnp.logical_not(late))
        def _():
            load_down(i)

        @pl.when(i == 5)
        def _():
            for part in range(PARTS):
                for q in (0, 1):
                    far_piece(q, part).start()

        @pl.when(late)
        def _():
            with scope('late_gu'):
                load_up(i)

        with scope('load_gu'):
            load(i, 0, finish)
            load(i, 1, finish)

        def up(t, carry):
            x_load(i, t).wait()
            xs = xt[t].reshape(rows, d)
            a = jnp.dot(xs, bg[...], preferred_element_type=F32)
            u = jnp.dot(xs, bu[...], preferred_element_type=F32)
            hbuf[t] = (jax.nn.silu(a) * u).astype(BF16)
            return carry

        with scope('up'):
            lax.fori_loop(0, 2, up, 0)

        @pl.when(i == 1)
        def _():
            with scope('line0'):
                line_arrived(0, (0, 1, 2))

        @pl.when((i == 0) | (i == 2) | (i == 4))
        def _():
            with scope('next_gu'):
                load_up(i + 1)

        @pl.when(i == 4)
        def _():
            with scope('line1_d'):
                line_arrived(1, (2,))

        @pl.when(i == 6)
        def _():
            with scope('far0_d'):
                far_arrived(0, (2,))

        @pl.when(i >= 1)
        def _():
            with scope('relay'):
                relay_rows(i - 1)

        @pl.when(i >= 2)
        def _():
            with scope('combine'):
                combine(i - 2)

        @pl.when(i == 1)
        def _():
            with scope('next_gu'):
                load_up(i + 1)

        @pl.when(i == 3)
        def _():
            with scope('line1_gu'):
                line_arrived(1, (0, 1))

        @pl.when(i == 5)
        def _():
            with scope('far0_gu'):
                far_arrived(0, (0, 1))

        @pl.when(late)
        def _():
            with scope('late_d'):
                load_down(i)

        with scope('load_d'):
            load(i, 2, finish)
        down([pl.ds(0, d)])
        with scope('store'):
            for t in (0, 1):
                o_store(i, t).start()
            for t in (0, 1):
                o_store(i, t).wait()
        send(i)
        return carry

    load_up(0)
    lax.fori_loop(0, EXPERTS - 1, expert, 0)

    last = EXPERTS - 1
    for t in (0, 1):
        x_load(last, t).start()
    def strip_arrived(part):
        far_strip(0, part).wait_recv()
        far_strip(1, part).wait_recv()
        hand_strip(part).start()

    def strip_arrived(part):
        with scope('strip'):
            received(strip_of(hu.at[7], c, 0, 2, part), urecv.at[part])
            hand_strip(part).start()

    def gate_half(t, carry):
        x_load(last, t).wait()
        a = jnp.dot(xt[t].reshape(rows, d), bg[...], preferred_element_type=F32)
        abuf[t] = jax.nn.silu(a)
        return carry

    with scope('last_g'):
        far_arrived(1, (0,))
    with scope('combine'):
        combine(last - 2)
    with scope('last_g'):
        hand_on(last, 0).wait_recv()
        g_load = pltpu.make_async_copy(hg.at[last], bg, wsem.at[0])
        g_load.start()
    strip_arrived(0)
    with scope('last_g'):
        g_load.wait()
    with scope('gate_half'):
        lax.fori_loop(0, 2, gate_half, 0)
    strip_arrived(1)
    with scope('relay'):
        relay_rows(last - 1)

    def piece_arrived(part):
        with scope('piece'):
            received(hd.at[7, :, piece(c, part)], grecv.at[part])
            hand_piece(part).start()

    def piece_load(color, part):
        at = piece(color, part)
        return pltpu.make_async_copy(hd.at[last, :, at], bd.at[:, at], wsem.at[color])

    for part in range(UPS):
        with scope('last_u'):
            hand_strip(part).wait_recv()
            u_load = pltpu.make_async_copy(hu.at[last, :, strip(part)], bu.at[:, strip(part)], wsem.at[1])
            u_load.start()
            u_load.wait()

        def up_half(t, carry):
            u = jnp.dot(xt[t].reshape(rows, d), bu[:, strip(part)], preferred_element_type=F32)
            hbuf[t, :, strip(part)] = (abuf[t, :, strip(part)] * u).astype(BF16)
            return carry

        with scope('up_half'):
            lax.fori_loop(0, 2, up_half, 0)
        if part + 2 < UPS:
            strip_arrived(part + 2)
    piece_arrived(0)

    first, second = sums(0), sums(1)

    def then_first(j, color):
        spread_sums(j, color, 0)

    def then_second(j, color):
        spread_sums(j, color, 1)

    def spread_sums(j, color, part):
        @pl.when(j == 0)
        def _():
            far_sum(color, 0, part).start()
            far_sum(color, 1, part).start()

        for h in (0, 1):
            @pl.when(j == 1 + h)
            def _():
                near_sum(color, h, 0, part).start()

    for step in (0, 1):
        with scope('last_d'):
            if step:
                hand_piece(0).wait_recv()
            color = c if step == 0 else 1 - c
            piece_load(color, 0).start()
            piece_load(color, 0).wait()
        if step:
            piece_arrived(1)
        down([piece(color, 0)])
        for k in (0, 1):
            @pl.when(color == k)
            def _():
                send(last, 0, (k,))

    for part in range(1, PARTS):
        with scope('last_d'):
            hand_piece(part).wait_recv()
            for color in (0, 1):
                piece_load(color, part).start()
            for color in (0, 1):
                piece_load(color, part).wait()
        down([piece(0, part), piece(1, part)])
        send(last, part)
        if part + 1 < PARTS:
            piece_arrived(part + 1)
        with scope('relay'):
            relay_rows(last, part - 1)
        with scope('between'):
            if part == 1:
                fetch_rows(last - 1)
            if part == 2:
                await_rows(last - 1)
                add_fetched(last - 1, 0, 4)
            if part == 3:
                add_fetched(last - 1, 4, 8)
    rows_arrived(last, range(FIRST))
    with scope('first_sums'):
        add_last(first, 0, 2, then_first)
    with scope('relay'):
        relay_rows(last, PARTS - 1)
    with scope('first_sums'):
        add_last(first, 2, 8, then_first)
    rows_arrived(last, range(FIRST, PARTS))
    with scope('second_sums'):
        add_last(second, 0, 8, then_second)
    for part in range(SUMS):
        for color, h in both:
            with scope('farsum_wait'):
                far_sum(color, h, part).wait_recv()
            r, w = pl.ds(h * half, half), sums(part)
            acc[color, 1 + 2 * h, r, w] = acc[color, 1 + 2 * h, r, w] + rf2[color, h, :, w]
            near_sum(color, h, 1, part).start()
    for part in range(SUMS):
        w = sums(part)
        for color in (0, 1):
            with scope('nearsum_wait'):
                received(rn2.at[color, :, :, w], n2recv.at[color, part])
            here = pl.ds(color * cols + w.start, w.size)
            out[:, here] = (acc[color, 0, :, w] + rn2[color, 0, :, w] + rn2[color, 1, :, w]).astype(out.dtype)

    sent(acc.at[:, pl.ds(1, 3)], ssend)
    for i in range(EXPERTS - 1):
        sent(o_hbm.at[i], rsend.at[i])
    sent(stage, rsend.at[last])
    for n, ref in enumerate((all_ids, all_gates)):
        sent(ref.at[pl.ds(1, BLOCKS - 1)], msend.at[n])
    for m in range(3):
        sent(held[m].at[pl.ds(0, EXPERTS - 1)], wsend.at[m])


def run_moe(hidden, ids, gates, w_gate, w_up, w_down):
    tokens, d = hidden.shape
    f = w_gate.shape[1]
    half, cols = tokens // 2, d // 2
    hbm = pl.BlockSpec(memory_space=pl.ANY)
    dma = pltpu.SemaphoreType.DMA
    flops = 2 * EXPERTS * BLOCKS * ROW_CAP * d * (3 * f + 4 * tokens)

    return pl.pallas_call(
        moe_kernel,
        in_specs=[hbm] * 6,
        out_specs=[pl.BlockSpec(memory_space=pltpu.VMEM)] + [hbm] * 7,
        out_shape=[
            pltpu.VMEM((tokens, d), BF16),
            jax.ShapeDtypeStruct((EXPERTS, 4, 4, ROW_CAP, d), BF16),
            jax.ShapeDtypeStruct((EXPERTS, BLOCKS, ROW_CAP, d), BF16),
            jax.ShapeDtypeStruct((EXPERTS, 2, 3, 4, ROW_CAP, cols), BF16),
            jax.ShapeDtypeStruct((EXPERTS, 2, 2, 2, ROW_CAP, cols), BF16),
            jax.ShapeDtypeStruct((8, d, f), BF16),
            jax.ShapeDtypeStruct((8, d, f), BF16),
            jax.ShapeDtypeStruct((8, f, d), BF16),
        ],
        scratch_shapes=[
            pltpu.VMEM((BLOCKS, tokens, d), BF16),
            pltpu.VMEM((BLOCKS,) + ids.shape, jnp.int32),
            pltpu.VMEM((BLOCKS,) + gates.shape, F32),
            pltpu.VMEM((BLOCKS, EXPERTS, tokens), F32),
            pltpu.VMEM((2, 4, 4, 4, EXPERTS, tokens), F32),
            pltpu.VMEM((2, 4, tokens, cols), F32),
            pltpu.VMEM((2, 2, half, cols), F32),
            pltpu.VMEM((2, 2, tokens, cols), F32),
            pltpu.VMEM((2, 2, 2, ROW_CAP, cols), BF16),
            pltpu.VMEM((2, 3, 4, ROW_CAP, cols), BF16),
            pltpu.VMEM((4, 4, ROW_CAP, d), BF16),
            pltpu.VMEM((2, TILE, ROW_CAP, d), BF16),
            pltpu.VMEM((2, TILE * ROW_CAP, f), F32),
            pltpu.VMEM((2, TILE * ROW_CAP, f), BF16),
            pltpu.VMEM((d, f), BF16),
            pltpu.VMEM((d, f), BF16),
            pltpu.VMEM((f, d), BF16),
            dma(()), dma((2, 5, 3)), dma((2,)), dma((2,)), dma((3,)), dma((2, 2, 3)), dma((4,)), dma((3, 2)), dma((16,)), dma((PARTS,)), dma((PARTS,)), dma((UPS,)), dma((UPS,)),
            dma((EXPERTS,)), dma((EXPERTS - 1 + PARTS,)), dma((EXPERTS - 1 + PARTS,)), dma(()), dma((2, 2, SUMS)), dma((2, SUMS)), dma((3,)), dma((2,)), dma((3,)), dma((2,)), dma((2,)),
        ],
        compiler_params=pltpu.CompilerParams(collective_id=0, has_side_effects=True, vmem_limit_bytes=62 * MIB),
        cost_estimate=pl.CostEstimate(flops=flops, bytes_accessed=400 * MIB, transcendentals=0),
        name='run_moe',
    )(hidden, ids, gates, w_gate, w_up, w_down)[0]


def solution(mesh):
    grid = Mesh(mesh.devices.reshape((mesh.shape['dp'],) + SIZES), ('dp',) + GRID)

    def body(hidden, route_idx, gate_weights, w_gate, w_up, w_down):
        return run_moe(hidden, route_idx.T, gate_weights.T, w_gate[0], w_up[0], w_down[0])

    r = P(('dp',) + GRID, None)
    e = P(GRID, None, None)
    return jax.shard_map(body, mesh=grid, in_specs=(r, r, r, e, e, e), out_specs=r, check_vma=False)
```

```python
import jax
import jax.numpy as jnp
from jax import lax
from jax.experimental import pallas as pl
from jax.experimental.pallas import tpu as pltpu
from jax.sharding import Mesh, PartitionSpec as P

BF16 = jnp.bfloat16
F32 = jnp.float32
MESH = pl.DeviceIdType.MESH
GRID = ('z', 'y', 'x', 'c')
SIZES = (4, 4, 4, 2)
ROW_CAP = 64
EXPERTS = 8
BLOCKS = 16
TILE = 8
EDGES = (0, 256, 512, 768, 1024)
PARTS = len(EDGES) - 1
SUMS = 2
FIRST = 2
OPENING = 128
UPS = 3
MIB = 1024 * 1024
scope = jax.named_scope


def expert_ids(place, x, c, line):
    dx = jnp.where((place == 2) | (place == 4), 3, 0) + jnp.where((place == 3) | (place == 5), 1, 0)
    dx += jnp.where(place >= 6, 2, 0)
    core = jnp.where(place == 0, c, 0) + jnp.where(place == 1, 1 - c, 0)
    core += jnp.where((place == 4) | (place == 5) | (place == 7), 1, 0)
    return line * EXPERTS + lax.rem(x + dx, 4) * 2 + core


def moe_kernel(hid, ids, gates, wg, wu, wd, out, o_hbm, x_hbm, rows_in, relay, hg, hu, hd,
               tok, all_ids, all_gates, slots, tabs, acc, rf2, rn2, last_relay, last_in, stage, xt, abuf, hbuf, bg, bu, bd,
               tsend, trecv, msend, mrecv, wsend, irecv, frecv, drecv, precv, grecv, qrecv, urecv, vrecv,
               rsend, rrecv, hrecv, ssend, f2recv, n2recv, lsem, ssem, wsem, xsem, csem, free):
    z, y, x, c = (lax.axis_index(a) for a in GRID)
    right, left = lax.rem(x + 1, 4), lax.rem(x + 3, 4)
    tokens, d = hid.shape
    half, cols = tokens // 2, d // 2
    rows = TILE * ROW_CAP
    own = (wg, wu, wd)
    held = (hg, hu, hd)
    partner = {'c': 1 - c}

    def remote(src, dst, send, recv, where):
        return pltpu.make_async_remote_copy(src_ref=src, dst_ref=dst, send_sem=send, recv_sem=recv, device_id=where, device_id_type=MESH)

    def received(ref, sem):
        remote(ref, ref, sem, sem, partner).wait_recv()

    def sent(ref, sem):
        remote(ref, ref, sem, sem, partner).wait_send()

    def along(dim, step):
        return {'z': lax.rem(z + (1 - dim) * step, 4), 'y': lax.rem(y + dim * step, 4)}

    def quarter(ref, m, lane, q, count=1):
        n = own[m].shape[0] // 4
        return ref.at[pl.ds(pl.multiple_of((2 * lane + q) * n, n), count * n), :]

    def line_copies(way, k, m, src, which=(0, 1)):
        n = own[m].shape[0] // 2
        cuts = (0, OPENING, n) if (k, m) == (1, 0) else (0, n)
        dst, where = held[m].at[2 + 2 * k + way], {'x': right if way == 0 else left}
        copies = []
        for j in which[:len(cuts) - 1]:
            a, b = cuts[j:j + 2]
            at = pl.ds(pl.multiple_of(c * n + a, 64), b - a)
            copies.append(remote(src.at[at, :], dst.at[at, :], wsend.at[m], irecv.at[way, k, m], where))
        return copies

    def far_copy(k, m, q):
        src, dst = held[m].at[2 + 2 * k + q], held[m].at[6 + k]
        return remote(quarter(src, m, c, q), quarter(dst, m, c, q), wsend.at[m], frecv.at[3 * k + m], {'x': right if q == 0 else left})

    def hand_own(m, n):
        lane = 1 - c if n == 0 else c
        return remote(quarter(own[m], m, lane, 0, 2), quarter(held[m].at[c], m, lane, 0, 2), wsend.at[m], drecv.at[m, n], partner)

    def hand_on(slot, m):
        ref = quarter(held[m].at[slot], m, c, 0, 2)
        return remote(ref, ref, wsend.at[m], precv.at[3 * (slot - 2) + m], partner)

    def start_line(k, m, src, which=(0, 1)):
        for way in (0, 1):
            for cp in line_copies(way, k, m, src, which):
                cp.start()

    def piece(color, part):
        return pl.ds(pl.multiple_of(color * cols + EDGES[part], 128), EDGES[part + 1] - EDGES[part])

    def far_piece(q, part):
        n = wd.shape[0] // 2
        at = pl.ds(q * n, n), piece(c, part)
        return remote(hd.at[4 + q, *at], bd.at[*at], wsend.at[2], grecv.at[part], {'x': right if q == 0 else left})

    def hand_piece(part):
        ref = bd.at[:, piece(c, part)]
        return remote(ref, ref, wsend.at[2], qrecv.at[part], partner)

    def strip(part):
        n = wu.shape[1] // UPS
        return pl.ds(part * n, n)

    def strip_of(ref, lane, q, count, part):
        n = ref.shape[0] // 4
        return ref.at[pl.ds(pl.multiple_of((2 * lane + q) * n, n), count * n), strip(part)]

    def far_strip(q, part):
        return remote(strip_of(hu.at[4 + q], c, q, 1, part), strip_of(hu.at[7], c, q, 1, part), wsend.at[1], urecv.at[part], {'x': right if q == 0 else left})

    def hand_strip(part):
        ref = strip_of(hu.at[7], c, 0, 2, part)
        return remote(ref, ref, wsend.at[1], vrecv.at[part], partner)

    def place(k, a, b):
        return a * 4 + b if k == 0 else b * 4 + a

    def part(k, a, b, h=None):
        r = pl.ds(0, tokens) if h is None else pl.ds(h * half, half)
        return tok.at[place(k, a, b), r, pl.ds(k * cols, cols)]

    def first_copy(k, way):
        sems = tsend, trecv.at[k, 4, min(way, 2)], along(k, 1 + 2 * (way % 2))
        if way < 2:
            return remote(part(k, 0, 0), part(k, 3 - 2 * way, 0), *sems)
        return remote(part(k, 7 - 2 * way, 0, way - 2), part(k, 2, 0, way - 2), *sems)

    def second_copy(k, a, way):
        sems = tsend, trecv.at[k, a, min(way, 2)], along(1 - k, 1 + 2 * (way % 2))
        if way < 2:
            return remote(part(k, a, 0), part(k, a, 3 - 2 * way), *sems)
        return remote(part(k, a, 7 - 2 * way, way - 2), part(k, a, 2, way - 2), *sems)

    def route_copies(dz, dy):
        s = ((4 - dz) % 4) * 4 + (4 - dy) % 4
        where = {'z': lax.rem(z + dz, 4), 'y': lax.rem(y + dy, 4)}
        return [remote(ref.at[0], ref.at[s], msend.at[n], mrecv.at[n], where) for n, ref in enumerate((all_ids, all_gates))]

    peers = [(dz, dy) for dz in range(4) for dy in range(4) if dz or dy]

    def spread(color, i, ring, m, n, part=None):
        ref, w = (o_hbm.at[i], pl.ds(color * cols, cols)) if part is None else (stage, piece(color, part))
        if color == 0:
            return ref.at[pl.ds(m, n), ring, :, w]
        return ref.at[ring, pl.ds(m, n), :, w]

    def landing(i, color, s, m, n, part):
        if part is None:
            return rows_in.at[i, color, s - 1, pl.ds(m, n)]
        return last_in.at[color, s - 1, pl.ds(m, n), :, within(part)]

    def halfway(i, color, h, part):
        return relay.at[i, color, h] if part is None else last_relay.at[color, h, :, :, within(part)]

    def within(part):
        return pl.ds(0, cols) if part is None else pl.ds(EDGES[part], EDGES[part + 1] - EDGES[part])

    def sums(part):
        return pl.ds(part * (cols // SUMS), cols // SUMS)

    def row_sems(send, recv, i, part, color, h):
        return send.at[i], recv.at[i if part is None else i + part], along(1 - color, 1 + 2 * h)

    def near_rows(i, color, h, part=None):
        return remote(spread(color, i, 1 + 2 * h, 0, 4, part), landing(i, color, 3 - 2 * h, 0, 4, part), *row_sems(rsend, rrecv, i, part, color, h))

    def far_rows(i, color, h, part=None):
        return remote(spread(color, i, 2, 2 * h, 2, part), halfway(i, color, h, part), *row_sems(rsend, hrecv, i, part, color, h))

    def pass_rows(i, color, h, part=None):
        return remote(halfway(i, color, h, part), landing(i, color, 2, 2 * h, 2, part), *row_sems(rsend, rrecv, i, part, color, h))

    def far_sum(color, h, part):
        r, w = pl.ds(h * half, half), sums(part)
        return remote(acc.at[color, 2, r, w], rf2.at[color, h, :, w], ssend, f2recv.at[color, h, part], along(color, 1 + 2 * h))

    def near_sum(color, h, waits, part):
        r, w = pl.ds((h if waits else 1 - h) * half, half), sums(part)
        return remote(acc.at[color, 1 + 2 * h, r, w], rn2.at[color, h, r, w], ssend, n2recv.at[color, part], along(color, 1 + 2 * h))

    both = [(color, h) for color in (0, 1) for h in (0, 1)]

    own_tok = pltpu.make_async_copy(hid, tok.at[0], lsem.at[0])
    own_tok.start()
    own_routes = [pltpu.make_async_copy(ids, all_ids.at[0], lsem.at[1]), pltpu.make_async_copy(gates, all_gates.at[0], lsem.at[2])]
    for cp in own_routes:
        cp.start()

    barrier = pltpu.get_barrier_semaphore()
    for where in [partner, {'x': right}, {'x': left}] + [{'z': lax.rem(z + dz, 4), 'y': lax.rem(y + dy, 4)} for dz, dy in peers]:
        pl.semaphore_signal(barrier, inc=1, device_id=where, device_id_type=MESH)
    pl.semaphore_wait(barrier, 3 + len(peers))

    for n in (0, 1):
        for m in range(3):
            hand_own(m, n).start()

    @pl.when(c == 0)
    def _():
        for m in range(3):
            start_line(0, m, own[m])

    @pl.when(c == 1)
    def _():
        start_line(1, 0, own[0], (0,))

    own_tok.wait()
    for k in (0, 1):
        for way in (0, 1):
            first_copy(k, way).start()
            second_copy(k, 0, way).start()
    for cp in own_routes:
        cp.wait()
    for dz, dy in peers:
        for cp in route_copies(dz, dy):
            cp.start()
    for m in range(3):
        hand_own(m, 0).wait_recv()

        @pl.when(c == 1)
        def _():
            start_line(0, m, held[m].at[0])

    for m in range(3):
        @pl.when(c == 0)
        def _():
            start_line(1, m, held[m].at[1])

        @pl.when(c == 1)
        def _():
            start_line(1, m, own[m], (1,) if m == 0 else (0,))

    for k in (0, 1):
        first_copy(k, 0).wait_recv()
        first_copy(k, 2).start()
        second_copy(k, 3, 0).start()
        second_copy(k, 3, 1).start()
        first_copy(k, 1).wait_recv()
        first_copy(k, 3).start()
        second_copy(k, 1, 0).start()
        second_copy(k, 1, 1).start()
    for k in (0, 1):
        for way in (0, 1):
            second_copy(k, 0, way).wait_recv()
            second_copy(k, 0, 2 + way).start()
    for k in (0, 1):
        received(part(k, 2, 0), trecv.at[k, 4, 2])
        second_copy(k, 2, 0).start()
        second_copy(k, 2, 1).start()

    for n, ref in enumerate((all_ids, all_gates)):
        received(ref.at[pl.ds(1, BLOCKS - 1)], mrecv.at[n])
    order = lax.broadcasted_iota(jnp.int32, (EXPERTS, tokens), 0)
    earlier = lax.broadcasted_iota(jnp.int32, (tokens, tokens), 0) < lax.broadcasted_iota(jnp.int32, (tokens, tokens), 1)
    earlier = jnp.where(earlier, 1.0, 0.0).astype(BF16)

    def table(s, line):
        mine = expert_ids(order, x, c, line)
        rec, weight = all_ids[s], all_gates[s]
        chosen = jnp.zeros((EXPERTS, tokens), F32)
        gate = jnp.zeros((EXPERTS, tokens), F32)
        for k in range(rec.shape[0]):
            hit = rec[k:k + 1, :] == mine
            chosen += jnp.where(hit, 1.0, 0.0)
            gate += jnp.where(hit, weight[k:k + 1, :], 0.0)
        rank = jnp.dot(chosen.astype(BF16), earlier, preferred_element_type=F32)
        return jnp.where(chosen > 0.5, rank, -1.0), gate

    def own_table(s, carry):
        slots[s] = table(s, z * 4 + y)[0]
        return carry

    lax.fori_loop(0, BLOCKS, own_table, 0)

    def ring_table(n, carry):
        color, m, s = n // 16, lax.rem(n // 4, 4), lax.rem(n, 4)
        line = lax.rem(z + color * s, 4) * 4 + lax.rem(y + (1 - color) * s, 4)
        slot, gate = table((4 - 3 * color) * m, line)
        tabs[color, m, s, 0] = slot
        for p in range(1, 4):
            term = (gate * (1 - 2.0 ** -8) if p == 1 else gate).astype(BF16).astype(F32)
            tabs[color, m, s, p] = term
            gate = gate - term
        return carry

    def turn(a):
        for k in (0, 1):
            for way in (0, 1):
                second_copy(k, a, way).wait_recv()
                second_copy(k, a, 2 + way).start()

    turn(3)
    turn(1)
    turn(2)
    lax.fori_loop(0, 32, ring_table, 0)
    for a in range(4):
        for k in (0, 1):
            received(part(k, a, 2), trecv.at[k, a, 2])

    def x_store(s, b):
        return pltpu.make_async_copy(stage.at[pl.ds(2 * b, 2)].reshape(EXPERTS, ROW_CAP, d), x_hbm.at[:, s], ssem.at[b])

    lanes = lax.broadcasted_iota(jnp.int32, (ROW_CAP, tokens), 0).astype(F32)

    def gather(s, carry):
        b = lax.rem(s, 2)
        pick = jnp.concatenate([jnp.where(slots[s, pl.ds(e, 1), :] == lanes, 1.0, 0.0).astype(BF16) for e in range(EXPERTS)], axis=0)
        got = jnp.dot(pick, tok[s], preferred_element_type=F32).astype(BF16)

        @pl.when(s >= 2)
        def _():
            x_store(s, b).wait()

        stage[pl.ds(2 * b, 2)] = got.reshape(2, 4, ROW_CAP, d)
        x_store(s, b).start()
        return carry

    lax.fori_loop(0, BLOCKS, gather, 0)
    acc[...] = jnp.zeros(acc.shape, F32)
    x_store(0, 0).wait()
    x_store(0, 1).wait()
    sent(tok.at[pl.ds(1, BLOCKS - 1)], tsend)

    def load(i, m, go):
        dst = (bg, bu, bd)[m]

        @pl.when(i == 0)
        def _():
            go(pltpu.make_async_copy(own[m], dst, wsem.at[m]))

        @pl.when(i == 1)
        def _():
            go(pltpu.make_async_copy(held[m].at[1 - c], dst, wsem.at[m]))

        @pl.when(i >= 2)
        def _():
            go(pltpu.make_async_copy(held[m].at[i], dst, wsem.at[m]))

    def line_arrived(k, ms):
        for m in ms:
            for way in (0, 1):
                received(quarter(held[m].at[2 + 2 * k + way], m, c, 0, 2), irecv.at[way, k, m])
                if (k, m) == (1, 1):
                    for part in range(UPS):
                        far_strip(way, part).start()
                elif (k, m) != (1, 2):
                    far_copy(k, m, way).start()
                hand_on(2 + 2 * k + way, m).start()

    def far_arrived(k, ms):
        for m in ms:
            received(quarter(held[m].at[6 + k], m, c, 0, 2), frecv.at[3 * k + m])
            hand_on(6 + k, m).start()

    def handed(i, ms):
        @pl.when(i == 1)
        def _():
            for m in ms:
                hand_own(m, 1).wait_recv()

        @pl.when(i >= 2)
        def _():
            for m in ms:
                hand_on(i, m).wait_recv()

    def x_load(i, t):
        return pltpu.make_async_copy(x_hbm.at[i, pl.ds(t * TILE, TILE)], xt.at[t], xsem.at[t])

    def o_store(i, t):
        return pltpu.make_async_copy(stage.at[pl.ds(2 * t, 2)], o_hbm.at[i, pl.ds(2 * t, 2)], ssem.at[t])

    def begin(cp):
        cp.start()

    def finish(cp):
        cp.wait()

    def relay_rows(i, part=None):
        if part is None:
            received(relay.at[i], hrecv.at[i])
        else:
            received(last_relay.at[:, :, :, :, within(part)], hrecv.at[i + part])
        for color, h in both:
            pass_rows(i, color, h, part).start()

    def row_loads(i, color):
        at = pl.ds(8 * lax.rem(i, 2) + 4 * color, 4)
        srcs = [spread(color, i, 0, 0, 4)] + [rows_in.at[i, color, s] for s in range(3)]
        return [pltpu.make_async_copy(src, tok.at[at, pl.ds(s * ROW_CAP, ROW_CAP), pl.ds(0, cols)], csem.at[color]) for s, src in enumerate(srcs)]

    def rows_arrived(i, parts=(None,)):
        with scope('rows_wait'):
            for part in parts:
                if part is None:
                    received(rows_in.at[i], rrecv.at[i])
                else:
                    received(last_in.at[:, :, :, :, within(part)], rrecv.at[i + part])

    def fetch_rows(i):
        rows_arrived(i)
        for color in (0, 1):
            for cp in row_loads(i, color):
                cp.start()

    def await_rows(i):
        with scope('rowload_wait'):
            for color in (0, 1):
                ref = tok.at[pl.ds(8 * lax.rem(i, 2) + 4 * color, 4), :, pl.ds(0, cols)]
                pltpu.make_async_copy(ref, ref, csem.at[color]).wait()

    def add_rows(i, w, take, start=0, stop=8, then=None):
        def one(n, carry):
            j, color = n // 2, lax.rem(n, 2)
            m = lax.rem(2 + 3 * j + 3 * (j * (j - 1) // 2), 4)
            got = take(color, m)
            total = acc[color, m, :, w]
            for p in range(1, 4):
                g = jnp.concatenate([
                    jnp.where(tabs[color, m, s, 0, pl.ds(i, 1), :] == lanes, tabs[color, m, s, p, pl.ds(i, 1), :], 0.0).astype(BF16)
                    for s in range(4)], axis=0)
                total += lax.dot_general(g, got, (((0,), (0,)), ((), ())), preferred_element_type=F32)
            acc[color, m, :, w] = total
            if then is not None:
                then(j, color)
            return carry

        lax.fori_loop(start, stop, one, 0)

    def add_fetched(i, start=0, stop=8):
        add_rows(i, pl.ds(0, cols), lambda color, m: tok[8 * lax.rem(i, 2) + 4 * color + m, :, pl.ds(0, cols)], start, stop)

    def add_last(w, start, stop, then):
        def take(color, m):
            here = pl.ds(pl.multiple_of(color * cols + w.start, 128), w.size)
            return jnp.concatenate([stage[(1 - color) * m, color * m, :, here]] + [last_in[color, s, m, :, w] for s in range(3)], axis=0)

        add_rows(EXPERTS - 1, w, take, start, stop, then)

    def combine(i):
        fetch_rows(i)
        await_rows(i)
        add_fetched(i)

    def load_up(i):
        handed(i, (0, 1))
        load(i, 0, begin)
        load(i, 1, begin)

    def load_down(i):
        handed(i, (2,))
        load(i, 2, begin)

    def down(ws):
        def one(t, carry):
            for w in ws:
                o = jnp.dot(hbuf[t], bd[:, w], preferred_element_type=F32).astype(BF16)
                stage[pl.ds(2 * t, 2), :, :, w] = o.reshape(2, 4, ROW_CAP, o.shape[-1])
            return carry

        with scope('down'):
            lax.fori_loop(0, 2, one, 0)

    def send(i, part=None, colors=(0, 1)):
        for color in colors:
            for h in (0, 1):
                far_rows(i, color, h, part).start()
        for color in colors:
            for h in (0, 1):
                near_rows(i, color, h, part).start()

    def expert(i, carry):
        late = (i == 4) | (i == 6)
        for t in (0, 1):
            x_load(i, t).start()

        @pl.when(jnp.logical_not(late))
        def _():
            load_down(i)


        @pl.when(late)
        def _():
            with scope('late_gu'):
                load_up(i)

        with scope('load_gu'):
            load(i, 0, finish)
            load(i, 1, finish)

        def up(t, carry):
            x_load(i, t).wait()
            xs = xt[t].reshape(rows, d)
            a = jnp.dot(xs, bg[...], preferred_element_type=F32)
            u = jnp.dot(xs, bu[...], preferred_element_type=F32)
            hbuf[t] = (jax.nn.silu(a) * u).astype(BF16)
            return carry

        with scope('up'):
            lax.fori_loop(0, 2, up, 0)

        @pl.when(i == 1)
        def _():
            with scope('line0'):
                line_arrived(0, (0, 1, 2))

        @pl.when((i == 0) | (i == 2) | (i == 4))
        def _():
            with scope('next_gu'):
                load_up(i + 1)

        @pl.when(i == 4)
        def _():
            with scope('line1_d'):
                line_arrived(1, (2,))

        @pl.when(i == 6)
        def _():
            with scope('far0_d'):
                far_arrived(0, (2,))

        @pl.when(i >= 1)
        def _():
            with scope('relay'):
                relay_rows(i - 1)

        @pl.when(i >= 2)
        def _():
            with scope('combine'):
                combine(i - 2)

        @pl.when(i == 1)
        def _():
            with scope('next_gu'):
                load_up(i + 1)

        @pl.when(i == 3)
        def _():
            with scope('line1_gu'):
                line_arrived(1, (0, 1))

        @pl.when(i == 5)
        def _():
            with scope('far0_gu'):
                far_arrived(0, (0, 1))

        @pl.when(late)
        def _():
            with scope('late_d'):
                load_down(i)

        with scope('load_d'):
            load(i, 2, finish)
        down([pl.ds(0, d)])
        with scope('store'):
            for t in (0, 1):
                o_store(i, t).start()
            for t in (0, 1):
                o_store(i, t).wait()
        send(i)
        return carry

    load_up(0)
    lax.fori_loop(0, EXPERTS - 1, expert, 0)

    last = EXPERTS - 1
    for t in (0, 1):
        x_load(last, t).start()
    for where in (partner, {'x': right}, {'x': left}):
        pl.semaphore_signal(free, inc=1, device_id=where, device_id_type=MESH)
    with scope('free'):
        pl.semaphore_wait(free, 3)
    for part in range(PARTS):
        for q in (0, 1):
            far_piece(q, part).start()
    def strip_arrived(part):
        far_strip(0, part).wait_recv()
        far_strip(1, part).wait_recv()
        hand_strip(part).start()

    def strip_arrived(part):
        with scope('strip'):
            received(strip_of(hu.at[7], c, 0, 2, part), urecv.at[part])
            hand_strip(part).start()

    def gate_half(t, carry):
        x_load(last, t).wait()
        a = jnp.dot(xt[t].reshape(rows, d), bg[...], preferred_element_type=F32)
        abuf[t] = jax.nn.silu(a)
        return carry

    with scope('last_g'):
        far_arrived(1, (0,))
    with scope('combine'):
        combine(last - 2)
    with scope('last_g'):
        hand_on(last, 0).wait_recv()
        g_load = pltpu.make_async_copy(hg.at[last], bg, wsem.at[0])
        g_load.start()
    strip_arrived(0)
    with scope('last_g'):
        g_load.wait()
    with scope('gate_half'):
        lax.fori_loop(0, 2, gate_half, 0)
    strip_arrived(1)
    with scope('relay'):
        relay_rows(last - 1)

    def piece_arrived(part):
        with scope('piece'):
            received(bd.at[:, piece(c, part)], grecv.at[part])
            hand_piece(part).start()

    for part in range(UPS):
        with scope('last_u'):
            hand_strip(part).wait_recv()
            u_load = pltpu.make_async_copy(hu.at[last, :, strip(part)], bu.at[:, strip(part)], wsem.at[1])
            u_load.start()
            u_load.wait()

        def up_half(t, carry):
            u = jnp.dot(xt[t].reshape(rows, d), bu[:, strip(part)], preferred_element_type=F32)
            hbuf[t, :, strip(part)] = (abuf[t, :, strip(part)] * u).astype(BF16)
            return carry

        with scope('up_half'):
            lax.fori_loop(0, 2, up_half, 0)
        if 1 <= part < UPS - 1:
            strip_arrived(part + 1)
    piece_arrived(0)

    first, second = sums(0), sums(1)

    def then_first(j, color):
        spread_sums(j, color, 0)

    def then_second(j, color):
        spread_sums(j, color, 1)

    def spread_sums(j, color, part):
        @pl.when(j == 0)
        def _():
            far_sum(color, 0, part).start()
            far_sum(color, 1, part).start()

        for h in (0, 1):
            @pl.when(j == 1 + h)
            def _():
                near_sum(color, h, 0, part).start()

    for step in (0, 1):
        color = c if step == 0 else 1 - c
        if step:
            with scope('last_d'):
                hand_piece(0).wait_recv()
        down([piece(color, 0)])
        for k in (0, 1):
            @pl.when(color == k)
            def _():
                send(last, 0, (k,))
    piece_arrived(1)

    for part in range(1, PARTS):
        with scope('last_d'):
            hand_piece(part).wait_recv()
        down([piece(0, part), piece(1, part)])
        send(last, part)
        if part + 1 < PARTS:
            piece_arrived(part + 1)
        with scope('relay'):
            relay_rows(last, part - 1)
        with scope('between'):
            if part == 1:
                fetch_rows(last - 1)
            if part == 2:
                await_rows(last - 1)
                add_fetched(last - 1, 0, 4)
            if part == 3:
                add_fetched(last - 1, 4, 8)
    rows_arrived(last, range(FIRST))
    with scope('first_sums'):
        add_last(first, 0, 2, then_first)
    with scope('relay'):
        relay_rows(last, PARTS - 1)
    with scope('first_sums'):
        add_last(first, 2, 8, then_first)
    rows_arrived(last, range(FIRST, PARTS))
    with scope('second_sums'):
        add_last(second, 0, 8, then_second)
    for part in range(SUMS):
        for color, h in both:
            with scope('farsum_wait'):
                far_sum(color, h, part).wait_recv()
            r, w = pl.ds(h * half, half), sums(part)
            acc[color, 1 + 2 * h, r, w] = acc[color, 1 + 2 * h, r, w] + rf2[color, h, :, w]
            near_sum(color, h, 1, part).start()
    for part in range(SUMS):
        w = sums(part)
        for color in (0, 1):
            with scope('nearsum_wait'):
                received(rn2.at[color, :, :, w], n2recv.at[color, part])
            here = pl.ds(color * cols + w.start, w.size)
            out[:, here] = (acc[color, 0, :, w] + rn2[color, 0, :, w] + rn2[color, 1, :, w]).astype(out.dtype)

    sent(acc.at[:, pl.ds(1, 3)], ssend)
    for i in range(EXPERTS - 1):
        sent(o_hbm.at[i], rsend.at[i])
    sent(stage, rsend.at[last])
    for n, ref in enumerate((all_ids, all_gates)):
        sent(ref.at[pl.ds(1, BLOCKS - 1)], msend.at[n])
    for m in range(3):
        sent(held[m].at[pl.ds(0, EXPERTS - 1)], wsend.at[m])


def run_moe(hidden, ids, gates, w_gate, w_up, w_down):
    tokens, d = hidden.shape
    f = w_gate.shape[1]
    half, cols = tokens // 2, d // 2
    hbm = pl.BlockSpec(memory_space=pl.ANY)
    dma = pltpu.SemaphoreType.DMA
    flops = 2 * EXPERTS * BLOCKS * ROW_CAP * d * (3 * f + 4 * tokens)

    return pl.pallas_call(
        moe_kernel,
        in_specs=[hbm] * 6,
        out_specs=[pl.BlockSpec(memory_space=pltpu.VMEM)] + [hbm] * 7,
        out_shape=[
            pltpu.VMEM((tokens, d), BF16),
            jax.ShapeDtypeStruct((EXPERTS, 4, 4, ROW_CAP, d), BF16),
            jax.ShapeDtypeStruct((EXPERTS, BLOCKS, ROW_CAP, d), BF16),
            jax.ShapeDtypeStruct((EXPERTS, 2, 3, 4, ROW_CAP, cols), BF16),
            jax.ShapeDtypeStruct((EXPERTS, 2, 2, 2, ROW_CAP, cols), BF16),
            jax.ShapeDtypeStruct((8, d, f), BF16),
            jax.ShapeDtypeStruct((8, d, f), BF16),
            jax.ShapeDtypeStruct((8, f, d), BF16),
        ],
        scratch_shapes=[
            pltpu.VMEM((BLOCKS, tokens, d), BF16),
            pltpu.VMEM((BLOCKS,) + ids.shape, jnp.int32),
            pltpu.VMEM((BLOCKS,) + gates.shape, F32),
            pltpu.VMEM((BLOCKS, EXPERTS, tokens), F32),
            pltpu.VMEM((2, 4, 4, 4, EXPERTS, tokens), F32),
            pltpu.VMEM((2, 4, tokens, cols), F32),
            pltpu.VMEM((2, 2, half, cols), F32),
            pltpu.VMEM((2, 2, tokens, cols), F32),
            pltpu.VMEM((2, 2, 2, ROW_CAP, cols), BF16),
            pltpu.VMEM((2, 3, 4, ROW_CAP, cols), BF16),
            pltpu.VMEM((4, 4, ROW_CAP, d), BF16),
            pltpu.VMEM((2, TILE, ROW_CAP, d), BF16),
            pltpu.VMEM((2, TILE * ROW_CAP, f), F32),
            pltpu.VMEM((2, TILE * ROW_CAP, f), BF16),
            pltpu.VMEM((d, f), BF16),
            pltpu.VMEM((d, f), BF16),
            pltpu.VMEM((f, d), BF16),
            dma(()), dma((2, 5, 3)), dma((2,)), dma((2,)), dma((3,)), dma((2, 2, 3)), dma((4,)), dma((3, 2)), dma((16,)), dma((PARTS,)), dma((PARTS,)), dma((UPS,)), dma((UPS,)),
            dma((EXPERTS,)), dma((EXPERTS - 1 + PARTS,)), dma((EXPERTS - 1 + PARTS,)), dma(()), dma((2, 2, SUMS)), dma((2, SUMS)), dma((3,)), dma((2,)), dma((3,)), dma((2,)), dma((2,)), pltpu.SemaphoreType.REGULAR,
        ],
        compiler_params=pltpu.CompilerParams(collective_id=0, has_side_effects=True, vmem_limit_bytes=62 * MIB),
        cost_estimate=pl.CostEstimate(flops=flops, bytes_accessed=400 * MIB, transcendentals=0),
        name='run_moe',
    )(hidden, ids, gates, w_gate, w_up, w_down)[0]


def solution(mesh):
    grid = Mesh(mesh.devices.reshape((mesh.shape['dp'],) + SIZES), ('dp',) + GRID)

    def body(hidden, route_idx, gate_weights, w_gate, w_up, w_down):
        return run_moe(hidden, route_idx.T, gate_weights.T, w_gate[0], w_up[0], w_down[0])

    r = P(('dp',) + GRID, None)
    e = P(GRID, None, None)
    return jax.shard_map(body, mesh=grid, in_specs=(r, r, r, e, e, e), out_specs=r, check_vma=False)
```

```python
import jax
import jax.numpy as jnp
from jax import lax
from jax.experimental import pallas as pl
from jax.experimental.pallas import tpu as pltpu
from jax.sharding import Mesh, PartitionSpec as P

BF16 = jnp.bfloat16
F32 = jnp.float32
MESH = pl.DeviceIdType.MESH
GRID = ('z', 'y', 'x', 'c')
SIZES = (4, 4, 4, 2)
ROW_CAP = 64
EXPERTS = 8
BLOCKS = 16
TILE = 8
EDGES = (0, 128, 256, 512, 768, 1024)
PARTS = len(EDGES) - 1
SUMS = 2
FIRST = 3
OPENING = 128
UPS = 3
MIB = 1024 * 1024
scope = jax.named_scope


def expert_ids(place, x, c, line):
    dx = jnp.where((place == 2) | (place == 4), 3, 0) + jnp.where((place == 3) | (place == 5), 1, 0)
    dx += jnp.where(place >= 6, 2, 0)
    core = jnp.where(place == 0, c, 0) + jnp.where(place == 1, 1 - c, 0)
    core += jnp.where((place == 4) | (place == 5) | (place == 7), 1, 0)
    return line * EXPERTS + lax.rem(x + dx, 4) * 2 + core


def moe_kernel(hid, ids, gates, wg, wu, wd, out, o_hbm, x_hbm, rows_in, relay, hg, hu, hd,
               tok, all_ids, all_gates, slots, tabs, acc, rf2, rn2, last_relay, last_in, stage, xt, abuf, hbuf, bg, bu, bd,
               tsend, trecv, msend, mrecv, wsend, irecv, frecv, drecv, precv, grecv, qrecv, urecv, vrecv,
               rsend, rrecv, hrecv, ssend, f2recv, n2recv, lsem, ssem, wsem, xsem, csem, up_free, down_free):
    z, y, x, c = (lax.axis_index(a) for a in GRID)
    right, left = lax.rem(x + 1, 4), lax.rem(x + 3, 4)
    tokens, d = hid.shape
    half, cols = tokens // 2, d // 2
    rows = TILE * ROW_CAP
    own = (wg, wu, wd)
    held = (hg, hu, hd)
    partner = {'c': 1 - c}

    def remote(src, dst, send, recv, where):
        return pltpu.make_async_remote_copy(src_ref=src, dst_ref=dst, send_sem=send, recv_sem=recv, device_id=where, device_id_type=MESH)

    def received(ref, sem):
        remote(ref, ref, sem, sem, partner).wait_recv()

    def sent(ref, sem):
        remote(ref, ref, sem, sem, partner).wait_send()

    def along(dim, step):
        return {'z': lax.rem(z + (1 - dim) * step, 4), 'y': lax.rem(y + dim * step, 4)}

    def quarter(ref, m, lane, q, count=1):
        n = own[m].shape[0] // 4
        return ref.at[pl.ds(pl.multiple_of((2 * lane + q) * n, n), count * n), :]

    def line_copies(way, k, m, src, which=(0, 1)):
        n = own[m].shape[0] // 2
        cuts = (0, OPENING, n) if (k, m) == (1, 0) else (0, n)
        dst, where = held[m].at[2 + 2 * k + way], {'x': right if way == 0 else left}
        copies = []
        for j in which[:len(cuts) - 1]:
            a, b = cuts[j:j + 2]
            at = pl.ds(pl.multiple_of(c * n + a, 64), b - a)
            copies.append(remote(src.at[at, :], dst.at[at, :], wsend.at[m], irecv.at[k, m], where))
        return copies

    def far_copy(k, m, q):
        src, dst = held[m].at[2 + 2 * k + q], held[m].at[6 + k]
        return remote(quarter(src, m, c, q), quarter(dst, m, c, q), wsend.at[m], frecv.at[3 * k + m], {'x': right if q == 0 else left})

    def hand_own(m, n):
        lane = 1 - c if n == 0 else c
        return remote(quarter(own[m], m, lane, 0, 2), quarter(held[m].at[c], m, lane, 0, 2), wsend.at[m], drecv.at[m, n], partner)

    def hand_on(slot, m):
        ref = quarter(held[m].at[slot], m, c, 0, 2)
        return remote(ref, ref, wsend.at[m], precv.at[2 * (slot - 2) + m // 2], partner)

    def start_line(k, m, src, which=(0, 1)):
        for way in (0, 1):
            for cp in line_copies(way, k, m, src, which):
                cp.start()

    def piece(color, part):
        return pl.ds(pl.multiple_of(color * cols + EDGES[part], 128), EDGES[part + 1] - EDGES[part])

    def far_piece(q, part):
        n = wd.shape[0] // 2
        at = pl.ds(q * n, n), piece(c, part)
        return remote(hd.at[4 + q, *at], bd.at[*at], wsend.at[2], grecv.at[part], {'x': right if q == 0 else left})

    def hand_piece(part):
        ref = bd.at[:, piece(c, part)]
        return remote(ref, ref, wsend.at[2], qrecv.at[part], partner)

    def strip(part):
        n = wu.shape[1] // UPS
        return pl.ds(part * n, n)

    def strip_of(ref, lane, q, count, part):
        n = ref.shape[0] // 4
        return ref.at[pl.ds(pl.multiple_of((2 * lane + q) * n, n), count * n), strip(part)]

    def far_strip(q, part):
        return remote(strip_of(hu.at[4 + q], c, q, 1, part), strip_of(bu, c, q, 1, part), wsend.at[1], urecv.at[part], {'x': right if q == 0 else left})

    def hand_strip(part):
        ref = strip_of(bu, c, 0, 2, part)
        return remote(ref, ref, wsend.at[1], vrecv.at[part], partner)

    def place(k, a, b):
        return a * 4 + b if k == 0 else b * 4 + a

    def part(k, a, b, h=None):
        r = pl.ds(0, tokens) if h is None else pl.ds(h * half, half)
        return tok.at[place(k, a, b), r, pl.ds(k * cols, cols)]

    def first_copy(k, way):
        sems = tsend, trecv.at[4, way // 2], along(k, 1 + 2 * (way % 2))
        if way < 2:
            return remote(part(k, 0, 0), part(k, 3 - 2 * way, 0), *sems)
        return remote(part(k, 7 - 2 * way, 0, way - 2), part(k, 2, 0, way - 2), *sems)

    def second_copy(k, a, way):
        sems = tsend, trecv.at[a, way // 2], along(1 - k, 1 + 2 * (way % 2))
        if way < 2:
            return remote(part(k, a, 0), part(k, a, 3 - 2 * way), *sems)
        return remote(part(k, a, 7 - 2 * way, way - 2), part(k, a, 2, way - 2), *sems)

    def route_copies(dz, dy):
        s = ((4 - dz) % 4) * 4 + (4 - dy) % 4
        where = {'z': lax.rem(z + dz, 4), 'y': lax.rem(y + dy, 4)}
        return [remote(ref.at[0], ref.at[s], msend.at[n], mrecv.at[n], where) for n, ref in enumerate((all_ids, all_gates))]

    peers = [(dz, dy) for dz in range(4) for dy in range(4) if dz or dy]

    def spread(color, i, ring, m, n, part=None):
        ref, w = (o_hbm.at[i], pl.ds(color * cols, cols)) if part is None else (stage, piece(color, part))
        if color == 0:
            return ref.at[pl.ds(m, n), ring, :, w]
        return ref.at[ring, pl.ds(m, n), :, w]

    def landing(i, color, s, m, n, part):
        if part is None:
            return rows_in.at[i, color, s - 1, pl.ds(m, n)]
        return last_in.at[color, s - 1, pl.ds(m, n), :, within(part)]

    def halfway(i, color, h, part):
        return relay.at[i, color, h] if part is None else last_relay.at[color, h, :, :, within(part)]

    def within(part):
        return pl.ds(0, cols) if part is None else pl.ds(EDGES[part], EDGES[part + 1] - EDGES[part])

    def sums(part):
        return pl.ds(part * (cols // SUMS), cols // SUMS)

    def row_sems(send, recv, i, part, color, h):
        return send, recv.at[i if part is None else i + part], along(1 - color, 1 + 2 * h)

    def near_rows(i, color, h, part=None):
        return remote(spread(color, i, 1 + 2 * h, 0, 4, part), landing(i, color, 3 - 2 * h, 0, 4, part), *row_sems(rsend, rrecv, i, part, color, h))

    def far_rows(i, color, h, part=None):
        return remote(spread(color, i, 2, 2 * h, 2, part), halfway(i, color, h, part), *row_sems(rsend, hrecv, i, part, color, h))

    def pass_rows(i, color, h, part=None):
        return remote(halfway(i, color, h, part), landing(i, color, 2, 2 * h, 2, part), *row_sems(rsend, rrecv, i, part, color, h))

    def far_sum(color, h, part):
        r, w = pl.ds(h * half, half), sums(part)
        return remote(acc.at[color, 2, r, w], rf2.at[color, h, :, w], ssend, f2recv.at[color, part], along(color, 1 + 2 * h))

    def near_sum(color, h, waits, part):
        r, w = pl.ds((h if waits else 1 - h) * half, half), sums(part)
        return remote(acc.at[color, 1 + 2 * h, r, w], rn2.at[color, h, r, w], ssend, n2recv.at[color, part], along(color, 1 + 2 * h))

    both = [(color, h) for color in (0, 1) for h in (0, 1)]

    own_tok = pltpu.make_async_copy(hid, tok.at[0], lsem.at[0])
    own_tok.start()
    own_routes = [pltpu.make_async_copy(ids, all_ids.at[0], lsem.at[1]), pltpu.make_async_copy(gates, all_gates.at[0], lsem.at[2])]
    for cp in own_routes:
        cp.start()

    barrier = pltpu.get_barrier_semaphore()
    for where in [partner, {'x': right}, {'x': left}] + [{'z': lax.rem(z + dz, 4), 'y': lax.rem(y + dy, 4)} for dz, dy in peers]:
        pl.semaphore_signal(barrier, inc=1, device_id=where, device_id_type=MESH)
    pl.semaphore_wait(barrier, 3 + len(peers))

    for n in (0, 1):
        for m in range(3):
            hand_own(m, n).start()

    @pl.when(c == 0)
    def _():
        for m in range(3):
            start_line(0, m, own[m])

    @pl.when(c == 1)
    def _():
        start_line(1, 0, own[0], (0,))

    own_tok.wait()
    for k in (0, 1):
        for way in (0, 1):
            first_copy(k, way).start()
            second_copy(k, 0, way).start()
    for cp in own_routes:
        cp.wait()
    for dz, dy in peers:
        for cp in route_copies(dz, dy):
            cp.start()
    for m in range(3):
        hand_own(m, 0).wait_recv()

        @pl.when(c == 1)
        def _():
            start_line(0, m, held[m].at[0])

    for m in range(3):
        @pl.when(c == 0)
        def _():
            start_line(1, m, held[m].at[1])

        @pl.when(c == 1)
        def _():
            start_line(1, m, own[m], (1,) if m == 0 else (0,))

    def tokens_arrived(a, late):
        received(tok.at[pl.ds(0, 1 if late else 2)], trecv.at[a, late])

    tokens_arrived(4, 0)
    for k in (0, 1):
        for way in (0, 1):
            first_copy(k, 2 + way).start()
            second_copy(k, 3, way).start()
            second_copy(k, 1, way).start()
    tokens_arrived(0, 0)
    for k in (0, 1):
        for way in (0, 1):
            second_copy(k, 0, 2 + way).start()
    tokens_arrived(4, 1)
    for k in (0, 1):
        for way in (0, 1):
            second_copy(k, 2, way).start()

    for n, ref in enumerate((all_ids, all_gates)):
        received(ref.at[pl.ds(1, BLOCKS - 1)], mrecv.at[n])
    order = lax.broadcasted_iota(jnp.int32, (EXPERTS, tokens), 0)
    earlier = lax.broadcasted_iota(jnp.int32, (tokens, tokens), 0) < lax.broadcasted_iota(jnp.int32, (tokens, tokens), 1)
    earlier = jnp.where(earlier, 1.0, 0.0).astype(BF16)

    def table(s, line):
        mine = expert_ids(order, x, c, line)
        rec, weight = all_ids[s], all_gates[s]
        chosen = jnp.zeros((EXPERTS, tokens), F32)
        gate = jnp.zeros((EXPERTS, tokens), F32)
        for k in range(rec.shape[0]):
            hit = rec[k:k + 1, :] == mine
            chosen += jnp.where(hit, 1.0, 0.0)
            gate += jnp.where(hit, weight[k:k + 1, :], 0.0)
        rank = jnp.dot(chosen.astype(BF16), earlier, preferred_element_type=F32)
        return jnp.where(chosen > 0.5, rank, -1.0), gate

    def own_table(s, carry):
        slots[s] = table(s, z * 4 + y)[0]
        return carry

    lax.fori_loop(0, BLOCKS, own_table, 0)

    def ring_table(n, carry):
        color, m, s = n // 16, lax.rem(n // 4, 4), lax.rem(n, 4)
        line = lax.rem(z + color * s, 4) * 4 + lax.rem(y + (1 - color) * s, 4)
        slot, gate = table((4 - 3 * color) * m, line)
        tabs[color, m, s, 0] = slot
        for p in range(1, 4):
            term = (gate * (1 - 2.0 ** -8) if p == 1 else gate).astype(BF16).astype(F32)
            tabs[color, m, s, p] = term
            gate = gate - term
        return carry

    def turn(a):
        tokens_arrived(a, 0)
        for k in (0, 1):
            for way in (0, 1):
                second_copy(k, a, 2 + way).start()

    turn(3)
    turn(1)
    turn(2)
    lax.fori_loop(0, 32, ring_table, 0)
    for a in range(4):
        tokens_arrived(a, 1)

    def x_store(s, b):
        return pltpu.make_async_copy(stage.at[pl.ds(2 * b, 2)].reshape(EXPERTS, ROW_CAP, d), x_hbm.at[:, s], ssem.at[b])

    lanes = lax.broadcasted_iota(jnp.int32, (ROW_CAP, tokens), 0).astype(F32)

    def gather(s, carry):
        b = lax.rem(s, 2)
        pick = jnp.concatenate([jnp.where(slots[s, pl.ds(e, 1), :] == lanes, 1.0, 0.0).astype(BF16) for e in range(EXPERTS)], axis=0)
        got = jnp.dot(pick, tok[s], preferred_element_type=F32).astype(BF16)

        @pl.when(s >= 2)
        def _():
            x_store(s, b).wait()

        stage[pl.ds(2 * b, 2)] = got.reshape(2, 4, ROW_CAP, d)
        x_store(s, b).start()
        return carry

    lax.fori_loop(0, BLOCKS, gather, 0)
    acc[...] = jnp.zeros(acc.shape, F32)
    x_store(0, 0).wait()
    x_store(0, 1).wait()
    sent(tok.at[pl.ds(1, BLOCKS - 1)], tsend)

    def load(i, m, go):
        dst = (bg, bu, bd)[m]

        @pl.when(i == 0)
        def _():
            go(pltpu.make_async_copy(own[m], dst, wsem.at[m]))

        @pl.when(i == 1)
        def _():
            go(pltpu.make_async_copy(held[m].at[1 - c], dst, wsem.at[m]))

        @pl.when(i >= 2)
        def _():
            go(pltpu.make_async_copy(held[m].at[i], dst, wsem.at[m]))

    def line_arrived(k, ms):
        for m in ms:
            received(held[m].at[0], irecv.at[k, m])
            for way in (0, 1):
                if k == 0 or m == 0:
                    far_copy(k, m, way).start()
                hand_on(2 + 2 * k + way, m).start()

    def far_arrived(k, ms):
        for m in ms:
            received(quarter(held[m].at[6 + k], m, c, 0, 2), frecv.at[3 * k + m])
            hand_on(6 + k, m).start()

    def handed(i, ms):
        @pl.when(i == 1)
        def _():
            for m in ms:
                hand_own(m, 1).wait_recv()

        @pl.when(i >= 2)
        def _():
            if ms == (2,):
                hand_on(i, 2).wait_recv()
            else:
                received(held[0].at[0], precv.at[2 * (i - 2)])

    def x_load(i, t):
        return pltpu.make_async_copy(x_hbm.at[i, pl.ds(t * TILE, TILE)], xt.at[t], xsem.at[t])

    def o_store(i, t):
        return pltpu.make_async_copy(stage.at[pl.ds(2 * t, 2)], o_hbm.at[i, pl.ds(2 * t, 2)], ssem.at[t])

    def begin(cp):
        cp.start()

    def finish(cp):
        cp.wait()

    def relay_rows(i, part=None):
        if part is None:
            received(relay.at[i], hrecv.at[i])
        else:
            received(last_relay.at[:, :, :, :, within(part)], hrecv.at[i + part])
        for color, h in both:
            pass_rows(i, color, h, part).start()

    def row_loads(i, color):
        at = pl.ds(8 * lax.rem(i, 2) + 4 * color, 4)
        srcs = [spread(color, i, 0, 0, 4)] + [rows_in.at[i, color, s] for s in range(3)]
        return [pltpu.make_async_copy(src, tok.at[at, pl.ds(s * ROW_CAP, ROW_CAP), pl.ds(0, cols)], csem.at[color]) for s, src in enumerate(srcs)]

    def rows_arrived(i, parts=(None,)):
        with scope('rows_wait'):
            for part in parts:
                if part is None:
                    received(rows_in.at[i], rrecv.at[i])
                else:
                    received(last_in.at[:, :, :, :, within(part)], rrecv.at[i + part])

    def fetch_rows(i):
        rows_arrived(i)
        for color in (0, 1):
            for cp in row_loads(i, color):
                cp.start()

    def await_rows(i):
        with scope('rowload_wait'):
            for color in (0, 1):
                ref = tok.at[pl.ds(8 * lax.rem(i, 2) + 4 * color, 4), :, pl.ds(0, cols)]
                pltpu.make_async_copy(ref, ref, csem.at[color]).wait()

    def add_rows(i, w, take, start=0, stop=8, then=None):
        def one(n, carry):
            j, color = n // 2, lax.rem(n, 2)
            m = lax.rem(2 + 3 * j + 3 * (j * (j - 1) // 2), 4)
            got = take(color, m)
            total = acc[color, m, :, w]
            for p in range(1, 4):
                g = jnp.concatenate([
                    jnp.where(tabs[color, m, s, 0, pl.ds(i, 1), :] == lanes, tabs[color, m, s, p, pl.ds(i, 1), :], 0.0).astype(BF16)
                    for s in range(4)], axis=0)
                total += lax.dot_general(g, got, (((0,), (0,)), ((), ())), preferred_element_type=F32)
            acc[color, m, :, w] = total
            if then is not None:
                then(j, color)
            return carry

        lax.fori_loop(start, stop, one, 0)

    def add_fetched(i, start=0, stop=8):
        add_rows(i, pl.ds(0, cols), lambda color, m: tok[8 * lax.rem(i, 2) + 4 * color + m, :, pl.ds(0, cols)], start, stop)

    def add_last(w, start, stop, then):
        def take(color, m):
            here = pl.ds(pl.multiple_of(color * cols + w.start, 128), w.size)
            return jnp.concatenate([stage[(1 - color) * m, color * m, :, here]] + [last_in[color, s, m, :, w] for s in range(3)], axis=0)

        add_rows(EXPERTS - 1, w, take, start, stop, then)

    def combine(i):
        fetch_rows(i)
        await_rows(i)
        add_fetched(i)

    def load_up(i):
        handed(i, (0, 1))
        load(i, 0, begin)
        load(i, 1, begin)

    def load_down(i):
        handed(i, (2,))
        load(i, 2, begin)

    def down(ws):
        def one(t, carry):
            for w in ws:
                o = jnp.dot(hbuf[t], bd[:, w], preferred_element_type=F32).astype(BF16)
                stage[pl.ds(2 * t, 2), :, :, w] = o.reshape(2, 4, ROW_CAP, o.shape[-1])
            return carry

        with scope('down'):
            lax.fori_loop(0, 2, one, 0)

    def send(i, part=None, colors=(0, 1)):
        for color in colors:
            for h in (0, 1):
                far_rows(i, color, h, part).start()
        for color in colors:
            for h in (0, 1):
                near_rows(i, color, h, part).start()

    def release(sem):
        for where in (partner, {'x': right}, {'x': left}):
            pl.semaphore_signal(sem, inc=1, device_id=where, device_id_type=MESH)

    def expert(i, carry):
        late = (i == 4) | (i == 6)
        for t in (0, 1):
            x_load(i, t).start()

        @pl.when(jnp.logical_not(late))
        def _():
            load_down(i)


        @pl.when(late)
        def _():
            with scope('late_gu'):
                load_up(i)

        with scope('load_gu'):
            load(i, 0, finish)
            load(i, 1, finish)

        def up(t, carry):
            x_load(i, t).wait()
            xs = xt[t].reshape(rows, d)
            a = jnp.dot(xs, bg[...], preferred_element_type=F32)
            u = jnp.dot(xs, bu[...], preferred_element_type=F32)
            hbuf[t] = (jax.nn.silu(a) * u).astype(BF16)
            return carry

        with scope('up'):
            lax.fori_loop(0, 2, up, 0)

        @pl.when(i == 1)
        def _():
            with scope('line0'):
                line_arrived(0, (0, 1, 2))

        @pl.when(i == 6)
        def _():
            release(up_free)

        @pl.when((i == 0) | (i == 2) | (i == 4))
        def _():
            with scope('next_gu'):
                load_up(i + 1)

        @pl.when(i == 4)
        def _():
            with scope('line1_d'):
                line_arrived(1, (2,))

        @pl.when(i == 6)
        def _():
            with scope('far0_d'):
                far_arrived(0, (2,))

        @pl.when(i >= 1)
        def _():
            with scope('relay'):
                relay_rows(i - 1)

        @pl.when(i >= 2)
        def _():
            with scope('combine'):
                combine(i - 2)

        @pl.when(i == 1)
        def _():
            with scope('next_gu'):
                load_up(i + 1)

        @pl.when(i == 3)
        def _():
            with scope('line1_gu'):
                line_arrived(1, (0, 1))

        @pl.when(i == 5)
        def _():
            with scope('far0_gu'):
                far_arrived(0, (0, 1))

        @pl.when(i == 6)
        def _():
            pl.semaphore_wait(up_free, 3)
            for part in range(UPS):
                for q in (0, 1):
                    far_strip(q, part).start()

        @pl.when(late)
        def _():
            with scope('late_d'):
                load_down(i)

        with scope('load_d'):
            load(i, 2, finish)
        down([pl.ds(0, d)])
        with scope('store'):
            for t in (0, 1):
                o_store(i, t).start()
            for t in (0, 1):
                o_store(i, t).wait()
        send(i)
        return carry

    load_up(0)
    lax.fori_loop(0, EXPERTS - 1, expert, 0)

    last = EXPERTS - 1
    for t in (0, 1):
        x_load(last, t).start()
    release(down_free)
    pl.semaphore_wait(down_free, 3)
    for part in range(PARTS):
        for q in (0, 1):
            far_piece(q, part).start()
    def strip_arrived(part):
        far_strip(0, part).wait_recv()
        far_strip(1, part).wait_recv()
        hand_strip(part).start()

    def strip_arrived(part):
        with scope('strip'):
            received(strip_of(bu, c, 0, 2, part), urecv.at[part])
            hand_strip(part).start()

    def gate_half(t, carry):
        x_load(last, t).wait()
        a = jnp.dot(xt[t].reshape(rows, d), bg[...], preferred_element_type=F32)
        abuf[t] = jax.nn.silu(a)
        return carry

    with scope('last_g'):
        far_arrived(1, (0,))
    with scope('combine'):
        combine(last - 2)
    with scope('last_g'):
        hand_on(last, 0).wait_recv()
        g_load = pltpu.make_async_copy(hg.at[last], bg, wsem.at[0])
        g_load.start()
    strip_arrived(0)
    with scope('last_g'):
        g_load.wait()
    with scope('gate_half'):
        lax.fori_loop(0, 2, gate_half, 0)
    strip_arrived(1)
    with scope('relay'):
        relay_rows(last - 1)

    def piece_arrived(part):
        with scope('piece'):
            received(bd.at[:, piece(c, part)], grecv.at[part])
            hand_piece(part).start()

    for part in range(UPS):
        with scope('last_u'):
            hand_strip(part).wait_recv()

        def up_half(t, carry):
            u = jnp.dot(xt[t].reshape(rows, d), bu[:, strip(part)], preferred_element_type=F32)
            hbuf[t, :, strip(part)] = (abuf[t, :, strip(part)] * u).astype(BF16)
            return carry

        if 1 <= part < UPS - 1:
            strip_arrived(part + 1)
        with scope('up_half'):
            lax.fori_loop(0, 2, up_half, 0)
    piece_arrived(0)

    first, second = sums(0), sums(1)

    def then_first(j, color):
        spread_sums(j, color, 0)

    def then_second(j, color):
        spread_sums(j, color, 1)

    def spread_sums(j, color, part):
        @pl.when(j == 0)
        def _():
            far_sum(color, 0, part).start()
            far_sum(color, 1, part).start()

        for h in (0, 1):
            @pl.when(j == 1 + h)
            def _():
                near_sum(color, h, 0, part).start()

    def result(part, color):
        down([piece(color, part)])
        for k in (0, 1):
            @pl.when(color == k)
            def _():
                send(last, part, (k,))

    result(0, c)
    piece_arrived(1)
    with scope('last_d'):
        hand_piece(0).wait_recv()
    result(0, 1 - c)
    result(1, c)
    with scope('last_d'):
        hand_piece(1).wait_recv()
    result(1, 1 - c)
    with scope('relay'):
        relay_rows(last, 0)
    for part in range(2, PARTS):
        piece_arrived(part)
        result(part, c)
        if part == 2:
            with scope('relay'):
                relay_rows(last, 1)
            fetch_rows(last - 1)
        with scope('last_d'):
            hand_piece(part).wait_recv()
        result(part, 1 - c)
        if part > 2:
            with scope('relay'):
                relay_rows(last, part - 1)
        with scope('between'):
            if part == 2:
                await_rows(last - 1)
            add_fetched(last - 1, 2 * part - 4, 2 * part - 2 if part < PARTS - 1 else 8)
    rows_arrived(last, range(FIRST))
    with scope('first_sums'):
        add_last(first, 0, 2, then_first)
    with scope('relay'):
        relay_rows(last, PARTS - 1)
    with scope('first_sums'):
        add_last(first, 2, 8, then_first)
    rows_arrived(last, range(FIRST, PARTS))
    with scope('second_sums'):
        add_last(second, 0, 8, then_second)
    for part in range(SUMS):
        w = sums(part)
        for color in (0, 1):
            with scope('farsum_wait'):
                received(rf2.at[color, :, :, w], f2recv.at[color, part])
            for h in (0, 1):
                r = pl.ds(h * half, half)
                acc[color, 1 + 2 * h, r, w] = acc[color, 1 + 2 * h, r, w] + rf2[color, h, :, w]
                near_sum(color, h, 1, part).start()
    for part in range(SUMS):
        w = sums(part)
        for color in (0, 1):
            with scope('nearsum_wait'):
                received(rn2.at[color, :, :, w], n2recv.at[color, part])
            here = pl.ds(color * cols + w.start, w.size)
            out[:, here] = (acc[color, 0, :, w] + rn2[color, 0, :, w] + rn2[color, 1, :, w]).astype(out.dtype)

    sent(acc.at[:, pl.ds(1, 3)], ssend)
    sent(o_hbm, rsend)
    for n, ref in enumerate((all_ids, all_gates)):
        sent(ref.at[pl.ds(1, BLOCKS - 1)], msend.at[n])
    for m in range(3):
        sent(held[m].at[pl.ds(0, EXPERTS - 1)], wsend.at[m])


def run_moe(hidden, ids, gates, w_gate, w_up, w_down):
    tokens, d = hidden.shape
    f = w_gate.shape[1]
    half, cols = tokens // 2, d // 2
    hbm = pl.BlockSpec(memory_space=pl.ANY)
    dma = pltpu.SemaphoreType.DMA
    flops = 2 * EXPERTS * BLOCKS * ROW_CAP * d * (3 * f + 4 * tokens)

    return pl.pallas_call(
        moe_kernel,
        in_specs=[hbm] * 6,
        out_specs=[pl.BlockSpec(memory_space=pltpu.VMEM)] + [hbm] * 7,
        out_shape=[
            pltpu.VMEM((tokens, d), BF16),
            jax.ShapeDtypeStruct((EXPERTS, 4, 4, ROW_CAP, d), BF16),
            jax.ShapeDtypeStruct((EXPERTS, BLOCKS, ROW_CAP, d), BF16),
            jax.ShapeDtypeStruct((EXPERTS, 2, 3, 4, ROW_CAP, cols), BF16),
            jax.ShapeDtypeStruct((EXPERTS, 2, 2, 2, ROW_CAP, cols), BF16),
            jax.ShapeDtypeStruct((8, d, f), BF16),
            jax.ShapeDtypeStruct((8, d, f), BF16),
            jax.ShapeDtypeStruct((8, f, d), BF16),
        ],
        scratch_shapes=[
            pltpu.VMEM((BLOCKS, tokens, d), BF16),
            pltpu.VMEM((BLOCKS,) + ids.shape, jnp.int32),
            pltpu.VMEM((BLOCKS,) + gates.shape, F32),
            pltpu.VMEM((BLOCKS, EXPERTS, tokens), F32),
            pltpu.VMEM((2, 4, 4, 4, EXPERTS, tokens), F32),
            pltpu.VMEM((2, 4, tokens, cols), F32),
            pltpu.VMEM((2, 2, half, cols), F32),
            pltpu.VMEM((2, 2, tokens, cols), F32),
            pltpu.VMEM((2, 2, 2, ROW_CAP, cols), BF16),
            pltpu.VMEM((2, 3, 4, ROW_CAP, cols), BF16),
            pltpu.VMEM((4, 4, ROW_CAP, d), BF16),
            pltpu.VMEM((2, TILE, ROW_CAP, d), BF16),
            pltpu.VMEM((2, TILE * ROW_CAP, f), F32),
            pltpu.VMEM((2, TILE * ROW_CAP, f), BF16),
            pltpu.VMEM((d, f), BF16),
            pltpu.VMEM((d, f), BF16),
            pltpu.VMEM((f, d), BF16),
            dma(()), dma((5, 2)), dma((2,)), dma((2,)), dma((3,)), dma((2, 3)), dma((4,)), dma((3, 2)), dma((11,)), dma((PARTS,)), dma((PARTS,)), dma((UPS,)), dma((UPS,)),
            dma(()), dma((EXPERTS - 1 + PARTS,)), dma((EXPERTS - 1 + PARTS,)), dma(()), dma((2, SUMS)), dma((2, SUMS)), dma((3,)), dma((2,)), dma((3,)), dma((2,)), dma((2,)), pltpu.SemaphoreType.REGULAR, pltpu.SemaphoreType.REGULAR,
        ],
        compiler_params=pltpu.CompilerParams(collective_id=0, has_side_effects=True, vmem_limit_bytes=62 * MIB),
        cost_estimate=pl.CostEstimate(flops=flops, bytes_accessed=400 * MIB, transcendentals=0),
        name='run_moe',
    )(hidden, ids, gates, w_gate, w_up, w_down)[0]


def solution(mesh):
    grid = Mesh(mesh.devices.reshape((mesh.shape['dp'],) + SIZES), ('dp',) + GRID)

    def body(hidden, route_idx, gate_weights, w_gate, w_up, w_down):
        return run_moe(hidden, route_idx.T, gate_weights.T, w_gate[0], w_up[0], w_down[0])

    r = P(('dp',) + GRID, None)
    e = P(GRID, None, None)
    return jax.shard_map(body, mesh=grid, in_specs=(r, r, r, e, e, e), out_specs=r, check_vma=False)
```

```python
import jax
import jax.numpy as jnp
from jax import lax
from jax.experimental import pallas as pl
from jax.experimental.pallas import tpu as pltpu
from jax.sharding import Mesh, PartitionSpec as P

BF16 = jnp.bfloat16
F32 = jnp.float32
MESH = pl.DeviceIdType.MESH
GRID = ('z', 'y', 'x', 'c')
SIZES = (4, 4, 4, 2)
ROW_CAP = 64
EXPERTS = 8
BLOCKS = 16
TILE = 8
EDGES = (0, 128, 256, 512, 768, 1024)
PARTS = len(EDGES) - 1
SUMS = 2
FIRST = 3
OPENING = 128
UPS = 3
MIB = 1024 * 1024
BOTH = (0, 1)
RING = 4
PAIR = 2
WHOLE = None
OTHERS = pl.ds(1, BLOCKS - 1)
scope = jax.named_scope


def repeat(count, step):
    lax.fori_loop(0, count, step, 0)


def wrap(n):
    return lax.rem(n, RING)


def toward(h):
    return 1 + 2 * h


def expert_ids(place, x, c, line):
    dx = jnp.where((place == 2) | (place == 4), 3, 0) + jnp.where((place == 3) | (place == 5), 1, 0)
    dx += jnp.where(place >= 6, 2, 0)
    core = jnp.where(place == 0, c, 0) + jnp.where(place == 1, 1 - c, 0)
    core += jnp.where((place == 4) | (place == 5) | (place == 7), 1, 0)
    return line * EXPERTS + wrap(x + dx) * 2 + core


def moe_kernel(hid, ids, gates, wg, wu, wd, out, o_hbm, x_hbm, rows_in, relay, hg, hu, hd,
               tok, all_ids, all_gates, slots, tabs, acc, rf2, rn2, last_relay, last_in, stage, xt, abuf, ubuf, hbuf, bg, bu, bd,
               tsend, trecv, msend, mrecv, wsend, irecv, frecv, drecv, precv, grecv, qrecv, urecv, vrecv,
               rsend, rrecv, hrecv, ssend, f2recv, n2recv, lsem, ssem, wsem, xsem, csem, up_free, down_free):
    z, y, x, c = (lax.axis_index(a) for a in GRID)
    right, left = wrap(x + 1), wrap(x + 3)
    tokens, d = hid.shape
    half, cols = tokens // 2, d // 2
    every = pl.ds(0, cols)
    rows = TILE * ROW_CAP
    own = (wg, wu, wd)
    held = (hg, hu, hd)
    partner = {'c': 1 - c}

    def remote(src, dst, send, recv, where):
        return pltpu.make_async_remote_copy(src_ref=src, dst_ref=dst, send_sem=send, recv_sem=recv, device_id=where, device_id_type=MESH)

    def received(ref, sem):
        remote(ref, ref, sem, sem, partner).wait_recv()

    def sent(ref, sem):
        remote(ref, ref, sem, sem, partner).wait_send()

    def along(dim, step):
        return {'z': wrap(z + (1 - dim) * step), 'y': wrap(y + dim * step)}

    def quarter(ref, m, lane, q, count=1):
        n = own[m].shape[0] // 4
        return ref.at[pl.ds(pl.multiple_of((2 * lane + q) * n, n), count * n), :]

    def lane_of(ref, m, lane):
        return quarter(ref, m, lane, 0, 2)

    def line_copies(way, k, m, src, which=BOTH):
        n = own[m].shape[0] // 2
        cuts = (0, OPENING, n) if (k, m) == (1, 0) else (0, n)
        dst, where = held[m].at[2 + 2 * k + way], {'x': right if way == 0 else left}
        copies = []
        for j in which[:len(cuts) - 1]:
            a, b = cuts[j:j + 2]
            at = pl.ds(pl.multiple_of(c * n + a, 64), b - a)
            copies.append(remote(src.at[at, :], dst.at[at, :], wsend.at[m], irecv.at[k, m], where))
        return copies

    def far_copy(k, m, q):
        src, dst = held[m].at[2 + 2 * k + q], held[m].at[6 + k]
        return remote(quarter(src, m, c, q), quarter(dst, m, c, q), wsend.at[m], frecv.at[3 * k + m], {'x': right if q == 0 else left})

    def hand_own(m, n):
        lane = 1 - c if n == 0 else c
        return remote(lane_of(own[m], m, lane), lane_of(held[m].at[c], m, lane), wsend.at[m], drecv.at[m, n], partner)

    def hand_on(slot, m):
        ref = lane_of(held[m].at[slot], m, c)
        return remote(ref, ref, wsend.at[m], precv.at[2 * (slot - 2) + m // 2], partner)

    def start_line(k, m, src, which=BOTH):
        for way in BOTH:
            for cp in line_copies(way, k, m, src, which):
                cp.start()

    def piece(color, part):
        return pl.ds(pl.multiple_of(color * cols + EDGES[part], 128), EDGES[part + 1] - EDGES[part])

    def far_piece(q, part):
        n = wd.shape[0] // 2
        at = pl.ds(q * n, n), piece(c, part)
        return remote(hd.at[4 + q, *at], bd.at[*at], wsend.at[2], grecv.at[part], {'x': right if q == 0 else left})

    def hand_piece(part):
        ref = bd.at[:, piece(c, part)]
        return remote(ref, ref, wsend.at[2], qrecv.at[part], partner)

    def strip(part):
        n = wu.shape[1] // UPS
        return pl.ds(part * n, n)

    def strip_of(ref, lane, q, count, part):
        n = ref.shape[0] // 4
        return ref.at[pl.ds(pl.multiple_of((2 * lane + q) * n, n), count * n), strip(part)]

    def far_strip(q, part):
        return remote(strip_of(hu.at[4 + q], c, q, 1, part), strip_of(bu, c, q, 1, part), wsend.at[1], urecv.at[part], {'x': right if q == 0 else left})

    def hand_strip(part):
        ref = strip_of(bu, c, 0, 2, part)
        return remote(ref, ref, wsend.at[1], vrecv.at[part], partner)

    def place(k, a, b):
        return a * 4 + b if k == 0 else b * 4 + a

    def part(k, a, b, h=WHOLE):
        r = pl.ds(0, tokens) if h is WHOLE else pl.ds(h * half, half)
        return tok.at[place(k, a, b), r, pl.ds(k * cols, cols)]

    def first_copy(k, way):
        sems = tsend, trecv.at[4, way // 2], along(k, toward(way % 2))
        if way < 2:
            return remote(part(k, 0, 0), part(k, 3 - 2 * way, 0), *sems)
        return remote(part(k, 7 - 2 * way, 0, way - 2), part(k, 2, 0, way - 2), *sems)

    def second_copy(k, a, way):
        sems = tsend, trecv.at[a, way // 2], along(1 - k, toward(way % 2))
        if way < 2:
            return remote(part(k, a, 0), part(k, a, 3 - 2 * way), *sems)
        return remote(part(k, a, 7 - 2 * way, way - 2), part(k, a, 2, way - 2), *sems)

    def route_copies(dz, dy):
        s = ((4 - dz) % 4) * 4 + (4 - dy) % 4
        where = {'z': wrap(z + dz), 'y': wrap(y + dy)}
        return [remote(ref.at[0], ref.at[s], msend.at[n], mrecv.at[n], where) for n, ref in enumerate((all_ids, all_gates))]

    peers = [(dz, dy) for dz in range(4) for dy in range(4) if dz or dy]

    def spread(color, i, ring, m, n, part=WHOLE):
        ref, w = (o_hbm.at[i], pl.ds(color * cols, cols)) if part is WHOLE else (stage, piece(color, part))
        if color == 0:
            return ref.at[pl.ds(m, n), ring, :, w]
        return ref.at[ring, pl.ds(m, n), :, w]

    def landing(i, color, s, m, n, part):
        if part is WHOLE:
            return rows_in.at[i, color, s - 1, pl.ds(m, n)]
        return last_in.at[color, s - 1, pl.ds(m, n), :, within(part)]

    def halfway(i, color, h, part):
        return relay.at[i, color, h] if part is WHOLE else last_relay.at[color, h, :, :, within(part)]

    def within(part):
        return every if part is WHOLE else pl.ds(EDGES[part], EDGES[part + 1] - EDGES[part])

    def sums(part):
        return pl.ds(part * (cols // SUMS), cols // SUMS)

    def row_sems(send, recv, i, part, color, h):
        return send, recv.at[i if part is WHOLE else i + part], along(1 - color, toward(h))

    def near_rows(i, color, h, part=WHOLE):
        return remote(spread(color, i, toward(h), 0, 4, part), landing(i, color, 3 - 2 * h, 0, 4, part), *row_sems(rsend, rrecv, i, part, color, h))

    def far_rows(i, color, h, part=WHOLE):
        return remote(spread(color, i, 2, 2 * h, 2, part), halfway(i, color, h, part), *row_sems(rsend, hrecv, i, part, color, h))

    def pass_rows(i, color, h, part=WHOLE):
        return remote(halfway(i, color, h, part), landing(i, color, 2, 2 * h, 2, part), *row_sems(rsend, rrecv, i, part, color, h))

    def far_sum(color, h, part):
        r, w = pl.ds(h * half, half), sums(part)
        return remote(acc.at[color, 2, r, w], rf2.at[color, h, :, w], ssend, f2recv.at[color, part], along(color, toward(h)))

    def near_sum(color, h, waits, part):
        r, w = pl.ds((h if waits else 1 - h) * half, half), sums(part)
        return remote(acc.at[color, toward(h), r, w], rn2.at[color, h, r, w], ssend, n2recv.at[color, part], along(color, toward(h)))

    both = [(color, h) for color in BOTH for h in BOTH]

    own_tok = pltpu.make_async_copy(hid, tok.at[0], lsem.at[0])
    own_tok.start()
    own_routes = [pltpu.make_async_copy(ids, all_ids.at[0], lsem.at[1]), pltpu.make_async_copy(gates, all_gates.at[0], lsem.at[2])]
    for cp in own_routes:
        cp.start()

    barrier = pltpu.get_barrier_semaphore()
    for where in [partner, {'x': right}, {'x': left}] + [{'z': wrap(z + dz), 'y': wrap(y + dy)} for dz, dy in peers]:
        pl.semaphore_signal(barrier, inc=1, device_id=where, device_id_type=MESH)
    pl.semaphore_wait(barrier, 3 + len(peers))

    for n in BOTH:
        for m in range(3):
            hand_own(m, n).start()

    @pl.when(c == 0)
    def _():
        for m in range(3):
            start_line(0, m, own[m])

    @pl.when(c == 1)
    def _():
        start_line(1, 0, own[0], (0,))

    own_tok.wait()
    for k in BOTH:
        for way in BOTH:
            first_copy(k, way).start()
            second_copy(k, 0, way).start()
    for cp in own_routes:
        cp.wait()
    for dz, dy in peers:
        for cp in route_copies(dz, dy):
            cp.start()
    for m in range(3):
        hand_own(m, 0).wait_recv()

        @pl.when(c == 1)
        def _():
            start_line(0, m, held[m].at[0])

    for m in range(3):
        @pl.when(c == 0)
        def _():
            start_line(1, m, held[m].at[1])

        @pl.when(c == 1)
        def _():
            start_line(1, m, own[m], (1,) if m == 0 else (0,))

    def tokens_arrived(a, late):
        received(tok.at[pl.ds(0, 1 if late else 2)], trecv.at[a, late])

    tokens_arrived(4, 0)
    for k in BOTH:
        for way in BOTH:
            first_copy(k, 2 + way).start()
            second_copy(k, 3, way).start()
            second_copy(k, 1, way).start()
    tokens_arrived(0, 0)
    for k in BOTH:
        for way in BOTH:
            second_copy(k, 0, 2 + way).start()
    tokens_arrived(4, 1)
    for k in BOTH:
        for way in BOTH:
            second_copy(k, 2, way).start()

    for n, ref in enumerate((all_ids, all_gates)):
        received(ref.at[OTHERS], mrecv.at[n])
    order = lax.broadcasted_iota(jnp.int32, (EXPERTS, tokens), 0)
    earlier = lax.broadcasted_iota(jnp.int32, (tokens, tokens), 0) < lax.broadcasted_iota(jnp.int32, (tokens, tokens), 1)
    earlier = jnp.where(earlier, 1.0, 0.0).astype(BF16)

    def table(s, line):
        mine = expert_ids(order, x, c, line)
        rec, weight = all_ids[s], all_gates[s]
        chosen = jnp.zeros((EXPERTS, tokens), F32)
        gate = jnp.zeros((EXPERTS, tokens), F32)
        for k in range(rec.shape[0]):
            hit = rec[k:k + 1, :] == mine
            chosen += jnp.where(hit, 1.0, 0.0)
            gate += jnp.where(hit, weight[k:k + 1, :], 0.0)
        rank = jnp.dot(chosen.astype(BF16), earlier, preferred_element_type=F32)
        return jnp.where(chosen > 0.5, rank, -1.0), gate

    def own_table(s, carry):
        slots[s] = table(s, z * 4 + y)[0]
        return carry

    repeat(BLOCKS, own_table)

    def ring_table(n, carry):
        color, m, s = n // 16, wrap(n // 4), wrap(n)
        line = wrap(z + color * s) * 4 + wrap(y + (1 - color) * s)
        slot, gate = table((4 - 3 * color) * m, line)
        tabs[color, m, s, 0] = slot
        for p in range(1, 4):
            term = (gate * (1 - 2.0 ** -8) if p == 1 else gate).astype(BF16).astype(F32)
            tabs[color, m, s, p] = term
            gate = gate - term
        return carry

    def turn(a):
        tokens_arrived(a, 0)
        for k in BOTH:
            for way in BOTH:
                second_copy(k, a, 2 + way).start()

    turn(3)
    turn(1)
    turn(2)
    repeat(32, ring_table)
    for a in range(4):
        tokens_arrived(a, 1)

    def x_store(s, b):
        return pltpu.make_async_copy(stage.at[pl.ds(2 * b, 2)].reshape(EXPERTS, ROW_CAP, d), x_hbm.at[:, s], ssem.at[b])

    lanes = lax.broadcasted_iota(jnp.int32, (ROW_CAP, tokens), 0).astype(F32)

    def gather(s, carry):
        b = lax.rem(s, 2)
        pick = jnp.concatenate([jnp.where(slots[s, pl.ds(e, 1), :] == lanes, 1.0, 0.0).astype(BF16) for e in range(EXPERTS)], axis=0)
        got = jnp.dot(pick, tok[s], preferred_element_type=F32).astype(BF16)

        @pl.when(s >= 2)
        def _():
            x_store(s, b).wait()

        stage[pl.ds(2 * b, 2)] = got.reshape(2, 4, ROW_CAP, d)
        x_store(s, b).start()
        return carry

    repeat(BLOCKS, gather)
    acc[...] = jnp.zeros(acc.shape, F32)
    x_store(0, 0).wait()
    x_store(0, 1).wait()
    sent(tok.at[OTHERS], tsend)

    def load(i, m, go):
        dst = (bg, bu, bd)[m]

        @pl.when(i == 0)
        def _():
            go(pltpu.make_async_copy(own[m], dst, wsem.at[m]))

        @pl.when(i == 1)
        def _():
            go(pltpu.make_async_copy(held[m].at[1 - c], dst, wsem.at[m]))

        @pl.when(i >= 2)
        def _():
            go(pltpu.make_async_copy(held[m].at[i], dst, wsem.at[m]))

    def line_arrived(k, ms):
        for m in ms:
            received(held[m].at[0], irecv.at[k, m])
            for way in BOTH:
                if k == 0 or m == 0:
                    far_copy(k, m, way).start()
                hand_on(2 + 2 * k + way, m).start()

    def far_arrived(k, ms):
        for m in ms:
            received(lane_of(held[m].at[6 + k], m, c), frecv.at[3 * k + m])
            hand_on(6 + k, m).start()

    def handed(i, ms):
        @pl.when(i == 1)
        def _():
            for m in ms:
                hand_own(m, 1).wait_recv()

        @pl.when(i >= 2)
        def _():
            if ms == (2,):
                hand_on(i, 2).wait_recv()
            else:
                received(held[0].at[0], precv.at[2 * (i - 2)])

    def x_load(i, t):
        return pltpu.make_async_copy(x_hbm.at[i, pl.ds(t * TILE, TILE)], xt.at[t], xsem.at[t])

    def o_store(i, t):
        return pltpu.make_async_copy(stage.at[pl.ds(2 * t, 2)], o_hbm.at[i, pl.ds(2 * t, 2)], ssem.at[t])

    def begin(cp):
        cp.start()

    def finish(cp):
        cp.wait()

    def relay_rows(i, part=WHOLE):
        if part is WHOLE:
            received(relay.at[i], hrecv.at[i])
        else:
            received(last_relay.at[:, :, :, :, within(part)], hrecv.at[i + part])
        for color, h in both:
            pass_rows(i, color, h, part).start()

    def row_loads(i, color):
        at = pl.ds(8 * lax.rem(i, 2) + 4 * color, 4)
        srcs = [spread(color, i, 0, 0, 4)] + [rows_in.at[i, color, s] for s in range(3)]
        return [pltpu.make_async_copy(src, tok.at[at, pl.ds(s * ROW_CAP, ROW_CAP), every], csem.at[color]) for s, src in enumerate(srcs)]

    def rows_arrived(i, parts=(WHOLE,)):
        with scope('rows_wait'):
            for part in parts:
                if part is WHOLE:
                    received(rows_in.at[i], rrecv.at[i])
                else:
                    received(last_in.at[:, :, :, :, within(part)], rrecv.at[i + part])

    def fetch_rows(i):
        rows_arrived(i)
        for color in BOTH:
            for cp in row_loads(i, color):
                cp.start()

    def await_rows(i):
        with scope('rowload_wait'):
            for color in BOTH:
                ref = tok.at[pl.ds(8 * lax.rem(i, 2) + 4 * color, 4), :, every]
                pltpu.make_async_copy(ref, ref, csem.at[color]).wait()

    def add_rows(i, w, take, start=0, stop=8, then=WHOLE):
        def one(n, carry):
            j, color = n // 2, lax.rem(n, 2)
            m = wrap(2 + 3 * j + 3 * (j * (j - 1) // 2))
            got = take(color, m)
            total = acc[color, m, :, w]
            for p in range(1, 4):
                g = jnp.concatenate([
                    jnp.where(tabs[color, m, s, 0, pl.ds(i, 1), :] == lanes, tabs[color, m, s, p, pl.ds(i, 1), :], 0.0).astype(BF16)
                    for s in range(4)], axis=0)
                total += lax.dot_general(g, got, (((0,), (0,)), ((), ())), preferred_element_type=F32)
            acc[color, m, :, w] = total
            if then is not WHOLE:
                then(j, color)
            return carry

        lax.fori_loop(start, stop, one, 0)

    def add_fetched(i, start=0, stop=8):
        add_rows(i, every, lambda color, m: tok[8 * lax.rem(i, 2) + 4 * color + m, :, every], start, stop)

    def add_last(w, start, stop, then):
        def take(color, m):
            here = pl.ds(pl.multiple_of(color * cols + w.start, 128), w.size)
            return jnp.concatenate([stage[(1 - color) * m, color * m, :, here]] + [last_in[color, s, m, :, w] for s in range(3)], axis=0)

        add_rows(EXPERTS - 1, w, take, start, stop, then)

    def combine(i):
        fetch_rows(i)
        await_rows(i)
        add_fetched(i)

    def load_up(i):
        handed(i, BOTH)
        load(i, 0, begin)
        load(i, 1, begin)

    def load_down(i):
        handed(i, (2,))
        load(i, 2, begin)

    def down(ws):
        def one(t, carry):
            for w in ws:
                o = jnp.dot(hbuf[t], bd[:, w], preferred_element_type=F32).astype(BF16)
                stage[pl.ds(2 * t, 2), :, :, w] = o.reshape(2, 4, ROW_CAP, o.shape[-1])
            return carry

        with scope('down'):
            repeat(2, one)

    def send(i, part=WHOLE, colors=BOTH):
        for color in colors:
            for h in BOTH:
                far_rows(i, color, h, part).start()
        for color in colors:
            for h in BOTH:
                near_rows(i, color, h, part).start()

    def release(sem):
        for where in (partner, {'x': right}, {'x': left}):
            pl.semaphore_signal(sem, inc=1, device_id=where, device_id_type=MESH)

    def expert(i, carry):
        late = (i == 4) | (i == 6)
        for t in BOTH:
            x_load(i, t).start()

        @pl.when(jnp.logical_not(late))
        def _():
            load_down(i)


        @pl.when(late)
        def _():
            with scope('late_gu'):
                load_up(i)

        with scope('load_gu'):
            load(i, 0, finish)
            load(i, 1, finish)

        def up(t, carry):
            x_load(i, t).wait()
            xs = xt[t].reshape(rows, d)
            a = jnp.dot(xs, bg[...], preferred_element_type=F32)
            u = jnp.dot(xs, bu[...], preferred_element_type=F32)
            hbuf[t] = (jax.nn.silu(a) * u).astype(BF16)
            return carry

        with scope('up'):
            repeat(2, up)

        @pl.when(i == 1)
        def _():
            with scope('line0'):
                line_arrived(0, (0, 1, 2))

        @pl.when(i == 6)
        def _():
            release(up_free)

        @pl.when((i == 0) | (i == 2) | (i == 4))
        def _():
            with scope('next_gu'):
                load_up(i + 1)

        @pl.when(i == 4)
        def _():
            with scope('line1_d'):
                line_arrived(1, (2,))

        @pl.when(i == 6)
        def _():
            with scope('far0_d'):
                far_arrived(0, (2,))

        @pl.when(i >= 1)
        def _():
            with scope('relay'):
                relay_rows(i - 1)

        @pl.when(i >= 2)
        def _():
            with scope('combine'):
                combine(i - 2)

        @pl.when(i == 1)
        def _():
            with scope('next_gu'):
                load_up(i + 1)

        @pl.when(i == 3)
        def _():
            with scope('line1_gu'):
                line_arrived(1, BOTH)

        @pl.when(i == 5)
        def _():
            with scope('far0_gu'):
                far_arrived(0, BOTH)

        @pl.when(i == 6)
        def _():
            pl.semaphore_wait(up_free, 3)
            for part in range(UPS):
                for q in BOTH:
                    far_strip(q, part).start()

        @pl.when(late)
        def _():
            with scope('late_d'):
                load_down(i)

        with scope('load_d'):
            load(i, 2, finish)
        down([pl.ds(0, d)])
        with scope('store'):
            for t in BOTH:
                o_store(i, t).start()
            for t in BOTH:
                o_store(i, t).wait()
        send(i)
        return carry

    load_up(0)
    repeat(EXPERTS - 1, expert)

    last = EXPERTS - 1
    for t in BOTH:
        x_load(last, t).start()
    release(down_free)
    pl.semaphore_wait(down_free, 3)
    for part in range(PARTS):
        for q in BOTH:
            far_piece(q, part).start()
    def strip_arrived(part):
        far_strip(0, part).wait_recv()
        far_strip(1, part).wait_recv()
        hand_strip(part).start()

    def strip_arrived(part):
        with scope('strip'):
            received(strip_of(bu, c, 0, 2, part), urecv.at[part])
            hand_strip(part).start()

    def gate_half(t, carry):
        x_load(last, t).wait()
        a = jnp.dot(xt[t].reshape(rows, d), bg[...], preferred_element_type=F32)
        abuf[t] = jax.nn.silu(a)
        return carry

    with scope('last_g'):
        far_arrived(1, (0,))
    with scope('combine'):
        combine(last - 2)
    with scope('last_g'):
        hand_on(last, 0).wait_recv()
        g_load = pltpu.make_async_copy(hg.at[last], bg, wsem.at[0])
        g_load.start()
    strip_arrived(0)
    with scope('last_g'):
        g_load.wait()
    with scope('gate_half'):
        repeat(2, gate_half)
    strip_arrived(1)
    with scope('relay'):
        relay_rows(last - 1)

    def piece_arrived(part):
        with scope('piece'):
            received(bd.at[:, piece(c, part)], grecv.at[part])
            hand_piece(part).start()

    def up_half(part):
        def one(t, carry):
            u = jnp.dot(xt[t].reshape(rows, d), bu[:, strip(part)], preferred_element_type=F32)
            hbuf[t, :, strip(part)] = (abuf[t, :, strip(part)] * u).astype(BF16)
            return carry

        with scope('last_u'):
            hand_strip(part).wait_recv()
        with scope('up_half'):
            repeat(PAIR, one)

    for part in range(UPS - 1):
        up_half(part)
    end = UPS - 1
    strip_arrived(end)

    def by_lane(t, lane):
        at = pl.ds(pl.multiple_of(lane * (d // PAIR), 128), d // PAIR)
        return jnp.dot(xt[t, :, :, at].reshape(rows, d // PAIR), bu[at, strip(end)], preferred_element_type=F32)

    def own_lane(t, carry):
        ubuf[t] = by_lane(t, c)
        return carry

    def other_lane(t, carry):
        u = ubuf[t] + by_lane(t, 1 - c)
        hbuf[t, :, strip(end)] = (abuf[t, :, strip(end)] * u).astype(BF16)
        return carry

    with scope('own_lane'):
        repeat(PAIR, own_lane)
    with scope('last_u'):
        hand_strip(end).wait_recv()
    with scope('other_lane'):
        repeat(PAIR, other_lane)
    piece_arrived(0)

    first, second = sums(0), sums(1)

    def then_first(j, color):
        spread_sums(j, color, 0)

    def then_second(j, color):
        spread_sums(j, color, 1)

    def spread_sums(j, color, part):
        @pl.when(j == 0)
        def _():
            far_sum(color, 0, part).start()
            far_sum(color, 1, part).start()

        for h in BOTH:
            @pl.when(j == 1 + h)
            def _():
                near_sum(color, h, 0, part).start()

    def result(part, color):
        down([piece(color, part)])
        for k in BOTH:
            @pl.when(color == k)
            def _():
                send(last, part, (k,))

    result(0, c)
    with scope('last_d'):
        hand_piece(0).wait_recv()
    result(0, 1 - c)
    piece_arrived(1)
    result(1, c)
    with scope('last_d'):
        hand_piece(1).wait_recv()
    result(1, 1 - c)
    with scope('relay'):
        relay_rows(last, 0)
    for part in range(2, PARTS):
        piece_arrived(part)
        result(part, c)
        if part == 2:
            with scope('relay'):
                relay_rows(last, 1)
            fetch_rows(last - 1)
        with scope('last_d'):
            hand_piece(part).wait_recv()
        result(part, 1 - c)
        if part > 2:
            with scope('relay'):
                relay_rows(last, part - 1)
        with scope('between'):
            if part == 2:
                await_rows(last - 1)
            add_fetched(last - 1, 2 * part - 4, 2 * part - 2 if part < PARTS - 1 else 8)
    rows_arrived(last, range(FIRST))
    with scope('first_sums'):
        add_last(first, 0, 2, then_first)
    with scope('relay'):
        relay_rows(last, PARTS - 1)
    with scope('first_sums'):
        add_last(first, 2, 8, then_first)
    rows_arrived(last, range(FIRST, PARTS))
    with scope('second_sums'):
        add_last(second, 0, 8, then_second)
    for part in range(SUMS):
        w = sums(part)
        for color in BOTH:
            with scope('farsum_wait'):
                received(rf2.at[color, :, :, w], f2recv.at[color, part])
            for h in BOTH:
                r = pl.ds(h * half, half)
                acc[color, toward(h), r, w] = acc[color, toward(h), r, w] + rf2[color, h, :, w]
                near_sum(color, h, 1, part).start()
    for part in range(SUMS):
        w = sums(part)
        for color in BOTH:
            with scope('nearsum_wait'):
                received(rn2.at[color, :, :, w], n2recv.at[color, part])
            here = pl.ds(color * cols + w.start, w.size)
            out[:, here] = (acc[color, 0, :, w] + rn2[color, 0, :, w] + rn2[color, 1, :, w]).astype(out.dtype)

    sent(acc.at[:, pl.ds(1, 3)], ssend)
    sent(o_hbm, rsend)
    for n, ref in enumerate((all_ids, all_gates)):
        sent(ref.at[OTHERS], msend.at[n])
    for m in range(3):
        sent(held[m].at[pl.ds(0, EXPERTS - 1)], wsend.at[m])


def run_moe(hidden, ids, gates, w_gate, w_up, w_down):
    tokens, d = hidden.shape
    f = w_gate.shape[1]
    half, cols = tokens // 2, d // 2
    hbm = pl.BlockSpec(memory_space=pl.ANY)
    dma = pltpu.SemaphoreType.DMA
    flops = 2 * EXPERTS * BLOCKS * ROW_CAP * d * (3 * f + 4 * tokens)

    return pl.pallas_call(
        moe_kernel,
        in_specs=[hbm] * 6,
        out_specs=[pl.BlockSpec(memory_space=pltpu.VMEM)] + [hbm] * 7,
        out_shape=[
            pltpu.VMEM((tokens, d), BF16),
            jax.ShapeDtypeStruct((EXPERTS, RING, RING, ROW_CAP, d), BF16),
            jax.ShapeDtypeStruct((EXPERTS, BLOCKS, ROW_CAP, d), BF16),
            jax.ShapeDtypeStruct((EXPERTS, PAIR, 3, RING, ROW_CAP, cols), BF16),
            jax.ShapeDtypeStruct((EXPERTS, PAIR, PAIR, PAIR, ROW_CAP, cols), BF16),
            jax.ShapeDtypeStruct((EXPERTS, d, f), BF16),
            jax.ShapeDtypeStruct((EXPERTS, d, f), BF16),
            jax.ShapeDtypeStruct((EXPERTS, f, d), BF16),
        ],
        scratch_shapes=[
            pltpu.VMEM((BLOCKS, tokens, d), BF16),
            pltpu.VMEM((BLOCKS,) + ids.shape, jnp.int32),
            pltpu.VMEM((BLOCKS,) + gates.shape, F32),
            pltpu.VMEM((BLOCKS, EXPERTS, tokens), F32),
            pltpu.VMEM((PAIR, RING, RING, 4, EXPERTS, tokens), F32),
            pltpu.VMEM((PAIR, RING, tokens, cols), F32),
            pltpu.VMEM((PAIR, PAIR, half, cols), F32),
            pltpu.VMEM((PAIR, PAIR, tokens, cols), F32),
            pltpu.VMEM((PAIR, PAIR, PAIR, ROW_CAP, cols), BF16),
            pltpu.VMEM((PAIR, 3, RING, ROW_CAP, cols), BF16),
            pltpu.VMEM((RING, RING, ROW_CAP, d), BF16),
            pltpu.VMEM((PAIR, TILE, ROW_CAP, d), BF16),
            pltpu.VMEM((PAIR, TILE * ROW_CAP, f), F32),
            pltpu.VMEM((PAIR, TILE * ROW_CAP, f // UPS), F32),
            pltpu.VMEM((PAIR, TILE * ROW_CAP, f), BF16),
            pltpu.VMEM((d, f), BF16),
            pltpu.VMEM((d, f), BF16),
            pltpu.VMEM((f, d), BF16),
            dma(()), dma((5, 2)), dma((PAIR,)), dma((PAIR,)), dma((3,)), dma((2, 3)), dma((4,)), dma((3, 2)), dma((11,)), dma((PARTS,)), dma((PARTS,)), dma((UPS,)), dma((UPS,)),
            dma(()), dma((EXPERTS - 1 + PARTS,)), dma((EXPERTS - 1 + PARTS,)), dma(()), dma((PAIR, SUMS)), dma((PAIR, SUMS)), dma((3,)), dma((PAIR,)), dma((3,)), dma((PAIR,)), dma((PAIR,)), pltpu.SemaphoreType.REGULAR, pltpu.SemaphoreType.REGULAR,
        ],
        compiler_params=pltpu.CompilerParams(collective_id=0, has_side_effects=True, vmem_limit_bytes=62 * MIB),
        cost_estimate=pl.CostEstimate(flops=flops, bytes_accessed=400 * MIB, transcendentals=0),
        name='run_moe',
    )(hidden, ids, gates, w_gate, w_up, w_down)[0]


def solution(mesh):
    grid = Mesh(mesh.devices.reshape((mesh.shape['dp'],) + SIZES), ('dp',) + GRID)

    def body(hidden, route_idx, gate_weights, w_gate, w_up, w_down):
        return run_moe(hidden, route_idx.T, gate_weights.T, w_gate[0], w_up[0], w_down[0])

    r = P(('dp',) + GRID, None)
    e = P(GRID, None, None)
    return jax.shard_map(body, mesh=grid, in_specs=(r, r, r, e, e, e), out_specs=r, check_vma=False)
```

```python
import jax
import jax.numpy as jnp
from jax import lax
from jax.experimental import pallas as pl
from jax.experimental.pallas import tpu as pltpu
from jax.sharding import Mesh, PartitionSpec as P

BF16 = jnp.bfloat16
F32 = jnp.float32
MESH = pl.DeviceIdType.MESH
GRID = ('z', 'y', 'x', 'c')
SIZES = (4, 4, 4, 2)
ROW_CAP = 64
EXPERTS = 8
BLOCKS = 16
TILE = 8
EDGES = (0, 128, 256, 512, 768, 1024)
PARTS = len(EDGES) - 1
SUMS = 2
FIRST = 3
OPENING = 128
UPS = 3
MIB = 1024 * 1024
BOTH = (0, 1)
RING = 4
PAIR = 2
WHOLE = None
OTHERS = pl.ds(1, BLOCKS - 1)
scope = jax.named_scope


def repeat(count, step):
    lax.fori_loop(0, count, step, 0)


def wrap(n):
    return lax.rem(n, RING)


def toward(h):
    return 1 + 2 * h


def expert_ids(place, x, c, line):
    dx = jnp.where((place == 2) | (place == 4), 3, 0) + jnp.where((place == 3) | (place == 5), 1, 0)
    dx += jnp.where(place >= 6, 2, 0)
    core = jnp.where(place == 0, c, 0) + jnp.where(place == 1, 1 - c, 0)
    core += jnp.where((place == 4) | (place == 5) | (place == 7), 1, 0)
    return line * EXPERTS + wrap(x + dx) * 2 + core


def moe_kernel(hid, ids, gates, wg, wu, wd, out, o_hbm, x_hbm, rows_in, relay, hg, hu, hd,
               tok, all_ids, all_gates, slots, tabs, acc, rf2, rn2, last_relay, last_in, stage, xt, abuf, ubuf, hbuf, bg, bu, bd,
               tsend, trecv, msend, mrecv, wsend, irecv, frecv, drecv, precv, grecv, qrecv, urecv, vrecv,
               rsend, rrecv, hrecv, ssend, f2recv, n2recv, ssem, wsem, xsem, csem, up_free, down_free):
    z, y, x, c = (lax.axis_index(a) for a in GRID)
    right, left = wrap(x + 1), wrap(x + 3)
    tokens, d = hid.shape
    half, cols = tokens // 2, d // 2
    every = pl.ds(0, cols)
    rows = TILE * ROW_CAP
    own = (wg, wu, wd)
    held = (hg, hu, hd)
    partner = {'c': 1 - c}

    def remote(src, dst, send, recv, where):
        return pltpu.make_async_remote_copy(src_ref=src, dst_ref=dst, send_sem=send, recv_sem=recv, device_id=where, device_id_type=MESH)

    def received(ref, sem):
        remote(ref, ref, sem, sem, partner).wait_recv()

    def sent(ref, sem):
        remote(ref, ref, sem, sem, partner).wait_send()

    def along(dim, step):
        return {'z': wrap(z + (1 - dim) * step), 'y': wrap(y + dim * step)}

    def quarter(ref, m, lane, q, count=1):
        n = own[m].shape[0] // 4
        return ref.at[pl.ds(pl.multiple_of((2 * lane + q) * n, n), count * n), :]

    def lane_of(ref, m, lane):
        return quarter(ref, m, lane, 0, 2)

    def line_copies(way, k, m, src, which=BOTH):
        n = own[m].shape[0] // 2
        cuts = (0, OPENING, n) if (k, m) == (1, 0) else (0, n)
        dst, where = held[m].at[2 + 2 * k + way], {'x': right if way == 0 else left}
        copies = []
        for j in which[:len(cuts) - 1]:
            a, b = cuts[j:j + 2]
            at = pl.ds(pl.multiple_of(c * n + a, 64), b - a)
            copies.append(remote(src.at[at, :], dst.at[at, :], wsend.at[m], irecv.at[k * (1 + m // 2)], where))
        return copies

    def far_copy(k, m, q):
        src, dst = held[m].at[2 + 2 * k + q], held[m].at[6 + k]
        return remote(quarter(src, m, c, q), quarter(dst, m, c, q), wsend.at[m], frecv.at[3 * k + m], {'x': right if q == 0 else left})

    def hand_own(m, n):
        lane = 1 - c if n == 0 else c
        return remote(lane_of(own[m], m, lane), lane_of(held[m].at[c], m, lane), wsend.at[m], drecv.at[m, n], partner)

    def hand_on(slot, m):
        ref = lane_of(held[m].at[slot], m, c)
        return remote(ref, ref, wsend.at[m], precv.at[2 * (slot - 2) + m // 2], partner)

    def start_line(k, m, src, which=BOTH):
        for way in BOTH:
            for cp in line_copies(way, k, m, src, which):
                cp.start()

    def piece(color, part):
        return pl.ds(pl.multiple_of(color * cols + EDGES[part], 128), EDGES[part + 1] - EDGES[part])

    def far_piece(q, part):
        n = wd.shape[0] // 2
        at = pl.ds(q * n, n), piece(c, part)
        return remote(hd.at[4 + q, *at], bd.at[*at], wsend.at[2], grecv.at[part], {'x': right if q == 0 else left})

    def hand_piece(part):
        ref = bd.at[:, piece(c, part)]
        return remote(ref, ref, wsend.at[2], qrecv.at[part], partner)

    def strip(part):
        n = wu.shape[1] // UPS
        return pl.ds(part * n, n)

    def strip_of(ref, lane, q, count, part):
        n = ref.shape[0] // 4
        return ref.at[pl.ds(pl.multiple_of((2 * lane + q) * n, n), count * n), strip(part)]

    def far_strip(q, part):
        return remote(strip_of(hu.at[4 + q], c, q, 1, part), strip_of(bu, c, q, 1, part), wsend.at[1], urecv.at[part], {'x': right if q == 0 else left})

    def hand_strip(part):
        ref = strip_of(bu, c, 0, 2, part)
        return remote(ref, ref, wsend.at[1], vrecv.at[part], partner)

    def place(k, a, b):
        return a * 4 + b if k == 0 else b * 4 + a

    def part(k, a, b, h=WHOLE):
        r = pl.ds(0, tokens) if h is WHOLE else pl.ds(h * half, half)
        return tok.at[place(k, a, b), r, pl.ds(k * cols, cols)]

    def first_copy(k, way):
        sems = tsend, trecv.at[4, way // 2], along(k, toward(way % 2))
        if way < 2:
            return remote(part(k, 0, 0), part(k, 3 - 2 * way, 0), *sems)
        return remote(part(k, 7 - 2 * way, 0, way - 2), part(k, 2, 0, way - 2), *sems)

    def second_copy(k, a, way):
        sems = tsend, trecv.at[0 if way >= PAIR else a, way // 2], along(1 - k, toward(way % 2))
        if way < 2:
            return remote(part(k, a, 0), part(k, a, 3 - 2 * way), *sems)
        return remote(part(k, a, 7 - 2 * way, way - 2), part(k, a, 2, way - 2), *sems)

    def route_copies(dz, dy):
        s = ((4 - dz) % 4) * 4 + (4 - dy) % 4
        where = {'z': wrap(z + dz), 'y': wrap(y + dy)}
        return [remote(ref.at[0], ref.at[s], msend.at[n], mrecv.at[n], where) for n, ref in enumerate((all_ids, all_gates))]

    peers = [(dz, dy) for dz in range(4) for dy in range(4) if dz or dy]

    def spread(color, i, ring, m, n, part=WHOLE):
        ref, w = (o_hbm.at[i], pl.ds(color * cols, cols)) if part is WHOLE else (stage, piece(color, part))
        if color == 0:
            return ref.at[pl.ds(m, n), ring, :, w]
        return ref.at[ring, pl.ds(m, n), :, w]

    def landing(i, color, s, m, n, part):
        if part is WHOLE:
            return rows_in.at[i, color, s - 1, pl.ds(m, n)]
        return last_in.at[color, s - 1, pl.ds(m, n), :, within(part)]

    def halfway(i, color, h, part):
        return relay.at[i, color, h] if part is WHOLE else last_relay.at[color, h, :, :, within(part)]

    def within(part):
        return every if part is WHOLE else pl.ds(EDGES[part], EDGES[part + 1] - EDGES[part])

    def sums(part):
        return pl.ds(part * (cols // SUMS), cols // SUMS)

    def row_sems(send, recv, i, part, color, h):
        return send, recv.at[i if part is WHOLE else i + part], along(1 - color, toward(h))

    def near_rows(i, color, h, part=WHOLE):
        return remote(spread(color, i, toward(h), 0, 4, part), landing(i, color, 3 - 2 * h, 0, 4, part), *row_sems(rsend, rrecv, i, part, color, h))

    def far_rows(i, color, h, part=WHOLE):
        return remote(spread(color, i, 2, 2 * h, 2, part), halfway(i, color, h, part), *row_sems(rsend, hrecv, i, part, color, h))

    def pass_rows(i, color, h, part=WHOLE):
        return remote(halfway(i, color, h, part), landing(i, color, 2, 2 * h, 2, part), *row_sems(rsend, rrecv, i, part, color, h))

    def far_sum(color, h, part):
        r, w = pl.ds(h * half, half), sums(part)
        return remote(acc.at[color, 2, r, w], rf2.at[color, h, :, w], ssend, f2recv.at[color, part], along(color, toward(h)))

    def near_sum(color, h, waits, part):
        r, w = pl.ds((h if waits else 1 - h) * half, half), sums(part)
        return remote(acc.at[color, toward(h), r, w], rn2.at[color, h, r, w], ssend, n2recv.at[color, part], along(color, toward(h)))

    both = [(color, h) for color in BOTH for h in BOTH]

    own_tok = pltpu.make_async_copy(hid, tok.at[0], wsem.at[0])
    own_tok.start()
    own_routes = [pltpu.make_async_copy(ids, all_ids.at[0], wsem.at[1]), pltpu.make_async_copy(gates, all_gates.at[0], wsem.at[2])]
    for cp in own_routes:
        cp.start()

    barrier = pltpu.get_barrier_semaphore()
    for where in [partner, {'x': right}, {'x': left}] + [{'z': wrap(z + dz), 'y': wrap(y + dy)} for dz, dy in peers]:
        pl.semaphore_signal(barrier, inc=1, device_id=where, device_id_type=MESH)
    pl.semaphore_wait(barrier, 3 + len(peers))

    for n in BOTH:
        for m in range(3):
            hand_own(m, n).start()

    @pl.when(c == 0)
    def _():
        for m in range(3):
            start_line(0, m, own[m])

    @pl.when(c == 1)
    def _():
        start_line(1, 0, own[0], (0,))

    own_tok.wait()
    for k in BOTH:
        for way in BOTH:
            first_copy(k, way).start()
            second_copy(k, 0, way).start()
    for cp in own_routes:
        cp.wait()
    for dz, dy in peers:
        for cp in route_copies(dz, dy):
            cp.start()
    for m in range(3):
        hand_own(m, 0).wait_recv()

        @pl.when(c == 1)
        def _():
            start_line(0, m, held[m].at[0])

    for m in range(3):
        @pl.when(c == 0)
        def _():
            start_line(1, m, held[m].at[1])

        @pl.when(c == 1)
        def _():
            start_line(1, m, own[m], (1,) if m == 0 else (0,))

    def tokens_arrived(a, late):
        received(tok.at[pl.ds(0, 1 if late else 2)], trecv.at[a, late])

    tokens_arrived(4, 0)
    for k in BOTH:
        for way in BOTH:
            first_copy(k, 2 + way).start()
            second_copy(k, 3, way).start()
            second_copy(k, 1, way).start()
    tokens_arrived(0, 0)
    for k in BOTH:
        for way in BOTH:
            second_copy(k, 0, 2 + way).start()
    tokens_arrived(4, 1)
    for k in BOTH:
        for way in BOTH:
            second_copy(k, 2, way).start()

    for n, ref in enumerate((all_ids, all_gates)):
        received(ref.at[OTHERS], mrecv.at[n])
    order = lax.broadcasted_iota(jnp.int32, (EXPERTS, tokens), 0)
    earlier = lax.broadcasted_iota(jnp.int32, (tokens, tokens), 0) < lax.broadcasted_iota(jnp.int32, (tokens, tokens), 1)
    earlier = jnp.where(earlier, 1.0, 0.0).astype(BF16)

    def table(s, line):
        mine = expert_ids(order, x, c, line)
        rec, weight = all_ids[s], all_gates[s]
        chosen = jnp.zeros((EXPERTS, tokens), F32)
        gate = jnp.zeros((EXPERTS, tokens), F32)
        for k in range(rec.shape[0]):
            hit = rec[k:k + 1, :] == mine
            chosen += jnp.where(hit, 1.0, 0.0)
            gate += jnp.where(hit, weight[k:k + 1, :], 0.0)
        rank = jnp.dot(chosen.astype(BF16), earlier, preferred_element_type=F32)
        return jnp.where(chosen > 0.5, rank, -1.0), gate

    def own_table(s, carry):
        slots[s] = table(s, z * 4 + y)[0]
        return carry

    repeat(BLOCKS, own_table)

    def ring_table(n, carry):
        color, m, s = n // 16, wrap(n // 4), wrap(n)
        line = wrap(z + color * s) * 4 + wrap(y + (1 - color) * s)
        slot, gate = table((4 - 3 * color) * m, line)
        tabs[color, m, s, 0] = slot
        for p in range(1, 4):
            term = (gate * (1 - 2.0 ** -8) if p == 1 else gate).astype(BF16).astype(F32)
            tabs[color, m, s, p] = term
            gate = gate - term
        return carry

    def turn(a):
        tokens_arrived(a, 0)
        for k in BOTH:
            for way in BOTH:
                second_copy(k, a, 2 + way).start()

    turn(3)
    turn(1)
    turn(2)
    repeat(32, ring_table)
    received(tok.at[pl.ds(0, RING)], trecv.at[0, 1])

    def x_store(s, b):
        return pltpu.make_async_copy(stage.at[pl.ds(2 * b, 2)].reshape(EXPERTS, ROW_CAP, d), x_hbm.at[:, s], ssem.at[b])

    lanes = lax.broadcasted_iota(jnp.int32, (ROW_CAP, tokens), 0).astype(F32)

    def gather(s, carry):
        b = lax.rem(s, 2)
        pick = jnp.concatenate([jnp.where(slots[s, pl.ds(e, 1), :] == lanes, 1.0, 0.0).astype(BF16) for e in range(EXPERTS)], axis=0)
        got = jnp.dot(pick, tok[s], preferred_element_type=F32).astype(BF16)

        @pl.when(s >= 2)
        def _():
            x_store(s, b).wait()

        stage[pl.ds(2 * b, 2)] = got.reshape(2, 4, ROW_CAP, d)
        x_store(s, b).start()
        return carry

    repeat(BLOCKS, gather)
    acc[...] = jnp.zeros(acc.shape, F32)
    x_store(0, 0).wait()
    x_store(0, 1).wait()
    sent(tok.at[OTHERS], tsend)

    def load(i, m, go):
        dst = (bg, bu, bd)[m]

        @pl.when(i == 0)
        def _():
            go(pltpu.make_async_copy(own[m], dst, wsem.at[m]))

        @pl.when(i == 1)
        def _():
            go(pltpu.make_async_copy(held[m].at[1 - c], dst, wsem.at[m]))

        @pl.when(i >= 2)
        def _():
            go(pltpu.make_async_copy(held[m].at[i], dst, wsem.at[m]))

    def line_arrived(k, ms):
        received(hg.at[pl.ds(0, len(ms))], irecv.at[k * (1 + ms[0] // 2)])
        for m in ms:
            for way in BOTH:
                if k == 0 or m == 0:
                    far_copy(k, m, way).start()
                hand_on(2 + 2 * k + way, m).start()

    def far_arrived(k, ms):
        for m in ms:
            received(lane_of(held[m].at[6 + k], m, c), frecv.at[3 * k + m])
            hand_on(6 + k, m).start()

    def handed(i, ms):
        @pl.when(i == 1)
        def _():
            for m in ms:
                hand_own(m, 1).wait_recv()

        @pl.when(i >= 2)
        def _():
            if ms == (2,):
                hand_on(i, 2).wait_recv()
            else:
                received(held[0].at[0], precv.at[2 * (i - 2)])

    def x_load(i, t):
        return pltpu.make_async_copy(x_hbm.at[i, pl.ds(t * TILE, TILE)], xt.at[t], xsem.at[t])

    def o_store(i, t):
        return pltpu.make_async_copy(stage.at[pl.ds(2 * t, 2)], o_hbm.at[i, pl.ds(2 * t, 2)], ssem.at[t])

    def begin(cp):
        cp.start()

    def finish(cp):
        cp.wait()

    def relay_rows(i, part=WHOLE):
        if part is WHOLE:
            received(relay.at[i], hrecv.at[i])
        else:
            received(last_relay.at[:, :, :, :, within(part)], hrecv.at[i + part])
        for color, h in both:
            pass_rows(i, color, h, part).start()

    def row_loads(i, color):
        at = pl.ds(8 * lax.rem(i, 2) + 4 * color, 4)
        srcs = [spread(color, i, 0, 0, 4)] + [rows_in.at[i, color, s] for s in range(3)]
        return [pltpu.make_async_copy(src, tok.at[at, pl.ds(s * ROW_CAP, ROW_CAP), every], csem.at[color]) for s, src in enumerate(srcs)]

    def rows_arrived(i, parts=(WHOLE,)):
        with scope('rows_wait'):
            for part in parts:
                if part is WHOLE:
                    received(rows_in.at[i], rrecv.at[i])
                else:
                    received(last_in.at[:, :, :, :, within(part)], rrecv.at[i + part])

    def fetch_rows(i):
        rows_arrived(i)
        for color in BOTH:
            for cp in row_loads(i, color):
                cp.start()

    def await_rows(i):
        with scope('rowload_wait'):
            for color in BOTH:
                ref = tok.at[pl.ds(8 * lax.rem(i, 2) + 4 * color, 4), :, every]
                pltpu.make_async_copy(ref, ref, csem.at[color]).wait()

    def add_rows(i, w, take, start=0, stop=8, then=WHOLE):
        def one(n, carry):
            j, color = n // 2, lax.rem(n, 2)
            m = wrap(2 + 3 * j + 3 * (j * (j - 1) // 2))
            got = take(color, m)
            total = acc[color, m, :, w]
            for p in range(1, 4):
                g = jnp.concatenate([
                    jnp.where(tabs[color, m, s, 0, pl.ds(i, 1), :] == lanes, tabs[color, m, s, p, pl.ds(i, 1), :], 0.0).astype(BF16)
                    for s in range(4)], axis=0)
                total += lax.dot_general(g, got, (((0,), (0,)), ((), ())), preferred_element_type=F32)
            acc[color, m, :, w] = total
            if then is not WHOLE:
                then(j, color)
            return carry

        lax.fori_loop(start, stop, one, 0)

    def add_fetched(i, start=0, stop=8):
        add_rows(i, every, lambda color, m: tok[8 * lax.rem(i, 2) + 4 * color + m, :, every], start, stop)

    def add_last(w, start, stop, then):
        def take(color, m):
            here = pl.ds(pl.multiple_of(color * cols + w.start, 128), w.size)
            return jnp.concatenate([stage[(1 - color) * m, color * m, :, here]] + [last_in[color, s, m, :, w] for s in range(3)], axis=0)

        add_rows(EXPERTS - 1, w, take, start, stop, then)

    def combine(i):
        fetch_rows(i)
        await_rows(i)
        add_fetched(i)

    def load_up(i):
        handed(i, BOTH)
        load(i, 0, begin)
        load(i, 1, begin)

    def load_down(i):
        handed(i, (2,))
        load(i, 2, begin)

    def down(ws):
        def one(t, carry):
            for w in ws:
                o = jnp.dot(hbuf[t], bd[:, w], preferred_element_type=F32).astype(BF16)
                stage[pl.ds(2 * t, 2), :, :, w] = o.reshape(2, 4, ROW_CAP, o.shape[-1])
            return carry

        with scope('down'):
            repeat(2, one)

    def send(i, part=WHOLE, colors=BOTH):
        for color in colors:
            for h in BOTH:
                far_rows(i, color, h, part).start()
        for color in colors:
            for h in BOTH:
                near_rows(i, color, h, part).start()

    def release(sem):
        for where in (partner, {'x': right}, {'x': left}):
            pl.semaphore_signal(sem, inc=1, device_id=where, device_id_type=MESH)

    def expert(i, carry):
        late = (i == 4) | (i == 6)
        for t in BOTH:
            x_load(i, t).start()

        @pl.when(jnp.logical_not(late))
        def _():
            load_down(i)


        @pl.when(late)
        def _():
            with scope('late_gu'):
                load_up(i)

        with scope('load_gu'):
            load(i, 0, finish)
            load(i, 1, finish)

        def up(t, carry):
            x_load(i, t).wait()
            xs = xt[t].reshape(rows, d)
            a = jnp.dot(xs, bg[...], preferred_element_type=F32)
            u = jnp.dot(xs, bu[...], preferred_element_type=F32)
            hbuf[t] = (jax.nn.silu(a) * u).astype(BF16)
            return carry

        with scope('up'):
            repeat(2, up)

        @pl.when(i == 1)
        def _():
            with scope('line0'):
                line_arrived(0, (0, 1, 2))

        @pl.when(i == 6)
        def _():
            release(up_free)

        @pl.when((i == 0) | (i == 2) | (i == 4))
        def _():
            with scope('next_gu'):
                load_up(i + 1)

        @pl.when(i == 4)
        def _():
            with scope('line1_d'):
                line_arrived(1, (2,))

        @pl.when(i == 6)
        def _():
            with scope('far0_d'):
                far_arrived(0, (2,))

        @pl.when(i >= 1)
        def _():
            with scope('relay'):
                relay_rows(i - 1)

        @pl.when(i >= 2)
        def _():
            with scope('combine'):
                combine(i - 2)

        @pl.when(i == 1)
        def _():
            with scope('next_gu'):
                load_up(i + 1)

        @pl.when(i == 3)
        def _():
            with scope('line1_gu'):
                line_arrived(1, BOTH)

        @pl.when(i == 5)
        def _():
            with scope('far0_gu'):
                far_arrived(0, BOTH)

        @pl.when(i == 6)
        def _():
            pl.semaphore_wait(up_free, 3)
            for part in range(UPS):
                for q in BOTH:
                    far_strip(q, part).start()

        @pl.when(late)
        def _():
            with scope('late_d'):
                load_down(i)

        with scope('load_d'):
            load(i, 2, finish)
        down([pl.ds(0, d)])
        with scope('store'):
            for t in BOTH:
                o_store(i, t).start()
            for t in BOTH:
                o_store(i, t).wait()
        send(i)
        return carry

    load_up(0)
    repeat(EXPERTS - 1, expert)

    last = EXPERTS - 1
    for t in BOTH:
        x_load(last, t).start()
    release(down_free)
    pl.semaphore_wait(down_free, 3)
    for part in range(PARTS):
        for q in BOTH:
            far_piece(q, part).start()
    def strip_arrived(part):
        far_strip(0, part).wait_recv()
        far_strip(1, part).wait_recv()
        hand_strip(part).start()

    def strip_arrived(part):
        with scope('strip'):
            received(strip_of(bu, c, 0, 2, part), urecv.at[part])
            hand_strip(part).start()

    def gate_half(t, carry):
        x_load(last, t).wait()
        a = jnp.dot(xt[t].reshape(rows, d), bg[...], preferred_element_type=F32)
        abuf[t] = jax.nn.silu(a)
        return carry

    with scope('last_g'):
        far_arrived(1, (0,))
    with scope('combine'):
        combine(last - 2)
    with scope('last_g'):
        hand_on(last, 0).wait_recv()
        g_load = pltpu.make_async_copy(hg.at[last], bg, wsem.at[0])
        g_load.start()
    strip_arrived(0)
    with scope('last_g'):
        g_load.wait()
    with scope('gate_half'):
        repeat(2, gate_half)
    strip_arrived(1)
    with scope('relay'):
        relay_rows(last - 1)

    def piece_arrived(part):
        with scope('piece'):
            received(bd.at[:, piece(c, part)], grecv.at[part])
            hand_piece(part).start()

    def up_half(part):
        def one(t, carry):
            u = jnp.dot(xt[t].reshape(rows, d), bu[:, strip(part)], preferred_element_type=F32)
            hbuf[t, :, strip(part)] = (abuf[t, :, strip(part)] * u).astype(BF16)
            return carry

        with scope('last_u'):
            hand_strip(part).wait_recv()
        with scope('up_half'):
            repeat(PAIR, one)

    for part in range(UPS - 1):
        up_half(part)
    end = UPS - 1
    strip_arrived(end)

    def by_lane(t, lane):
        at = pl.ds(pl.multiple_of(lane * (d // PAIR), 128), d // PAIR)
        return jnp.dot(xt[t, :, :, at].reshape(rows, d // PAIR), bu[at, strip(end)], preferred_element_type=F32)

    def own_lane(t, carry):
        ubuf[t] = by_lane(t, c)
        return carry

    def other_lane(t, carry):
        u = ubuf[t] + by_lane(t, 1 - c)
        hbuf[t, :, strip(end)] = (abuf[t, :, strip(end)] * u).astype(BF16)
        return carry

    with scope('own_lane'):
        repeat(PAIR, own_lane)
    with scope('last_u'):
        hand_strip(end).wait_recv()
    with scope('other_lane'):
        repeat(PAIR, other_lane)
    piece_arrived(0)

    first, second = sums(0), sums(1)

    def then_first(j, color):
        spread_sums(j, color, 0)

    def then_second(j, color):
        spread_sums(j, color, 1)

    def spread_sums(j, color, part):
        @pl.when(j == 0)
        def _():
            far_sum(color, 0, part).start()
            far_sum(color, 1, part).start()

        for h in BOTH:
            @pl.when(j == 1 + h)
            def _():
                near_sum(color, h, 0, part).start()

    def result(part, color):
        down([piece(color, part)])
        for k in BOTH:
            @pl.when(color == k)
            def _():
                send(last, part, (k,))

    result(0, c)
    with scope('last_d'):
        hand_piece(0).wait_recv()
    result(0, 1 - c)
    piece_arrived(1)
    result(1, c)
    with scope('last_d'):
        hand_piece(1).wait_recv()
    result(1, 1 - c)
    with scope('relay'):
        relay_rows(last, 0)
    for part in range(2, PARTS):
        piece_arrived(part)
        result(part, c)
        if part == 2:
            with scope('relay'):
                relay_rows(last, 1)
            fetch_rows(last - 1)
        with scope('last_d'):
            hand_piece(part).wait_recv()
        result(part, 1 - c)
        if part > 2:
            with scope('relay'):
                relay_rows(last, part - 1)
        with scope('between'):
            if part == 2:
                await_rows(last - 1)
            add_fetched(last - 1, 2 * part - 4, 2 * part - 2 if part < PARTS - 1 else 8)
    rows_arrived(last, range(FIRST))
    with scope('first_sums'):
        add_last(first, 0, 2, then_first)
    with scope('relay'):
        relay_rows(last, PARTS - 1)
    with scope('first_sums'):
        add_last(first, 2, 8, then_first)
    rows_arrived(last, range(FIRST, PARTS))
    with scope('second_sums'):
        add_last(second, 0, 8, then_second)
    for part in range(SUMS):
        w = sums(part)
        for color in BOTH:
            with scope('farsum_wait'):
                received(rf2.at[color, :, :, w], f2recv.at[color, part])
            for h in BOTH:
                r = pl.ds(h * half, half)
                acc[color, toward(h), r, w] = acc[color, toward(h), r, w] + rf2[color, h, :, w]
                near_sum(color, h, 1, part).start()
    for part in range(SUMS):
        w = sums(part)
        for color in BOTH:
            with scope('nearsum_wait'):
                received(rn2.at[color, :, :, w], n2recv.at[color, part])
            here = pl.ds(color * cols + w.start, w.size)
            out[:, here] = (acc[color, 0, :, w] + rn2[color, 0, :, w] + rn2[color, 1, :, w]).astype(out.dtype)

    sent(acc.at[:, pl.ds(1, 3)], ssend)
    sent(o_hbm, rsend)
    for n, ref in enumerate((all_ids, all_gates)):
        sent(ref.at[OTHERS], msend.at[n])
    for m in range(3):
        sent(held[m].at[pl.ds(0, EXPERTS - 1)], wsend.at[m])


def run_moe(hidden, ids, gates, w_gate, w_up, w_down):
    tokens, d = hidden.shape
    f = w_gate.shape[1]
    half, cols = tokens // 2, d // 2
    hbm = pl.BlockSpec(memory_space=pl.ANY)
    dma = pltpu.SemaphoreType.DMA
    flops = 2 * EXPERTS * BLOCKS * ROW_CAP * d * (3 * f + 4 * tokens)

    return pl.pallas_call(
        moe_kernel,
        in_specs=[hbm] * 6,
        out_specs=[pl.BlockSpec(memory_space=pltpu.VMEM)] + [hbm] * 7,
        out_shape=[
            pltpu.VMEM((tokens, d), BF16),
            jax.ShapeDtypeStruct((EXPERTS, RING, RING, ROW_CAP, d), BF16),
            jax.ShapeDtypeStruct((EXPERTS, BLOCKS, ROW_CAP, d), BF16),
            jax.ShapeDtypeStruct((EXPERTS, PAIR, 3, RING, ROW_CAP, cols), BF16),
            jax.ShapeDtypeStruct((EXPERTS, PAIR, PAIR, PAIR, ROW_CAP, cols), BF16),
            jax.ShapeDtypeStruct((EXPERTS, d, f), BF16),
            jax.ShapeDtypeStruct((EXPERTS, d, f), BF16),
            jax.ShapeDtypeStruct((EXPERTS, f, d), BF16),
        ],
        scratch_shapes=[
            pltpu.VMEM((BLOCKS, tokens, d), BF16),
            pltpu.VMEM((BLOCKS,) + ids.shape, jnp.int32),
            pltpu.VMEM((BLOCKS,) + gates.shape, F32),
            pltpu.VMEM((BLOCKS, EXPERTS, tokens), F32),
            pltpu.VMEM((PAIR, RING, RING, 4, EXPERTS, tokens), F32),
            pltpu.VMEM((PAIR, RING, tokens, cols), F32),
            pltpu.VMEM((PAIR, PAIR, half, cols), F32),
            pltpu.VMEM((PAIR, PAIR, tokens, cols), F32),
            pltpu.VMEM((PAIR, PAIR, PAIR, ROW_CAP, cols), BF16),
            pltpu.VMEM((PAIR, 3, RING, ROW_CAP, cols), BF16),
            pltpu.VMEM((RING, RING, ROW_CAP, d), BF16),
            pltpu.VMEM((PAIR, TILE, ROW_CAP, d), BF16),
            pltpu.VMEM((PAIR, TILE * ROW_CAP, f), F32),
            pltpu.VMEM((PAIR, TILE * ROW_CAP, f // UPS), F32),
            pltpu.VMEM((PAIR, TILE * ROW_CAP, f), BF16),
            pltpu.VMEM((d, f), BF16),
            pltpu.VMEM((d, f), BF16),
            pltpu.VMEM((f, d), BF16),
            dma(()), dma((5, 2)), dma((PAIR,)), dma((PAIR,)), dma((3,)), dma((3,)), dma((4,)), dma((3, 2)), dma((11,)), dma((PARTS,)), dma((PARTS,)), dma((UPS,)), dma((UPS,)),
            dma(()), dma((EXPERTS - 1 + PARTS,)), dma((EXPERTS - 1 + PARTS,)), dma(()), dma((PAIR, SUMS)), dma((PAIR, SUMS)), dma((PAIR,)), dma((3,)), dma((PAIR,)), dma((PAIR,)), pltpu.SemaphoreType.REGULAR, pltpu.SemaphoreType.REGULAR,
        ],
        compiler_params=pltpu.CompilerParams(collective_id=0, has_side_effects=True, vmem_limit_bytes=62 * MIB),
        cost_estimate=pl.CostEstimate(flops=flops, bytes_accessed=400 * MIB, transcendentals=0),
        name='run_moe',
    )(hidden, ids, gates, w_gate, w_up, w_down)[0]


def solution(mesh):
    grid = Mesh(mesh.devices.reshape((mesh.shape['dp'],) + SIZES), ('dp',) + GRID)

    def body(hidden, route_idx, gate_weights, w_gate, w_up, w_down):
        return run_moe(hidden, route_idx.T, gate_weights.T, w_gate[0], w_up[0], w_down[0])

    r = P(('dp',) + GRID, None)
    e = P(GRID, None, None)
    return jax.shard_map(body, mesh=grid, in_specs=(r, r, r, e, e, e), out_specs=r, check_vma=False)
```

```python
import jax
import jax.numpy as jnp
from jax import lax
from jax.experimental import pallas as pl
from jax.experimental.pallas import tpu as pltpu
from jax.sharding import Mesh, PartitionSpec as P

BF16 = jnp.bfloat16
F32 = jnp.float32
MESH = pl.DeviceIdType.MESH
GRID = ('z', 'y', 'x', 'c')
SIZES = (4, 4, 4, 2)
ROW_CAP = 64
EXPERTS = 8
BLOCKS = 16
TILE = 8
EDGES = (0, 128, 256, 512, 768, 1024)
PARTS = len(EDGES) - 1
SUMS = 2
FIRST = 3
OPENING = 128
UPS = 3
MIB = 1024 * 1024
BOTH = (0, 1)
RING = 4
PAIR = 2
WHOLE = None
OTHERS = pl.ds(1, BLOCKS - 1)
scope = jax.named_scope


def repeat(count, step):
    lax.fori_loop(0, count, step, 0)


def wrap(n):
    return lax.rem(n, RING)


def toward(h):
    return 1 + 2 * h


def expert_ids(place, x, c, line):
    dx = jnp.where((place == 2) | (place == 4), 3, 0) + jnp.where((place == 3) | (place == 5), 1, 0)
    dx += jnp.where(place >= 6, 2, 0)
    core = jnp.where(place == 0, c, 0) + jnp.where(place == 1, 1 - c, 0)
    core += jnp.where((place == 4) | (place == 5) | (place == 7), 1, 0)
    return line * EXPERTS + wrap(x + dx) * 2 + core


def moe_kernel(hid, ids, gates, wg, wu, wd, out, o_hbm, x_hbm, rows_in, relay, hg, hu, hd,
               tok, all_ids, all_gates, slots, tabs, acc, rf2, rn2, last_relay, last_in, stage, xt, abuf, ubuf, hbuf, bg, bu, bd,
               tsend, trecv, msend, mrecv, wsend, irecv, frecv, drecv, precv, grecv, qrecv, urecv, vrecv,
               rsend, rrecv, hrecv, ssend, f2recv, n2recv, ssem, wsem, xsem, csem, up_free, down_free):
    z, y, x, c = (lax.axis_index(a) for a in GRID)
    right, left = wrap(x + 1), wrap(x + 3)
    tokens, d = hid.shape
    half, cols = tokens // 2, d // 2
    every = pl.ds(0, cols)
    rows = TILE * ROW_CAP
    own = (wg, wu, wd)
    held = (hg, hu, hd)
    partner = {'c': 1 - c}

    def remote(src, dst, send, recv, where):
        return pltpu.make_async_remote_copy(src_ref=src, dst_ref=dst, send_sem=send, recv_sem=recv, device_id=where, device_id_type=MESH)

    def received(ref, sem):
        remote(ref, ref, sem, sem, partner).wait_recv()

    def sent(ref, sem):
        remote(ref, ref, sem, sem, partner).wait_send()

    def along(dim, step):
        return {'z': wrap(z + (1 - dim) * step), 'y': wrap(y + dim * step)}

    def quarter(ref, m, lane, q, count=1):
        n = own[m].shape[0] // 4
        return ref.at[pl.ds(pl.multiple_of((2 * lane + q) * n, n), count * n), :]

    def lane_of(ref, m, lane):
        return quarter(ref, m, lane, 0, 2)

    def line_copies(way, k, m, src, which=BOTH):
        n = own[m].shape[0] // 2
        cuts = (0, OPENING, n) if (k, m) == (1, 0) else (0, n)
        dst, where = held[m].at[2 + 2 * k + way], {'x': right if way == 0 else left}
        copies = []
        for j in which[:len(cuts) - 1]:
            a, b = cuts[j:j + 2]
            at = pl.ds(pl.multiple_of(c * n + a, 64), b - a)
            copies.append(remote(src.at[at, :], dst.at[at, :], wsend.at[m], irecv.at[k * (1 + m // 2)], where))
        return copies

    def far_copy(k, m, q):
        src, dst = held[m].at[2 + 2 * k + q], held[m].at[6 + k]
        return remote(quarter(src, m, c, q), quarter(dst, m, c, q), wsend.at[m], frecv.at[3 * k + m], {'x': right if q == 0 else left})

    def hand_own(m, n):
        lane = 1 - c if n == 0 else c
        return remote(lane_of(own[m], m, lane), lane_of(held[m].at[c], m, lane), wsend.at[m], drecv.at[m, n], partner)

    def hand_on(slot, m):
        ref = lane_of(held[m].at[slot], m, c)
        return remote(ref, ref, wsend.at[m], precv.at[2 * (slot - 2) + m // 2], partner)

    def start_line(k, m, src, which=BOTH):
        for way in BOTH:
            for cp in line_copies(way, k, m, src, which):
                cp.start()

    def piece(color, part):
        return pl.ds(pl.multiple_of(color * cols + EDGES[part], 128), EDGES[part + 1] - EDGES[part])

    def far_piece(q, part):
        n = wd.shape[0] // 2
        at = pl.ds(q * n, n), piece(c, part)
        return remote(hd.at[4 + q, *at], bd.at[*at], wsend.at[2], grecv.at[part], {'x': right if q == 0 else left})

    def hand_piece(part):
        ref = bd.at[:, piece(c, part)]
        return remote(ref, ref, wsend.at[2], qrecv.at[part], partner)

    def strip(part):
        n = wu.shape[1] // UPS
        return pl.ds(part * n, n)

    def strip_of(ref, lane, q, count, part):
        n = ref.shape[0] // 4
        return ref.at[pl.ds(pl.multiple_of((2 * lane + q) * n, n), count * n), strip(part)]

    def far_strip(q, part):
        return remote(strip_of(hu.at[4 + q], c, q, 1, part), strip_of(bu, c, q, 1, part), wsend.at[1], urecv.at[part], {'x': right if q == 0 else left})

    def hand_strip(part):
        ref = strip_of(bu, c, 0, 2, part)
        return remote(ref, ref, wsend.at[1], vrecv.at[part], partner)

    def place(k, a, b):
        return a * 4 + b if k == 0 else b * 4 + a

    def part(k, a, b, h=WHOLE):
        r = pl.ds(0, tokens) if h is WHOLE else pl.ds(h * half, half)
        return tok.at[place(k, a, b), r, pl.ds(k * cols, cols)]

    def first_copy(k, way):
        sems = tsend, trecv.at[4, way // 2], along(k, toward(way % 2))
        if way < 2:
            return remote(part(k, 0, 0), part(k, 3 - 2 * way, 0), *sems)
        return remote(part(k, 7 - 2 * way, 0, way - 2), part(k, 2, 0, way - 2), *sems)

    def second_copy(k, a, way):
        sems = tsend, trecv.at[0 if way >= PAIR else a, way // 2], along(1 - k, toward(way % 2))
        if way < 2:
            return remote(part(k, a, 0), part(k, a, 3 - 2 * way), *sems)
        return remote(part(k, a, 7 - 2 * way, way - 2), part(k, a, 2, way - 2), *sems)

    def route_copies(dz, dy):
        s = ((4 - dz) % 4) * 4 + (4 - dy) % 4
        where = {'z': wrap(z + dz), 'y': wrap(y + dy)}
        return [remote(ref.at[0], ref.at[s], msend.at[n], mrecv.at[n], where) for n, ref in enumerate((all_ids, all_gates))]

    peers = [(dz, dy) for dz in range(4) for dy in range(4) if dz or dy]

    def spread(color, i, ring, m, n, part=WHOLE):
        ref, w = (o_hbm.at[i], pl.ds(color * cols, cols)) if part is WHOLE else (stage, piece(color, part))
        if color == 0:
            return ref.at[pl.ds(m, n), ring, :, w]
        return ref.at[ring, pl.ds(m, n), :, w]

    def landing(i, color, s, m, n, part):
        if part is WHOLE:
            return rows_in.at[i, color, s - 1, pl.ds(m, n)]
        return last_in.at[color, s - 1, pl.ds(m, n), :, within(part)]

    def halfway(i, color, h, part):
        return relay.at[i, color, h] if part is WHOLE else last_relay.at[color, h, :, :, within(part)]

    def within(part):
        return every if part is WHOLE else pl.ds(EDGES[part], EDGES[part + 1] - EDGES[part])

    def sums(part):
        return pl.ds(part * (cols // SUMS), cols // SUMS)

    def row_sems(recv, n, color, h):
        return rsend, recv.at[n], along(1 - color, toward(h))

    def side(i, part):
        return i if part is WHOLE else i + (part >= FIRST)

    def near_rows(i, color, h, part=WHOLE):
        return remote(spread(color, i, toward(h), 0, 4, part), landing(i, color, 3 - 2 * h, 0, 4, part), *row_sems(rrecv, side(i, part), color, h))

    def far_rows(i, color, h, part=WHOLE):
        return remote(spread(color, i, 2, 2 * h, 2, part), halfway(i, color, h, part), *row_sems(hrecv, i if part is WHOLE else i + part, color, h))

    def pass_rows(i, color, h):
        return remote(halfway(i, color, h, WHOLE), landing(i, color, 2, 2 * h, 2, WHOLE), *row_sems(rrecv, i, color, h))

    def pass_last(color, h, start, stop):
        w = pl.ds(EDGES[start], EDGES[stop] - EDGES[start])
        dst = last_in.at[color, 1, pl.ds(2 * h, 2), :, w]
        return remote(last_relay.at[color, h, :, :, w], dst, *row_sems(rrecv, side(EXPERTS - 1, start), color, h))

    def far_sum(color, h, part):
        r, w = pl.ds(h * half, half), sums(part)
        return remote(acc.at[color, 2, r, w], rf2.at[color, h, :, w], ssend, f2recv.at[color, part], along(color, toward(h)))

    def near_sum(color, h, waits, part):
        r, w = pl.ds((h if waits else 1 - h) * half, half), sums(part)
        return remote(acc.at[color, toward(h), r, w], rn2.at[color, h, r, w], ssend, n2recv.at[color, part], along(color, toward(h)))

    both = [(color, h) for color in BOTH for h in BOTH]

    own_tok = pltpu.make_async_copy(hid, tok.at[0], wsem.at[0])
    own_tok.start()
    own_routes = [pltpu.make_async_copy(ids, all_ids.at[0], wsem.at[1]), pltpu.make_async_copy(gates, all_gates.at[0], wsem.at[2])]
    for cp in own_routes:
        cp.start()

    barrier = pltpu.get_barrier_semaphore()
    for where in [partner, {'x': right}, {'x': left}] + [{'z': wrap(z + dz), 'y': wrap(y + dy)} for dz, dy in peers]:
        pl.semaphore_signal(barrier, inc=1, device_id=where, device_id_type=MESH)
    pl.semaphore_wait(barrier, 3 + len(peers))

    for n in BOTH:
        for m in range(3):
            hand_own(m, n).start()

    @pl.when(c == 0)
    def _():
        for m in range(3):
            start_line(0, m, own[m])

    @pl.when(c == 1)
    def _():
        start_line(1, 0, own[0], (0,))

    own_tok.wait()
    for k in BOTH:
        for way in BOTH:
            first_copy(k, way).start()
            second_copy(k, 0, way).start()
    for cp in own_routes:
        cp.wait()
    for dz, dy in peers:
        for cp in route_copies(dz, dy):
            cp.start()
    for m in range(3):
        hand_own(m, 0).wait_recv()

        @pl.when(c == 1)
        def _():
            start_line(0, m, held[m].at[0])

    for m in range(3):
        @pl.when(c == 0)
        def _():
            start_line(1, m, held[m].at[1])

        @pl.when(c == 1)
        def _():
            start_line(1, m, own[m], (1,) if m == 0 else (0,))

    def tokens_arrived(a, late):
        received(tok.at[pl.ds(0, 1 if late else 2)], trecv.at[a, late])

    tokens_arrived(4, 0)
    for k in BOTH:
        for way in BOTH:
            first_copy(k, 2 + way).start()
            second_copy(k, 3, way).start()
            second_copy(k, 1, way).start()
    tokens_arrived(0, 0)
    for k in BOTH:
        for way in BOTH:
            second_copy(k, 0, 2 + way).start()
    tokens_arrived(4, 1)
    for k in BOTH:
        for way in BOTH:
            second_copy(k, 2, way).start()

    for n, ref in enumerate((all_ids, all_gates)):
        received(ref.at[OTHERS], mrecv.at[n])
    order = lax.broadcasted_iota(jnp.int32, (EXPERTS, tokens), 0)
    earlier = lax.broadcasted_iota(jnp.int32, (tokens, tokens), 0) < lax.broadcasted_iota(jnp.int32, (tokens, tokens), 1)
    earlier = jnp.where(earlier, 1.0, 0.0).astype(BF16)

    def table(s, line):
        mine = expert_ids(order, x, c, line)
        rec, weight = all_ids[s], all_gates[s]
        chosen = jnp.zeros((EXPERTS, tokens), F32)
        gate = jnp.zeros((EXPERTS, tokens), F32)
        for k in range(rec.shape[0]):
            hit = rec[k:k + 1, :] == mine
            chosen += jnp.where(hit, 1.0, 0.0)
            gate += jnp.where(hit, weight[k:k + 1, :], 0.0)
        rank = jnp.dot(chosen.astype(BF16), earlier, preferred_element_type=F32)
        return jnp.where(chosen > 0.5, rank, -1.0), gate

    def own_table(s, carry):
        slots[s] = table(s, z * 4 + y)[0]
        return carry

    repeat(BLOCKS, own_table)

    def ring_table(n, carry):
        color, m, s = n // 16, wrap(n // 4), wrap(n)
        line = wrap(z + color * s) * 4 + wrap(y + (1 - color) * s)
        slot, gate = table((4 - 3 * color) * m, line)
        tabs[color, m, s, 0] = slot
        for p in range(1, 4):
            term = (gate * (1 - 2.0 ** -8) if p == 1 else gate).astype(BF16).astype(F32)
            tabs[color, m, s, p] = term
            gate = gate - term
        return carry

    def turn(a):
        tokens_arrived(a, 0)
        for k in BOTH:
            for way in BOTH:
                second_copy(k, a, 2 + way).start()

    turn(3)
    turn(1)
    turn(2)
    repeat(32, ring_table)
    received(tok.at[pl.ds(0, RING)], trecv.at[0, 1])

    def x_store(s, b):
        return pltpu.make_async_copy(stage.at[pl.ds(2 * b, 2)].reshape(EXPERTS, ROW_CAP, d), x_hbm.at[:, s], ssem.at[b])

    lanes = lax.broadcasted_iota(jnp.int32, (ROW_CAP, tokens), 0).astype(F32)

    def gather(s, carry):
        b = lax.rem(s, 2)
        pick = jnp.concatenate([jnp.where(slots[s, pl.ds(e, 1), :] == lanes, 1.0, 0.0).astype(BF16) for e in range(EXPERTS)], axis=0)
        got = jnp.dot(pick, tok[s], preferred_element_type=F32).astype(BF16)

        @pl.when(s >= 2)
        def _():
            x_store(s, b).wait()

        stage[pl.ds(2 * b, 2)] = got.reshape(2, 4, ROW_CAP, d)
        x_store(s, b).start()
        return carry

    repeat(BLOCKS, gather)
    acc[...] = jnp.zeros(acc.shape, F32)
    x_store(0, 0).wait()
    x_store(0, 1).wait()
    sent(tok.at[OTHERS], tsend)

    def load(i, m, go):
        dst = (bg, bu, bd)[m]

        @pl.when(i == 0)
        def _():
            go(pltpu.make_async_copy(own[m], dst, wsem.at[m]))

        @pl.when(i == 1)
        def _():
            go(pltpu.make_async_copy(held[m].at[1 - c], dst, wsem.at[m]))

        @pl.when(i >= 2)
        def _():
            go(pltpu.make_async_copy(held[m].at[i], dst, wsem.at[m]))

    def line_arrived(k, ms):
        received(hg.at[pl.ds(0, len(ms))], irecv.at[k * (1 + ms[0] // 2)])
        for m in ms:
            for way in BOTH:
                if k == 0 or m == 0:
                    far_copy(k, m, way).start()
                hand_on(2 + 2 * k + way, m).start()

    def far_arrived(k, ms):
        for m in ms:
            received(lane_of(held[m].at[6 + k], m, c), frecv.at[3 * k + m])
            hand_on(6 + k, m).start()

    def handed(i, ms):
        @pl.when(i == 1)
        def _():
            for m in ms:
                hand_own(m, 1).wait_recv()

        @pl.when(i >= 2)
        def _():
            if ms == (2,):
                hand_on(i, 2).wait_recv()
            else:
                received(held[0].at[0], precv.at[2 * (i - 2)])

    def x_load(i, t):
        return pltpu.make_async_copy(x_hbm.at[i, pl.ds(t * TILE, TILE)], xt.at[t], xsem.at[t])

    def o_store(i, t):
        return pltpu.make_async_copy(stage.at[pl.ds(2 * t, 2)], o_hbm.at[i, pl.ds(2 * t, 2)], ssem.at[t])

    def begin(cp):
        cp.start()

    def finish(cp):
        cp.wait()

    def relay_rows(i):
        received(relay.at[i], hrecv.at[i])
        for color, h in both:
            pass_rows(i, color, h).start()

    def relay_last(start, stop):
        with scope('relay'):
            for part in range(start, stop):
                received(last_relay.at[:, :, :, :, within(part)], hrecv.at[EXPERTS - 1 + part])
            for color, h in both:
                pass_last(color, h, start, stop).start()

    def row_loads(i, color):
        at = pl.ds(8 * lax.rem(i, 2) + 4 * color, 4)
        srcs = [spread(color, i, 0, 0, 4)] + [rows_in.at[i, color, s] for s in range(3)]
        return [pltpu.make_async_copy(src, tok.at[at, pl.ds(s * ROW_CAP, ROW_CAP), every], csem.at[color]) for s, src in enumerate(srcs)]

    def last_arrived(part):
        with scope('rows_wait'):
            received(last_in.at[:, :, :, :, sums(part)], rrecv.at[EXPERTS - 1 + part])

    def fetch_rows(i):
        received(rows_in.at[i], rrecv.at[i])
        for color in BOTH:
            for cp in row_loads(i, color):
                cp.start()

    def await_rows(i):
        with scope('rowload_wait'):
            for color in BOTH:
                ref = tok.at[pl.ds(8 * lax.rem(i, 2) + 4 * color, 4), :, every]
                pltpu.make_async_copy(ref, ref, csem.at[color]).wait()

    def add_rows(i, w, take, start=0, stop=8, then=WHOLE):
        def one(n, carry):
            j, color = n // 2, lax.rem(n, 2)
            m = wrap(2 + 3 * j + 3 * (j * (j - 1) // 2))
            got = take(color, m)
            total = acc[color, m, :, w]
            for p in range(1, 4):
                g = jnp.concatenate([
                    jnp.where(tabs[color, m, s, 0, pl.ds(i, 1), :] == lanes, tabs[color, m, s, p, pl.ds(i, 1), :], 0.0).astype(BF16)
                    for s in range(4)], axis=0)
                total += lax.dot_general(g, got, (((0,), (0,)), ((), ())), preferred_element_type=F32)
            acc[color, m, :, w] = total
            if then is not WHOLE:
                then(j, color)
            return carry

        lax.fori_loop(start, stop, one, 0)

    def add_fetched(i, start=0, stop=8):
        add_rows(i, every, lambda color, m: tok[8 * lax.rem(i, 2) + 4 * color + m, :, every], start, stop)

    def add_last(w, start, stop, then):
        def take(color, m):
            here = pl.ds(pl.multiple_of(color * cols + w.start, 128), w.size)
            return jnp.concatenate([stage[(1 - color) * m, color * m, :, here]] + [last_in[color, s, m, :, w] for s in range(3)], axis=0)

        add_rows(EXPERTS - 1, w, take, start, stop, then)

    def combine(i):
        fetch_rows(i)
        await_rows(i)
        add_fetched(i)

    def load_up(i):
        handed(i, BOTH)
        load(i, 0, begin)
        load(i, 1, begin)

    def load_down(i):
        handed(i, (2,))
        load(i, 2, begin)

    def down(ws):
        def one(t, carry):
            for w in ws:
                o = jnp.dot(hbuf[t], bd[:, w], preferred_element_type=F32).astype(BF16)
                stage[pl.ds(2 * t, 2), :, :, w] = o.reshape(2, 4, ROW_CAP, o.shape[-1])
            return carry

        with scope('down'):
            repeat(2, one)

    def send(i, part=WHOLE, colors=BOTH):
        for color in colors:
            for h in BOTH:
                far_rows(i, color, h, part).start()
        for color in colors:
            for h in BOTH:
                near_rows(i, color, h, part).start()

    def release(sem):
        for where in (partner, {'x': right}, {'x': left}):
            pl.semaphore_signal(sem, inc=1, device_id=where, device_id_type=MESH)

    def expert(i, carry):
        late = (i == 4) | (i == 6)
        for t in BOTH:
            x_load(i, t).start()

        @pl.when(jnp.logical_not(late))
        def _():
            load_down(i)


        @pl.when(late)
        def _():
            with scope('late_gu'):
                load_up(i)

        with scope('load_gu'):
            load(i, 0, finish)
            load(i, 1, finish)

        def up(t, carry):
            x_load(i, t).wait()
            xs = xt[t].reshape(rows, d)
            a = jnp.dot(xs, bg[...], preferred_element_type=F32)
            u = jnp.dot(xs, bu[...], preferred_element_type=F32)
            hbuf[t] = (jax.nn.silu(a) * u).astype(BF16)
            return carry

        with scope('up'):
            repeat(2, up)

        @pl.when(i == 1)
        def _():
            with scope('line0'):
                line_arrived(0, (0, 1, 2))

        @pl.when(i == 6)
        def _():
            release(up_free)

        @pl.when((i == 0) | (i == 2) | (i == 4))
        def _():
            with scope('next_gu'):
                load_up(i + 1)

        @pl.when(i == 4)
        def _():
            with scope('line1_d'):
                line_arrived(1, (2,))

        @pl.when(i == 6)
        def _():
            with scope('far0_d'):
                far_arrived(0, (2,))

        @pl.when(i >= 1)
        def _():
            with scope('relay'):
                relay_rows(i - 1)

        @pl.when(i >= 2)
        def _():
            with scope('combine'):
                combine(i - 2)

        @pl.when(i == 1)
        def _():
            with scope('next_gu'):
                load_up(i + 1)

        @pl.when(i == 3)
        def _():
            with scope('line1_gu'):
                line_arrived(1, BOTH)

        @pl.when(i == 5)
        def _():
            with scope('far0_gu'):
                far_arrived(0, BOTH)

        @pl.when(i == 6)
        def _():
            pl.semaphore_wait(up_free, 3)
            for part in range(UPS):
                for q in BOTH:
                    far_strip(q, part).start()

        @pl.when(late)
        def _():
            with scope('late_d'):
                load_down(i)

        with scope('load_d'):
            load(i, 2, finish)
        down([pl.ds(0, d)])
        with scope('store'):
            for t in BOTH:
                o_store(i, t).start()
            for t in BOTH:
                o_store(i, t).wait()
        send(i)
        return carry

    load_up(0)
    repeat(EXPERTS - 1, expert)

    last = EXPERTS - 1
    for t in BOTH:
        x_load(last, t).start()
    release(down_free)
    pl.semaphore_wait(down_free, 3)
    for part in range(PARTS):
        for q in BOTH:
            far_piece(q, part).start()
    def strip_arrived(part):
        far_strip(0, part).wait_recv()
        far_strip(1, part).wait_recv()
        hand_strip(part).start()

    def strip_arrived(part):
        with scope('strip'):
            received(strip_of(bu, c, 0, 2, part), urecv.at[part])
            hand_strip(part).start()

    def gate_half(t, carry):
        x_load(last, t).wait()
        a = jnp.dot(xt[t].reshape(rows, d), bg[...], preferred_element_type=F32)
        abuf[t] = jax.nn.silu(a)
        return carry

    with scope('last_g'):
        far_arrived(1, (0,))
    with scope('combine'):
        combine(last - 2)
    with scope('last_g'):
        hand_on(last, 0).wait_recv()
        g_load = pltpu.make_async_copy(hg.at[last], bg, wsem.at[0])
        g_load.start()
    strip_arrived(0)
    with scope('last_g'):
        g_load.wait()
    with scope('gate_half'):
        repeat(2, gate_half)
    strip_arrived(1)
    with scope('relay'):
        relay_rows(last - 1)

    def piece_arrived(part):
        with scope('piece'):
            received(bd.at[:, piece(c, part)], grecv.at[part])
            hand_piece(part).start()

    def up_half(part):
        def one(t, carry):
            u = jnp.dot(xt[t].reshape(rows, d), bu[:, strip(part)], preferred_element_type=F32)
            hbuf[t, :, strip(part)] = (abuf[t, :, strip(part)] * u).astype(BF16)
            return carry

        with scope('last_u'):
            hand_strip(part).wait_recv()
        with scope('up_half'):
            repeat(PAIR, one)

    for part in range(UPS - 1):
        up_half(part)
    end = UPS - 1
    strip_arrived(end)

    def by_lane(t, lane):
        at = pl.ds(pl.multiple_of(lane * (d // PAIR), 128), d // PAIR)
        return jnp.dot(xt[t, :, :, at].reshape(rows, d // PAIR), bu[at, strip(end)], preferred_element_type=F32)

    def own_lane(t, carry):
        ubuf[t] = by_lane(t, c)
        return carry

    def other_lane(t, carry):
        u = ubuf[t] + by_lane(t, 1 - c)
        hbuf[t, :, strip(end)] = (abuf[t, :, strip(end)] * u).astype(BF16)
        return carry

    with scope('own_lane'):
        repeat(PAIR, own_lane)
    with scope('last_u'):
        hand_strip(end).wait_recv()
    with scope('other_lane'):
        repeat(PAIR, other_lane)
    piece_arrived(0)

    first, second = sums(0), sums(1)

    def then_first(j, color):
        spread_sums(j, color, 0)

    def then_second(j, color):
        spread_sums(j, color, 1)

    def spread_sums(j, color, part):
        @pl.when(j == 0)
        def _():
            far_sum(color, 0, part).start()
            far_sum(color, 1, part).start()

        for h in BOTH:
            @pl.when(j == 1 + h)
            def _():
                near_sum(color, h, 0, part).start()

    def result(part, color):
        down([piece(color, part)])
        for k in BOTH:
            @pl.when(color == k)
            def _():
                send(last, part, (k,))

    result(0, c)
    with scope('last_d'):
        hand_piece(0).wait_recv()
    result(0, 1 - c)
    piece_arrived(1)
    result(1, c)
    with scope('last_d'):
        hand_piece(1).wait_recv()
    result(1, 1 - c)
    relay_last(0, 1)
    for part in range(2, PARTS):
        piece_arrived(part)
        result(part, c)
        if part == 2:
            relay_last(1, 2)
            fetch_rows(last - 1)
        with scope('last_d'):
            hand_piece(part).wait_recv()
        result(part, 1 - c)
        if part > 2:
            relay_last(part - 1, part)
        with scope('between'):
            if part == 2:
                await_rows(last - 1)
            add_fetched(last - 1, 2 * part - 4, 2 * part - 2 if part < PARTS - 1 else 8)
    last_arrived(0)
    with scope('first_sums'):
        add_last(first, 0, 2, then_first)
    relay_last(PARTS - 1, PARTS)
    with scope('first_sums'):
        add_last(first, 2, 8, then_first)
    last_arrived(1)
    with scope('second_sums'):
        add_last(second, 0, 8, then_second)
    for part in range(SUMS):
        w = sums(part)
        for color in BOTH:
            with scope('farsum_wait'):
                received(rf2.at[color, :, :, w], f2recv.at[color, part])
            for h in BOTH:
                r = pl.ds(h * half, half)
                acc[color, toward(h), r, w] = acc[color, toward(h), r, w] + rf2[color, h, :, w]
                near_sum(color, h, 1, part).start()
    for part in range(SUMS):
        w = sums(part)
        for color in BOTH:
            with scope('nearsum_wait'):
                received(rn2.at[color, :, :, w], n2recv.at[color, part])
            here = pl.ds(color * cols + w.start, w.size)
            out[:, here] = (acc[color, 0, :, w] + rn2[color, 0, :, w] + rn2[color, 1, :, w]).astype(out.dtype)

    sent(acc.at[:, pl.ds(1, 3)], ssend)
    sent(o_hbm, rsend)
    for n, ref in enumerate((all_ids, all_gates)):
        sent(ref.at[OTHERS], msend.at[n])
    for m in range(3):
        sent(held[m].at[pl.ds(0, EXPERTS - 1)], wsend.at[m])


def run_moe(hidden, ids, gates, w_gate, w_up, w_down):
    tokens, d = hidden.shape
    f = w_gate.shape[1]
    half, cols = tokens // 2, d // 2
    hbm = pl.BlockSpec(memory_space=pl.ANY)
    dma = pltpu.SemaphoreType.DMA
    flops = 2 * EXPERTS * BLOCKS * ROW_CAP * d * (3 * f + 4 * tokens)

    return pl.pallas_call(
        moe_kernel,
        in_specs=[hbm] * 6,
        out_specs=[pl.BlockSpec(memory_space=pltpu.VMEM)] + [hbm] * 7,
        out_shape=[
            pltpu.VMEM((tokens, d), BF16),
            jax.ShapeDtypeStruct((EXPERTS, RING, RING, ROW_CAP, d), BF16),
            jax.ShapeDtypeStruct((EXPERTS, BLOCKS, ROW_CAP, d), BF16),
            jax.ShapeDtypeStruct((EXPERTS, PAIR, 3, RING, ROW_CAP, cols), BF16),
            jax.ShapeDtypeStruct((EXPERTS, PAIR, PAIR, PAIR, ROW_CAP, cols), BF16),
            jax.ShapeDtypeStruct((EXPERTS, d, f), BF16),
            jax.ShapeDtypeStruct((EXPERTS, d, f), BF16),
            jax.ShapeDtypeStruct((EXPERTS, f, d), BF16),
        ],
        scratch_shapes=[
            pltpu.VMEM((BLOCKS, tokens, d), BF16),
            pltpu.VMEM((BLOCKS,) + ids.shape, jnp.int32),
            pltpu.VMEM((BLOCKS,) + gates.shape, F32),
            pltpu.VMEM((BLOCKS, EXPERTS, tokens), F32),
            pltpu.VMEM((PAIR, RING, RING, 4, EXPERTS, tokens), F32),
            pltpu.VMEM((PAIR, RING, tokens, cols), F32),
            pltpu.VMEM((PAIR, PAIR, half, cols), F32),
            pltpu.VMEM((PAIR, PAIR, tokens, cols), F32),
            pltpu.VMEM((PAIR, PAIR, PAIR, ROW_CAP, cols), BF16),
            pltpu.VMEM((PAIR, 3, RING, ROW_CAP, cols), BF16),
            pltpu.VMEM((RING, RING, ROW_CAP, d), BF16),
            pltpu.VMEM((PAIR, TILE, ROW_CAP, d), BF16),
            pltpu.VMEM((PAIR, TILE * ROW_CAP, f), F32),
            pltpu.VMEM((PAIR, TILE * ROW_CAP, f // UPS), F32),
            pltpu.VMEM((PAIR, TILE * ROW_CAP, f), BF16),
            pltpu.VMEM((d, f), BF16),
            pltpu.VMEM((d, f), BF16),
            pltpu.VMEM((f, d), BF16),
            dma(()), dma((5, 2)), dma((PAIR,)), dma((PAIR,)), dma((3,)), dma((3,)), dma((4,)), dma((3, 2)), dma((11,)), dma((PARTS,)), dma((PARTS,)), dma((UPS,)), dma((UPS,)),
            dma(()), dma((EXPERTS + 1,)), dma((EXPERTS - 1 + PARTS,)), dma(()), dma((PAIR, SUMS)), dma((PAIR, SUMS)), dma((PAIR,)), dma((3,)), dma((PAIR,)), dma((PAIR,)), pltpu.SemaphoreType.REGULAR, pltpu.SemaphoreType.REGULAR,
        ],
        compiler_params=pltpu.CompilerParams(collective_id=0, has_side_effects=True, vmem_limit_bytes=62 * MIB),
        cost_estimate=pl.CostEstimate(flops=flops, bytes_accessed=400 * MIB, transcendentals=0),
        name='run_moe',
    )(hidden, ids, gates, w_gate, w_up, w_down)[0]


def solution(mesh):
    grid = Mesh(mesh.devices.reshape((mesh.shape['dp'],) + SIZES), ('dp',) + GRID)

    def body(hidden, route_idx, gate_weights, w_gate, w_up, w_down):
        return run_moe(hidden, route_idx.T, gate_weights.T, w_gate[0], w_up[0], w_down[0])

    r = P(('dp',) + GRID, None)
    e = P(GRID, None, None)
    return jax.shard_map(body, mesh=grid, in_specs=(r, r, r, e, e, e), out_specs=r, check_vma=False)
```
